32 devices in a mesh: cuts: 2 (over x), row: 16 (over z, y, core).
Axes of the slice: x: 2, y: 2, z: 4, core: 2. Of those that a mesh axis runs over, the one named last changes fastest.
Arguments:
- raw: bfloat16 [2, 3, 5, 1024, 1024], P('cuts', None, None, 'row'), may hold values from -6 to 6
- otf: float32 [2, 1024, 1024], P('cuts', 'row'), may hold values from 0.0135 to 121.5, as said below
- offsets: int32 [3, 2], replicated, may hold values from -256 to 255
- phase_order: int32 [3, 5], replicated, may hold values from 0 to 4, each once within a row
- unmix: float32 [2, 3, 5, 5], replicated, may hold values from -3 to 3
Outputs:
- recon: float32 [2, 1024, 1024], P('cuts', 'row')
The draws below stay inside these ranges and needn't reach their ends.
Inputs may be any that keep to these rules, and one draw needn't show every extreme that they name: `otf`: positive.
All inputs are finite; a program needn't handle non-finite values.
Results may differ from the reference program's by a relative error of at most 0.0072.
Values may be sent and summed in bfloat16 or wider, within the bound.
No kernel may reach another device: no remote copies, remote signals or barrier semaphores. Data moves between devices by JAX's collectives and lax.ppermute only.
A program may use at most 128 MiB of HBM per device.

```python
import math
import jax
import jax.numpy as jnp
from jax import lax

N = 1024
ANGLES = 3
PHASES = 5
BANDS = 5
SLICES = 2


def draw_otf(key, part):
    first = jax.random.fold_in(jax.random.fold_in(key, 11), 0)
    depth = jnp.arange(SLICES, dtype=jnp.float32) / max(SLICES - 1, 1)
    base = jnp.exp(jax.random.uniform(first, (SLICES, N, N), jnp.float32, math.log(0.15), math.log(1.5)))
    ramp = jnp.exp(depth * math.log(3.0))
    return base * ramp[:, None, None]


def with_ends(entries, key, least, largest):
    longest = entries.shape.index(max(entries.shape))
    spots = []
    for shift in (0, 1):
        where = [jax.random.randint(jax.random.fold_in(key, axis), (), 0, length) for axis, length in enumerate(entries.shape)]
        where[longest] = (where[longest] + shift) % entries.shape[longest]
        spots.append(tuple(where))
    return entries.at[spots[0]].set(least).at[spots[1]].set(largest)


def shard_levels(key, dims, pieces, smallest, high):
    def one(dim, blocks):
        heights = jax.random.uniform(jax.random.fold_in(jax.random.fold_in(key, 6), dim), (blocks,), jnp.float32, smallest / len(pieces), high / len(pieces))
        return jnp.repeat(jnp.exp(heights), dims[dim] // blocks).reshape((-1,) + (1,) * (len(dims) - dim - 1))

    gain = one(*pieces[0])
    for cut in pieces[1:]:
        gain = gain * one(*cut)
    return gain


def bell_draw(stream_key, dims, spread, limit, shards=(), held_as=jnp.bfloat16):
    array = jax.random.normal(stream_key, dims, jnp.float32) * spread
    if len(shards) > 0:
        array = shard_levels(stream_key, dims, shards, -0.22, 0.18) * array
    return jnp.clip(array, min=-limit, max=limit).astype(held_as)


def setup_inputs(seed: int = 0) -> dict:
    arg_keys = jax.random.split(jax.random.key(seed), 6)
    return {
        "raw": bell_draw(arg_keys[0], (SLICES, ANGLES, PHASES, N, N), 1.0, 6.0, ((0, 2), (3, 16))),
        "otf": draw_otf(jax.random.fold_in(arg_keys[5], 71), 0),
        "offsets": with_ends(jax.random.randint(arg_keys[2], (ANGLES, 2), 0 - N // 4, N // 4), jax.random.fold_in(arg_keys[2], 1), 0 - N // 4, (N // 4) - 1).astype(jnp.int32),
        "phase_order": jax.vmap(lambda own: jax.random.permutation(own, PHASES))(jax.random.split(arg_keys[3], ANGLES)).reshape((ANGLES, PHASES)).astype(jnp.int32),
        "unmix": bell_draw(arg_keys[4], (2, ANGLES, BANDS, PHASES), 0.45, 3.0, (), jnp.float32),
    }


MULTIPLES = (0, 1, -1, 2, -2)
WIENER = 0.1

def tables(pixels):
    indices = jnp.arange(pixels, dtype=jnp.int32)
    product = indices[:, None] * indices[None, :] % pixels
    phase = product.astype(jnp.float32) * (2.0 * math.pi / pixels)
    factor = 1.0 / math.sqrt(pixels)
    return ((jnp.cos(phase) * factor).astype(jnp.bfloat16), (jnp.sin(phase) * factor).astype(jnp.bfloat16))

def mixing(unmix, phase_order):
    phases = unmix.shape[-1]
    onehot = (phase_order[:, :, None] == jnp.arange(phases, dtype=jnp.int32)[None, None, :]).astype(jnp.float32)
    highest = lax.Precision.HIGHEST
    mix_re = jnp.einsum('amp,ajp->amj', unmix[0], onehot, precision=highest)
    mix_im = jnp.einsum('amp,ajp->amj', unmix[1], onehot, precision=highest)
    return (mix_re, mix_im)

def reference(raw, otf, offsets, phase_order, unmix):
    highest = lax.Precision.HIGHEST
    cosine, sine = tables(N)
    cos_wide = cosine.astype(jnp.float32)
    sin_wide = sine.astype(jnp.float32)
    mix_re, mix_im = mixing(unmix, phase_order)
    squares = lax.optimization_barrier(jnp.sum(otf * otf, axis=0))
    power = jnp.zeros((N, N), jnp.float32)
    for which_angle in range(ANGLES):
        for band_index in range(BANDS):
            power = power + jnp.roll(squares, (MULTIPLES[band_index] * offsets[which_angle, 0], MULTIPLES[band_index] * offsets[which_angle, 1]), axis=(0, 1))
    denom = WIENER + power / (SLICES * ANGLES)

    def one_slice(pair):
        frames, response_base = pair
        frames_wide = frames.astype(jnp.float32)
        spec_re = jnp.einsum('apyx,xk->apyk', frames_wide, cos_wide, precision=highest)
        spec_im = -jnp.einsum('apyx,xk->apyk', frames_wide, sin_wide, precision=highest)
        band_re = jnp.einsum('amj,ajyk->amyk', mix_re, spec_re, precision=highest) - jnp.einsum('amj,ajyk->amyk', mix_im, spec_im, precision=highest)
        band_im = jnp.einsum('amj,ajyk->amyk', mix_re, spec_im, precision=highest) + jnp.einsum('amj,ajyk->amyk', mix_im, spec_re, precision=highest)
        numer_re = jnp.zeros((N, N), jnp.float32)
        numer_im = jnp.zeros((N, N), jnp.float32)
        for which_angle in range(ANGLES):
            for band_index in range(BANDS):
                row_shift = MULTIPLES[band_index] * offsets[which_angle, 0]
                col_shift = MULTIPLES[band_index] * offsets[which_angle, 1]
                part_re = jnp.roll(band_re[which_angle, band_index], col_shift, axis=1).astype(jnp.bfloat16).astype(jnp.float32)
                part_im = jnp.roll(band_im[which_angle, band_index], col_shift, axis=1).astype(jnp.bfloat16).astype(jnp.float32)
                col_re = jnp.dot(cos_wide, part_re, precision=highest) + jnp.dot(sin_wide, part_im, precision=highest)
                col_im = jnp.dot(cos_wide, part_im, precision=highest) - jnp.dot(sin_wide, part_re, precision=highest)
                col_re = jnp.roll(col_re, row_shift, axis=0)
                col_im = jnp.roll(col_im, row_shift, axis=0)
                response = jnp.roll(response_base, (row_shift, col_shift), axis=(0, 1))
                numer_re = numer_re + response * col_re
                numer_im = numer_im + response * col_im
        ratio_re = (numer_re / denom).astype(jnp.bfloat16).astype(jnp.float32)
        ratio_im = (numer_im / denom).astype(jnp.bfloat16).astype(jnp.float32)
        half_re = (jnp.dot(cos_wide, ratio_re, precision=highest) - jnp.dot(sin_wide, ratio_im, precision=highest)).astype(jnp.bfloat16).astype(jnp.float32)
        half_im = (jnp.dot(cos_wide, ratio_im, precision=highest) + jnp.dot(sin_wide, ratio_re, precision=highest)).astype(jnp.bfloat16).astype(jnp.float32)
        return jnp.dot(half_re, cos_wide, precision=highest) - jnp.dot(half_im, sin_wide, precision=highest)
    return lax.map(one_slice, (raw, otf))
```

```python
import math

import jax
import jax.numpy as jnp
from jax import lax
from jax.sharding import PartitionSpec as P

MULTIPLES = (0, 1, -1, 2, -2)
WIENER = 0.1


def tables(pixels):
    fine = 1 << (max(pixels.bit_length() - 1, 0) // 2)
    coarse = pixels // fine
    rows = jnp.arange(pixels, dtype=jnp.int32)[:, None]
    step = 2.0 * math.pi / pixels

    def angle(columns):
        return (rows * columns[None, :] % pixels).astype(jnp.float32) * step

    high = angle(jnp.arange(coarse, dtype=jnp.int32) * fine)
    low = angle(jnp.arange(fine, dtype=jnp.int32))
    factor = 1.0 / math.sqrt(pixels)
    high_cos, high_sin, low_cos, low_sin = lax.optimization_barrier(
        (jnp.cos(high) * factor, jnp.sin(high) * factor, jnp.cos(low), jnp.sin(low))
    )
    high_cos, high_sin = (high_cos[:, :, None], high_sin[:, :, None])
    low_cos, low_sin = (low_cos[:, None, :], low_sin[:, None, :])
    cosine = (high_cos * low_cos - high_sin * low_sin).reshape(pixels, pixels)
    sine = (high_sin * low_cos + high_cos * low_sin).reshape(pixels, pixels)
    return lax.optimization_barrier((cosine.astype(jnp.bfloat16), sine.astype(jnp.bfloat16)))


def mixing(unmix, phase_order):
    phases = unmix.shape[-1]
    onehot = (phase_order[:, :, None] == jnp.arange(phases, dtype=jnp.int32)[None, None, :]).astype(
        jnp.float32
    )
    highest = lax.Precision.HIGHEST
    mix_re = jnp.einsum("amp,ajp->amj", unmix[0], onehot, precision=highest)
    mix_im = jnp.einsum("amp,ajp->amj", unmix[1], onehot, precision=highest)
    return (mix_re, mix_im)


def cyclic(field, amount):
    last = field.ndim - 1
    pixels = field.shape[last]
    offset_start = jnp.mod(-amount, pixels)
    doubled = jnp.concatenate([field, field], axis=last)
    return lax.dynamic_slice_in_dim(doubled, offset_start, pixels, last)


def shift_bands(field, offsets, column):
    stacked = []
    for which_angle in range(field.shape[1]):
        row_list = []
        for band_index in range(field.shape[2]):
            row_list.append(
                cyclic(
                    field[:, which_angle, band_index],
                    MULTIPLES[band_index] * offsets[which_angle, column],
                )
            )
        stacked.append(jnp.stack(row_list, axis=1))
    return jnp.stack(stacked, axis=1)


def shards(raw, otf, offsets, phase_order, unmix):
    pixels = raw.shape[-1]
    slab_rows = raw.shape[3]
    local_slices = raw.shape[0]
    angle_count = raw.shape[1]
    band_count = raw.shape[2]
    row_devices = lax.axis_size("row")
    row_index = lax.axis_index("row")
    cosine, sine = tables(pixels)
    tab_cos = cosine.reshape(row_devices, slab_rows, pixels)
    tab_sin = sine.reshape(row_devices, slab_rows, pixels)
    both_tables = jnp.concatenate([cosine, sine], axis=1)
    flattened = raw.reshape(-1, pixels)
    spectra = jnp.dot(flattened, both_tables, preferred_element_type=jnp.float32)
    spec_re = spectra[:, :pixels].reshape(raw.shape)
    spec_im = -spectra[:, pixels:].reshape(raw.shape)
    mix_re, mix_im = mixing(unmix, phase_order)
    band_re = jnp.zeros((local_slices, angle_count, band_count, slab_rows, pixels), jnp.float32)
    band_im = jnp.zeros((local_slices, angle_count, band_count, slab_rows, pixels), jnp.float32)
    for phase_slot in range(raw.shape[2]):
        weight_re = mix_re[None, :, :, phase_slot, None, None]
        weight_im = mix_im[None, :, :, phase_slot, None, None]
        frame_re = spec_re[:, :, phase_slot][:, :, None]
        frame_im = spec_im[:, :, phase_slot][:, :, None]
        band_re = band_re + (weight_re * frame_re - weight_im * frame_im)
        band_im = band_im + (weight_re * frame_im + weight_im * frame_re)
    band_re = shift_bands(band_re, offsets, 1).astype(jnp.bfloat16)
    band_im = shift_bands(band_im, offsets, 1).astype(jnp.bfloat16)
    real_part = lax.all_to_all(band_re, "row", split_axis=4, concat_axis=4, tiled=True)
    imag_part = lax.all_to_all(band_im, "row", split_axis=4, concat_axis=4, tiled=True)
    split_shape = real_part.shape[:3] + (slab_rows, row_devices, slab_rows)
    real_part = real_part.reshape(split_shape)
    imag_part = imag_part.reshape(split_shape)
    col_re = jnp.einsum(
        "samrdc,drt->samct", real_part, tab_cos, preferred_element_type=jnp.float32
    ) + jnp.einsum("samrdc,drt->samct", imag_part, tab_sin, preferred_element_type=jnp.float32)
    col_im = jnp.einsum(
        "samrdc,drt->samct", imag_part, tab_cos, preferred_element_type=jnp.float32
    ) - jnp.einsum("samrdc,drt->samct", real_part, tab_sin, preferred_element_type=jnp.float32)
    col_re, col_im = (col_re, col_im)
    col_re = shift_bands(col_re, offsets, 0)
    col_im = shift_bands(col_im, offsets, 0)
    whole = lax.all_gather(otf, "row", axis=1, tiled=True)
    doubled = jnp.concatenate([whole, whole], axis=2)
    stacked = []
    for which_angle in range(angle_count):
        row_list = []
        for band_index in range(band_count):
            offset_start = jnp.mod(
                row_index * slab_rows - MULTIPLES[band_index] * offsets[which_angle, 1], pixels
            )
            slab_piece = lax.dynamic_slice_in_dim(doubled, offset_start, slab_rows, 2)
            slab_piece = jnp.swapaxes(slab_piece, 1, 2)
            row_list.append(cyclic(slab_piece, MULTIPLES[band_index] * offsets[which_angle, 0]))
        stacked.append(jnp.stack(row_list, axis=1))
    response = jnp.stack(stacked, axis=1)
    numer_re = jnp.sum(response * col_re, axis=(1, 2))
    numer_im = jnp.sum(response * col_im, axis=(1, 2))
    local_power = jnp.sum(response * response, axis=(0, 1, 2))
    power = lax.psum(local_power, "cuts")
    slices_total = local_slices * lax.axis_size("cuts")
    denom = WIENER + power / (slices_total * angle_count)
    ratio_re = (numer_re / denom).astype(jnp.bfloat16)
    ratio_im = (numer_im / denom).astype(jnp.bfloat16)
    half_re = (
        jnp.einsum("sck,ky->scy", ratio_re, cosine, preferred_element_type=jnp.float32)
        - jnp.einsum("sck,ky->scy", ratio_im, sine, preferred_element_type=jnp.float32)
    ).astype(jnp.bfloat16)
    half_im = (
        jnp.einsum("sck,ky->scy", ratio_im, cosine, preferred_element_type=jnp.float32)
        + jnp.einsum("sck,ky->scy", ratio_re, sine, preferred_element_type=jnp.float32)
    ).astype(jnp.bfloat16)
    back_re, back_im = (
        lax.all_to_all(half_re, "row", split_axis=2, concat_axis=2, tiled=True),
        lax.all_to_all(half_im, "row", split_axis=2, concat_axis=2, tiled=True),
    )
    back_re = back_re.reshape(local_slices, slab_rows, row_devices, slab_rows)
    back_im = back_im.reshape(local_slices, slab_rows, row_devices, slab_rows)
    recon = jnp.einsum(
        "scdr,dcx->srx", back_re, tab_cos, preferred_element_type=jnp.float32
    ) - jnp.einsum("scdr,dcx->srx", back_im, tab_sin, preferred_element_type=jnp.float32)
    return recon


def solution(mesh):
    in_specs = (P("cuts", None, None, "row", None), P("cuts", "row", None), P(), P(), P())
    out_specs = P("cuts", "row", None)
    return jax.shard_map(shards, mesh=mesh, in_specs=in_specs, out_specs=out_specs, check_vma=False)
```

```python
import functools
import math

import jax
import jax.numpy as jnp
from jax import lax
from jax.experimental import pallas as pl
from jax.experimental.pallas import tpu as pltpu
from jax.sharding import PartitionSpec as P

MULTIPLES = (0, 1, -1, 2, -2)
WIENER = 0.1
LANES = 128
GROUP = 16


def tables(pixels):
    fine = 1 << (max(pixels.bit_length() - 1, 0) // 2)
    coarse = pixels // fine
    rows = jnp.arange(pixels, dtype=jnp.int32)[:, None]
    step = 2.0 * math.pi / pixels

    def angle(columns):
        return (rows * columns[None, :] % pixels).astype(jnp.float32) * step

    high = angle(jnp.arange(coarse, dtype=jnp.int32) * fine)
    low = angle(jnp.arange(fine, dtype=jnp.int32))
    factor = 1.0 / math.sqrt(pixels)
    high_cos, high_sin, low_cos, low_sin = lax.optimization_barrier(
        (jnp.cos(high) * factor, jnp.sin(high) * factor, jnp.cos(low), jnp.sin(low))
    )
    high_cos, high_sin = (high_cos[:, :, None], high_sin[:, :, None])
    low_cos, low_sin = (low_cos[:, None, :], low_sin[:, None, :])
    cosine = (high_cos * low_cos - high_sin * low_sin).reshape(pixels, pixels)
    sine = (high_sin * low_cos + high_cos * low_sin).reshape(pixels, pixels)
    return lax.optimization_barrier((cosine.astype(jnp.bfloat16), sine.astype(jnp.bfloat16)))


def mixing(unmix, phase_order):
    phases = unmix.shape[-1]
    onehot = (phase_order[:, :, None] == jnp.arange(phases, dtype=jnp.int32)[None, None, :]).astype(
        jnp.float32
    )
    mixed = jnp.sum(unmix[:, :, :, None, :] * onehot[None, :, None, :, :], axis=-1)
    return (mixed[0], mixed[1])


def band_kernel(angles, phases, shift_ref, raw_ref, cos_ref, sin_ref, coef_ref, out_ref, spec):
    frames = angles * phases
    slab = out_ref.shape[3] // 2
    pixels = raw_ref.shape[1]
    quarter = out_ref.shape[4]
    tile = 256

    @pl.loop(0, pixels // tile)
    def _(step):
        cut = pl.ds(pl.multiple_of(step * tile, tile), tile)
        spec[0, :, cut] = jnp.dot(raw_ref[...], cos_ref[:, cut], preferred_element_type=jnp.float32)
        spec[1, :, cut] = jnp.dot(raw_ref[...], sin_ref[:, cut], preferred_element_type=jnp.float32)

    def combine(rows, terms):
        real = imag = None
        for frame, column in terms:
            here = pl.ds(pl.multiple_of(frame * slab + rows, GROUP), GROUP)
            cosine_sum = spec[0, here, :]
            sine_sum = spec[1, here, :]
            weights = coef_ref[pl.ds(pl.multiple_of(rows, GROUP), GROUP), :]
            weight_re = weights[:, column : column + 1]
            weight_im = weights[:, column + 1 : column + 2]
            add_re = weight_re * cosine_sum + weight_im * sine_sum
            add_im = weight_im * cosine_sum - weight_re * sine_sum
            real = add_re if real is None else real + add_re
            imag = add_im if imag is None else imag + add_im
        return real, imag

    def store(band, rows, real, imag):
        for part, value in enumerate((real, imag)):
            value = value.astype(jnp.bfloat16)
            here = pl.ds(pl.multiple_of(part * slab + rows, GROUP), GROUP)
            for cut in range(4):
                out_ref[cut // 2, cut % 2, band, here, :] = value[
                    :, cut * quarter : (cut + 1) * quarter
                ]

    @pl.loop(0, slab // GROUP)
    def _(step):
        rows = step * GROUP
        terms = [(frame, 2 * frame) for frame in range(frames)]
        real, imag = combine(rows, terms)
        store(0, rows, real, imag)
        band = 0
        for which in range(angles):
            for multiple in range(1, len(MULTIPLES)):
                band += 1
                column = 2 * (frames + (band - 1) * phases)
                terms = [(which * phases + j, column + 2 * j) for j in range(phases)]
                real, imag = combine(rows, terms)
                shift = shift_ref[band]
                store(band, rows, pltpu.roll(real, shift, 1), pltpu.roll(imag, shift, 1))


def numer_kernel(
    slab, bands, angles, with_power, place_ref, row_ref, col_ref, pow_ref, own_ref, other_ref,
    lhs_ref, *rest
):
    pieces = rest[: len(rest) - (4 if with_power else 3)]
    rest = rest[len(pieces) :]
    out_ref = rest[0]
    power_ref = rest[1] if with_power else None
    wide, total = rest[-2:]
    pixels = lhs_ref.shape[1]
    lane_tiles = pixels // LANES
    extra = wide.shape[1] - pixels
    width = own_ref.shape[-1]
    tile = extra

    for index, piece in enumerate(pieces):
        start = pl.multiple_of(place_ref[index] * slab, slab)
        for lane in range(lane_tiles):
            wide[lane, pl.ds(start, slab), :] = piece[:, lane * LANES : (lane + 1) * LANES].astype(
                jnp.float32
            )
    for lane in range(lane_tiles):
        wide[lane, pixels : pixels + extra, :] = wide[lane, 0:extra, :]

    total[...] = jnp.zeros_like(total)

    def response(q0, band, column, count):
        start = (q0 + row_ref[band]) & (pixels - 1)
        rest_lanes = column & (LANES - 1)
        first = column // LANES
        turn = (LANES - rest_lanes) & (LANES - 1)
        lane = lax.broadcasted_iota(jnp.int32, (tile, LANES), 1)
        turned = [
            pltpu.roll(wide[(first + i) & (lane_tiles - 1), pl.ds(start, tile), :], turn, 1)
            for i in range(count + 1)
        ]
        return [
            jnp.where(lane < LANES - rest_lanes, turned[i], turned[i + 1]) for i in range(count)
        ]

    half = place_ref[len(pieces)]
    tiles = width // LANES

    @pl.loop(0, bands)
    def _(band):
        right = jnp.concatenate([own_ref[half, band], other_ref[0, band]], axis=0)

        @pl.loop(0, pixels // tile)
        def _(step):
            q0 = pl.multiple_of(step * tile, tile)
            weights = response(q0, band, col_ref[band], tiles)
            for part in range(2):
                product = jnp.dot(
                    lhs_ref[part, pl.ds(q0, tile), :], right, preferred_element_type=jnp.float32
                )
                for i in range(tiles):
                    total[part, pl.ds(q0, tile), i * LANES : (i + 1) * LANES] += (
                        weights[i] * product[:, i * LANES : (i + 1) * LANES]
                    )

    blocks = out_ref.shape[0]
    columns = width // blocks

    @pl.loop(0, pixels // tile)
    def _(step):
        q0 = pl.multiple_of(step * tile, tile)
        for block in range(blocks):
            cut = slice(block * columns, (block + 1) * columns)
            out_ref[block, pl.ds(q0, tile), :] = jnp.concatenate(
                [total[0, pl.ds(q0, tile), cut], total[1, pl.ds(q0, tile), cut]], axis=1
            ).astype(jnp.bfloat16)
        if with_power:
            gathered = None
            for band in range(bands):
                value = response(q0, band, pow_ref[band], 1)[0]
                value = value * value
                if band == 0:
                    gathered = value * float(angles)
                else:
                    gathered = gathered + value
            power_ref[pl.ds(q0, tile), :] = jnp.concatenate(
                [gathered[:, :columns], gathered[:, :columns]], axis=1
            )


def smem():
    return pl.BlockSpec(memory_space=pltpu.SMEM)


def vmem():
    return pl.BlockSpec(memory_space=pltpu.VMEM)


def swap(value, axis, mask):
    size = lax.axis_size(axis)
    return lax.ppermute(value, axis, [(i, i ^ mask) for i in range(size)])


def shards(raw, otf, offsets, phase_order, unmix):
    pixels = raw.shape[-1]
    slab = raw.shape[3]
    angles, phases = raw.shape[1:3]
    devices = lax.axis_size("row")
    index = lax.axis_index("row")
    slices = raw.shape[0] * lax.axis_size("cuts")
    chips = devices // 2
    levels = chips.bit_length() - 1
    core = index & 1
    chip = index >> 1
    columns = pixels // devices
    frames = angles * phases
    steps = len(MULTIPLES) - 1
    bands = 1 + angles * steps
    place = sum(((chip >> bit) & 1) << (levels - 1 - bit) for bit in range(levels))

    mine = otf.reshape(slab, pixels).astype(jnp.bfloat16)
    pieces = {0: mine}
    for mask in range(4, devices, 4):
        pieces[mask] = swap(mine, "row", mask)
    for mask in range(0, devices, 4):
        pieces[mask | 2] = swap(pieces[mask], "row", 2)
    for mask in range(0, devices, 2):
        pieces[mask | 1] = swap(pieces[mask], "row", 1)

    cosine, sine = tables(pixels)
    mix_re, mix_im = mixing(unmix, phase_order)
    factors = jnp.array(MULTIPLES[1:], dtype=jnp.int32)
    row_shift = (factors[None, :] * offsets[:, 0:1]).reshape(-1)
    col_shift = (factors[None, :] * offsets[:, 1:2]).reshape(-1)
    zero = jnp.zeros((1,), jnp.int32)
    row_all = jnp.concatenate([zero, row_shift])
    col_all = jnp.concatenate([zero, col_shift])

    def own_rows(which):
        return which * slab + jnp.arange(slab, dtype=jnp.int32)

    turn = (own_rows(index)[:, None] * row_shift[None, :]) & (pixels - 1)
    turn = turn.astype(jnp.float32) * (2.0 * math.pi / pixels)
    turn_re = jnp.cos(turn)[:, :, None]
    turn_im = jnp.sin(turn)[:, :, None]
    rest_re = mix_re[:, 1:].reshape(1, bands - 1, phases)
    rest_im = mix_im[:, 1:].reshape(1, bands - 1, phases)
    coef_re = (rest_re * turn_re - rest_im * turn_im).reshape(slab, -1)
    coef_im = (rest_re * turn_im + rest_im * turn_re).reshape(slab, -1)
    plain_re = jnp.broadcast_to(mix_re[:, 0].reshape(1, frames), (slab, frames))
    plain_im = jnp.broadcast_to(mix_im[:, 0].reshape(1, frames), (slab, frames))
    coef = jnp.stack(
        [
            jnp.concatenate([plain_re, coef_re], axis=1),
            jnp.concatenate([plain_im, coef_im], axis=1),
        ],
        axis=2,
    ).reshape(slab, -1)

    quarter = pixels // 4
    band_flops = 2 * frames * slab * pixels * 2 * pixels
    packed = pl.pallas_call(
        functools.partial(band_kernel, angles, phases),
        out_shape=jax.ShapeDtypeStruct((2, 2, bands, 2 * slab, quarter), jnp.bfloat16),
        in_specs=[smem(), vmem(), vmem(), vmem(), vmem()],
        out_specs=vmem(),
        scratch_shapes=[pltpu.VMEM((2, frames * slab, pixels), jnp.float32)],
        cost_estimate=pl.CostEstimate(
            flops=2 * band_flops, bytes_accessed=12 << 20, transcendentals=0
        ),
        name="bands",
    )(col_all & (pixels - 1), raw.reshape(frames * slab, pixels), cosine, sine, coef)

    near = chip & 1
    here = lax.dynamic_index_in_dim(packed, core, 0, keepdims=False)
    there = lax.dynamic_index_in_dim(packed, 1 - core, 0, keepdims=False)
    got = [
        swap(lax.dynamic_slice_in_dim(there, half, 1, 0), "row", 1) for half in (1 - near, near)
    ]

    def table_rows(which):
        cut = which * slab
        return (
            lax.dynamic_slice_in_dim(cosine, cut, slab, 0),
            lax.dynamic_slice_in_dim(sine, cut, slab, 0),
        )

    cos_own, sin_own = table_rows(index)
    cos_other, sin_other = table_rows(index ^ 1)
    left = jnp.stack(
        [
            jnp.concatenate([cos_own, sin_own, cos_other, sin_other], axis=0).T,
            jnp.concatenate([-sin_own, cos_own, -sin_other, cos_other], axis=0).T,
        ]
    )
    masks = sorted(pieces)
    tile = 128

    def partial(half, other, with_power):
        start = core * (pixels // 2) + half * quarter
        places = jnp.stack([index ^ mask for mask in masks] + [half])
        row_base = (-row_all) & (pixels - 1)
        col_base = (start - col_all) & (pixels - 1)
        own_start = core * (pixels // 2) + place * columns
        pow_base = (own_start - col_all) & (pixels - 1)
        out_shape = [jax.ShapeDtypeStruct((chips // 2, pixels, 2 * columns), jnp.bfloat16)]
        if with_power:
            out_shape.append(jax.ShapeDtypeStruct((pixels, 2 * columns), jnp.float32))
        return pl.pallas_call(
            functools.partial(numer_kernel, slab, bands, angles, with_power),
            out_shape=out_shape,
            in_specs=[smem()] * 4 + [vmem()] * (3 + len(masks)),
            out_specs=[vmem()] * len(out_shape),
            scratch_shapes=[
                pltpu.VMEM((pixels // LANES, pixels + tile, LANES), jnp.float32),
                pltpu.VMEM((2, pixels, quarter), jnp.float32),
            ],
            cost_estimate=pl.CostEstimate(
                flops=16 * bands * slab * pixels * quarter, bytes_accessed=8 << 20, transcendentals=0
            ),
            name="own" if with_power else "away",
        )(places, row_base, col_base, pow_base, here, other, left, *[pieces[m] for m in masks])

    (away,) = partial(1 - near, got[0], False)
    kept, power = partial(near, got[1], True)

    def split(blocks, bit):
        count = blocks.shape[0] // 2
        side = (chip >> bit) & 1
        return (
            lax.dynamic_slice_in_dim(blocks, (1 - side) * count, count, 0),
            lax.dynamic_slice_in_dim(blocks, side * count, count, 0),
        )

    def widen(value):
        return value.astype(jnp.float32)

    far, stay = [swap(part, "row", 2) for part in split(away, 1)]
    kept_far, kept_stay = split(kept, 1)
    far = widen(far) + widen(kept_far)
    stay = widen(stay) + widen(kept_stay)
    for bit in range(1, levels):
        got_next = swap(far.astype(jnp.bfloat16), "row", 2 << bit)
        stay = stay + widen(got_next)
        if bit < levels - 1:
            far, stay = split(stay, bit + 1)
    numer = stay[0]

    total_power = power
    moving = power
    cuts = lax.axis_size("cuts")
    for _ in range(cuts - 1):
        moving = lax.ppermute(moving, "cuts", [(i, (i + 1) % cuts) for i in range(cuts)])
        total_power = total_power + moving
    denom = WIENER + total_power / (slices * angles)
    ratio = (numer / denom).astype(jnp.bfloat16)

    by_cos = jnp.dot(cosine, ratio, preferred_element_type=jnp.float32)
    by_sin = jnp.dot(sine, ratio, preferred_element_type=jnp.float32)
    half = jnp.concatenate(
        [
            by_cos[:, :columns] - by_sin[:, columns:],
            by_cos[:, columns:] + by_sin[:, :columns],
        ],
        axis=1,
    ).astype(jnp.bfloat16)
    back = lax.all_to_all(
        half.reshape(devices, slab, 2 * columns), "row", split_axis=0, concat_axis=0, tiled=True
    )
    back = jnp.swapaxes(back, 0, 1).reshape(slab, devices * 2 * columns)

    def by_owner(table):
        table = table.reshape((2,) + (2,) * levels + (columns, pixels))
        order = tuple(range(levels, 0, -1)) + (0, levels + 1, levels + 2)
        return jnp.transpose(table, order).reshape(devices, columns, pixels)

    final = jnp.concatenate([by_owner(cosine), -by_owner(sine)], axis=1).reshape(-1, pixels)
    recon = jnp.dot(back, final, preferred_element_type=jnp.float32)
    return recon.reshape(otf.shape)


def solution(mesh):
    in_specs = (P("cuts", None, None, "row", None), P("cuts", "row", None), P(), P(), P())
    out_specs = P("cuts", "row", None)
    return jax.shard_map(shards, mesh=mesh, in_specs=in_specs, out_specs=out_specs, check_vma=False)
```

```python
import functools
import math

import jax
import jax.numpy as jnp
import numpy as np
from jax import lax
from jax.experimental import pallas as pl
from jax.experimental.pallas import tpu as pltpu
from jax.sharding import PartitionSpec as P


MULTIPLES = (0, 1, -1, 2, -2)
WIENER = 0.1
LANES = 128
GROUP = 16


def factors_of(pixels):
    rows = np.arange(pixels)[:, None]

    def angle(columns):
        return (rows * columns[None, :] % pixels) * (2.0 * math.pi / pixels)

    high = angle(np.arange(pixels // LANES) * LANES)
    low = angle(np.arange(LANES))
    factor = 1.0 / math.sqrt(pixels)
    return (
        jnp.asarray(np.concatenate([np.cos(high), np.sin(high)], axis=1) * factor, jnp.float32),
        jnp.asarray(np.stack([np.cos(low), np.sin(low)]), jnp.float32),
    )


def mixing(unmix, phase_order):
    phases = unmix.shape[-1]
    onehot = (phase_order[:, :, None] == jnp.arange(phases, dtype=jnp.int32)[None, None, :]).astype(
        jnp.float32
    )
    mixed = jnp.sum(unmix[:, :, :, None, :] * onehot[None, :, None, :, :], axis=-1)
    return (mixed[0], mixed[1])


def band_kernel(
    angles, phases, shift_ref, base_ref, raw_ref, high_ref, low_ref, coef_ref, *rest
):
    outs = rest[:4]
    cos_ref, sin_ref, spec, turned = rest[4:]
    frames = angles * phases
    slab = outs[0].shape[1] // 2
    pixels = raw_ref.shape[1]
    lane_tiles = pixels // LANES
    tile = 256

    @pl.loop(0, pixels // LANES)
    def _(step):
        rows = pl.ds(pl.multiple_of(step * LANES, LANES), LANES)
        low_cos = low_ref[0, rows, :]
        low_sin = low_ref[1, rows, :]
        high = high_ref[rows, :]
        for index in range(lane_tiles):
            cut = slice(index * LANES, (index + 1) * LANES)
            high_cos = high[:, index : index + 1]
            high_sin = high[:, lane_tiles + index : lane_tiles + index + 1]
            cos_ref[rows, cut] = (high_cos * low_cos - high_sin * low_sin).astype(jnp.bfloat16)
            sin_ref[rows, cut] = (high_sin * low_cos + high_cos * low_sin).astype(jnp.bfloat16)

    @pl.loop(0, pixels // tile)
    def _(step):
        cut = pl.ds(pl.multiple_of(step * tile, tile), tile)
        spec[0, :, cut] = jnp.dot(raw_ref[...], cos_ref[:, cut], preferred_element_type=jnp.float32)
        spec[1, :, cut] = jnp.dot(raw_ref[...], sin_ref[:, cut], preferred_element_type=jnp.float32)

    lane = lax.broadcasted_iota(jnp.int32, (GROUP, LANES), 1)

    @pl.loop(0, slab // GROUP)
    def _(step):
        rows = step * GROUP
        weights = coef_ref[pl.ds(pl.multiple_of(rows, GROUP), GROUP), :]

        def combine(band, terms):
            pairs = []
            for frame, column in terms:
                here = pl.ds(pl.multiple_of(frame * slab + rows, GROUP), GROUP)
                weight_re = jnp.broadcast_to(weights[:, column : column + 1], (GROUP, LANES))
                weight_im = jnp.broadcast_to(weights[:, column + 1 : column + 2], (GROUP, LANES))
                pairs.append((here, weight_re, weight_im))
            for index in range(lane_tiles):
                cut = slice(index * LANES, (index + 1) * LANES)
                real = imag = None
                for here, weight_re, weight_im in pairs:
                    cosine_sum = spec[0, here, cut]
                    sine_sum = spec[1, here, cut]
                    add_re = weight_re * cosine_sum + weight_im * sine_sum
                    add_im = weight_im * cosine_sum - weight_re * sine_sum
                    real = add_re if real is None else real + add_re
                    imag = add_im if imag is None else imag + add_im
                turned[band & 1, 0, index] = real
                turned[band & 1, 1, index] = imag
            move = (-shift_ref[band]) & (pixels - 1)
            rest_lanes = move & (LANES - 1)
            turn = (LANES - rest_lanes) & (LANES - 1)
            for which, out in enumerate(outs):
                first = base_ref[which] + move // LANES
                count = out.shape[2] // LANES
                for part in range(2):
                    tiles = [
                        pltpu.roll(
                            turned[band & 1, part, (first + i) & (lane_tiles - 1)], turn, 1
                        )
                        for i in range(count + 1)
                    ]
                    put = pl.ds(pl.multiple_of(part * slab + rows, GROUP), GROUP)
                    for i in range(count):
                        out[band, put, i * LANES : (i + 1) * LANES] = jnp.where(
                            lane < LANES - rest_lanes, tiles[i], tiles[i + 1]
                        ).astype(jnp.bfloat16)

        combine(0, [(frame, 2 * frame) for frame in range(frames)])
        band = 0
        for which in range(angles):
            for _ in MULTIPLES[1:]:
                band += 1
                column = 2 * (frames + (band - 1) * phases)
                combine(band, [(which * phases + j, column + 2 * j) for j in range(phases)])


def numer_kernel(
    slab, bands, angles, columns, with_power, place_ref, row_ref, col_ref, pow_ref, own_ref,
    other_ref, left_ref, near_ref, far_ref, *rest
):
    outs = rest[:2]
    power_ref = rest[2] if with_power else None
    wide, total = rest[-2:]
    lane_tiles = wide.shape[0]
    pixels = lane_tiles * LANES
    tile = wide.shape[1] - pixels
    tiles = own_ref.shape[2] // LANES
    half = tiles // 2
    pieces = near_ref.shape[0]

    for index in range(2 * pieces):
        ref = far_ref if index >= pieces else near_ref
        start = pl.multiple_of(place_ref[index] * slab, slab)
        for lane in range(lane_tiles):
            wide[lane, pl.ds(start, slab), :] = ref[
                index % pieces, :, lane * LANES : (lane + 1) * LANES
            ].astype(jnp.float32)
    for lane in range(lane_tiles):
        wide[lane, pixels : pixels + tile, :] = wide[lane, 0:tile, :]

    lanes = lax.broadcasted_iota(jnp.int32, (tile, LANES), 1)

    def response(q0, band, column, count):
        start = (q0 + row_ref[band]) & (pixels - 1)
        rest_lanes = column & (LANES - 1)
        first = column // LANES
        turn = (LANES - rest_lanes) & (LANES - 1)
        turned = [
            pltpu.roll(wide[(first + i) & (lane_tiles - 1), pl.ds(start, tile), :], turn, 1)
            for i in range(count + 1)
        ]
        return [
            jnp.where(lanes < LANES - rest_lanes, turned[i], turned[i + 1]) for i in range(count)
        ]

    side = place_ref[2 * pieces]

    @pl.loop(0, pixels // tile)
    def _(step):
        q0 = pl.multiple_of(step * tile, tile)
        left = left_ref[step]
        for band in range(bands):
            right = jnp.concatenate([own_ref[band], other_ref[band]], axis=0)
            product = jnp.dot(left, right, preferred_element_type=jnp.float32)
            weights = response(q0, band, col_ref[band], tiles)
            for i in range(tiles):
                cut = slice(i * LANES, (i + 1) * LANES)
                for part in range(2):
                    value = weights[i] * product[part * tile : (part + 1) * tile, cut]
                    if band == 0:
                        total[i, part] = value
                    else:
                        total[i, part] += value
        for which, out in enumerate(outs):
            first = (side if which == 1 else 1 - side) * half
            per_tile = LANES // columns
            for i in range(half):
                real = total[first + i, 0]
                imag = total[first + i, 1]
                for j in range(per_tile):
                    cut = slice(j * columns, (j + 1) * columns)
                    out[i * per_tile + j, pl.ds(q0, tile), :] = jnp.concatenate(
                        [real[:, cut], imag[:, cut]], axis=1
                    ).astype(jnp.bfloat16)
        if with_power:
            gathered = None
            for band in range(bands):
                value = response(q0, band, pow_ref[band], 1)[0]
                value = value * value
                if band == 0:
                    gathered = value * float(angles)
                else:
                    gathered = gathered + value
            power_ref[pl.ds(q0, tile), :] = jnp.concatenate(
                [gathered[:, :columns], gathered[:, :columns]], axis=1
            )


def image_kernel(back_ref, cos_ref, sin_ref, out_ref):
    devices, _, twice = back_ref.shape
    columns = twice // 2
    chips = devices // 2
    levels = chips.bit_length() - 1
    pixels = out_ref.shape[1]
    total = None
    for chip in range(chips):
        place = sum(((chip >> bit) & 1) << (levels - 1 - bit) for bit in range(levels))
        rows = []
        for core in range(2):
            start = core * (pixels // 2) + place * columns
            rows += [cos_ref[start : start + columns, :], sin_ref[start : start + columns, :]]
        left = jnp.concatenate([back_ref[2 * chip], back_ref[2 * chip + 1]], axis=1)
        value = jnp.dot(left, jnp.concatenate(rows, axis=0), preferred_element_type=jnp.float32)
        total = value if total is None else total + value
    out_ref[...] = total


def smem():
    return pl.BlockSpec(memory_space=pltpu.SMEM)


def vmem():
    return pl.BlockSpec(memory_space=pltpu.VMEM)


def swap(value, axis, mask):
    size = lax.axis_size(axis)
    return lax.ppermute(value, axis, [(i, i ^ mask) for i in range(size)])


def shards(raw, otf, offsets, phase_order, unmix):
    pixels = raw.shape[-1]
    slab = raw.shape[3]
    angles, phases = raw.shape[1:3]
    devices = lax.axis_size("row")
    index = lax.axis_index("row")
    slices = raw.shape[0] * lax.axis_size("cuts")
    chips = devices // 2
    levels = chips.bit_length() - 1
    core = index & 1
    chip = index >> 1
    columns = pixels // devices
    frames = angles * phases
    steps = len(MULTIPLES) - 1
    bands = 1 + angles * steps
    place = sum(((chip >> bit) & 1) << (levels - 1 - bit) for bit in range(levels))

    mine = otf.reshape(slab, pixels).astype(jnp.bfloat16)
    across = swap(mine, "row", 2)
    far = [swap(mine, "row", mask) for mask in range(4, devices, 4)]

    mix_re, mix_im = mixing(unmix, phase_order)
    factors = jnp.array(MULTIPLES[1:], dtype=jnp.int32)
    row_shift = (factors[None, :] * offsets[:, 0:1]).reshape(-1)
    col_shift = (factors[None, :] * offsets[:, 1:2]).reshape(-1)
    zero = jnp.zeros((1,), jnp.int32)
    row_all = jnp.concatenate([zero, row_shift])
    col_all = jnp.concatenate([zero, col_shift])

    def own_rows(which):
        return which * slab + jnp.arange(slab, dtype=jnp.int32)

    turn = (own_rows(index)[:, None] * row_shift[None, :]) & (pixels - 1)
    turn = turn.astype(jnp.float32) * (2.0 * math.pi / pixels)
    turn_re = jnp.cos(turn)[:, :, None]
    turn_im = jnp.sin(turn)[:, :, None]
    rest_re = mix_re[:, 1:].reshape(1, bands - 1, phases)
    rest_im = mix_im[:, 1:].reshape(1, bands - 1, phases)
    coef_re = (rest_re * turn_re - rest_im * turn_im).reshape(slab, -1)
    coef_im = (rest_re * turn_im + rest_im * turn_re).reshape(slab, -1)
    plain_re = jnp.broadcast_to(mix_re[:, 0].reshape(1, frames), (slab, frames))
    plain_im = jnp.broadcast_to(mix_im[:, 0].reshape(1, frames), (slab, frames))
    coef = jnp.stack(
        [
            jnp.concatenate([plain_re, coef_re], axis=1),
            jnp.concatenate([plain_im, coef_im], axis=1),
        ],
        axis=2,
    ).reshape(slab, -1)

    quarter = pixels // 4
    near = chip & 1
    half_tiles = quarter // LANES
    base = jnp.stack(
        [(2 * c + h) * half_tiles for c in (1 - core, core) for h in (1 - near, near)]
    )
    high, low = factors_of(pixels)
    table = jax.ShapeDtypeStruct((pixels, pixels), jnp.bfloat16)
    send_away, send_near, keep_away, keep_near, cosine, sine = pl.pallas_call(
        functools.partial(band_kernel, angles, phases),
        out_shape=[jax.ShapeDtypeStruct((bands, 2 * slab, quarter), jnp.bfloat16)] * 4
        + [table] * 2,
        in_specs=[smem(), smem(), vmem(), vmem(), vmem(), vmem()],
        out_specs=[vmem()] * 6,
        scratch_shapes=[
            pltpu.VMEM((2, frames * slab, pixels), jnp.float32),
            pltpu.VMEM((2, 2, pixels // LANES, GROUP, LANES), jnp.float32),
        ],
        cost_estimate=pl.CostEstimate(
            flops=8 * frames * slab * pixels * pixels,
            bytes_accessed=12 << 20,
            transcendentals=0,
        ),
        name="bands",
    )(col_all & (pixels - 1), base, raw.reshape(frames * slab, pixels), high, low, coef)

    got_away = swap(send_away, "row", 1)
    first_half = jnp.stack([mine] + far)
    second_half = jnp.concatenate([across[None], swap(jnp.stack(far), "row", 2)])
    own_pieces = jnp.concatenate([first_half, second_half])
    other_pieces = jnp.concatenate([swap(first_half, "row", 1), swap(second_half, "row", 1)])
    got_near = swap(send_near, "row", 1)
    masks = list(range(0, devices, 4)) + list(range(2, devices, 4))
    masks += [mask | 1 for mask in masks]

    def table_rows(which):
        cut = which * slab
        return (
            lax.dynamic_slice_in_dim(cosine, cut, slab, 0),
            lax.dynamic_slice_in_dim(sine, cut, slab, 0),
        )

    tile = 128
    cos_own, sin_own = table_rows(index)
    cos_other, sin_other = table_rows(index ^ 1)
    left = jnp.stack(
        [
            jnp.concatenate([cos_own, sin_own, cos_other, sin_other], axis=0).T,
            jnp.concatenate([-sin_own, cos_own, -sin_other, cos_other], axis=0).T,
        ]
    )
    left = left.reshape(2, pixels // tile, tile, 4 * slab)
    left = jnp.swapaxes(left, 0, 1).reshape(pixels // tile, 2 * tile, 4 * slab)
    row_base = (-row_all) & (pixels - 1)
    pow_base = (core * (pixels // 2) + place * columns - col_all) & (pixels - 1)
    places = jnp.stack([index ^ mask for mask in masks] + [(chip >> 1) & 1])

    def partial(half, own, other, with_power):
        start = core * (pixels // 2) + half * quarter
        col_base = (start - col_all) & (pixels - 1)
        out_shape = [jax.ShapeDtypeStruct((chips // 4, pixels, 2 * columns), jnp.bfloat16)] * 2
        if with_power:
            out_shape = out_shape + [jax.ShapeDtypeStruct((pixels, 2 * columns), jnp.float32)]
        return pl.pallas_call(
            functools.partial(numer_kernel, slab, bands, angles, columns, with_power),
            out_shape=out_shape,
            in_specs=[smem()] * 4 + [vmem()] * 5,
            out_specs=[vmem()] * len(out_shape),
            scratch_shapes=[
                pltpu.VMEM((pixels // LANES, pixels + tile, LANES), jnp.float32),
                pltpu.VMEM((quarter // LANES, 2, tile, LANES), jnp.float32),
            ],
            cost_estimate=pl.CostEstimate(
                flops=16 * bands * slab * pixels * quarter,
                bytes_accessed=8 << 20,
                transcendentals=0,
            ),
        )(places, row_base, col_base, pow_base, own, other, left, own_pieces, other_pieces)

    away_far, away_stay = partial(1 - near, keep_away, got_away, False)
    far, stay = swap(away_far, "row", 2), swap(away_stay, "row", 2)
    kept_far, kept_stay, power = partial(near, keep_near, got_near, True)

    def split(blocks, bit):
        count = blocks.shape[0] // 2
        side = (chip >> bit) & 1
        return (
            lax.dynamic_slice_in_dim(blocks, (1 - side) * count, count, 0),
            lax.dynamic_slice_in_dim(blocks, side * count, count, 0),
        )

    def widen(value):
        return value.astype(jnp.float32)

    far = widen(far) + widen(kept_far)
    stay = widen(stay) + widen(kept_stay)
    for bit in range(1, levels):
        got_next = swap(far.astype(jnp.bfloat16), "row", 2 << bit)
        stay = stay + widen(got_next)
        if bit < levels - 1:
            far, stay = split(stay, bit + 1)
    numer = stay[0]

    total_power = power
    moving = power
    cuts = lax.axis_size("cuts")
    for _ in range(cuts - 1):
        moving = lax.ppermute(moving, "cuts", [(i, (i + 1) % cuts) for i in range(cuts)])
        total_power = total_power + moving
    denom = WIENER + total_power / (slices * angles)
    ratio = (numer / denom).astype(jnp.bfloat16)

    by_cos = jnp.dot(cosine, ratio, preferred_element_type=jnp.float32)
    by_sin = jnp.dot(sine, ratio, preferred_element_type=jnp.float32)
    half = jnp.concatenate(
        [
            by_cos[:, :columns] - by_sin[:, columns:],
            -by_cos[:, columns:] - by_sin[:, :columns],
        ],
        axis=1,
    ).astype(jnp.bfloat16)
    back = lax.all_to_all(
        half.reshape(devices, slab, 2 * columns), "row", split_axis=0, concat_axis=0, tiled=True
    )
    recon = pl.pallas_call(
        image_kernel,
        out_shape=jax.ShapeDtypeStruct((slab, pixels), jnp.float32),
        in_specs=[vmem()] * 3,
        out_specs=vmem(),
        cost_estimate=pl.CostEstimate(
            flops=4 * slab * pixels * pixels, bytes_accessed=6 << 20, transcendentals=0
        ),
        name="image",
    )(back, cosine, sine)
    return recon.reshape(otf.shape)


def solution(mesh):
    in_specs = (P("cuts", None, None, "row", None), P("cuts", "row", None), P(), P(), P())
    out_specs = P("cuts", "row", None)

    return jax.shard_map(shards, mesh=mesh, in_specs=in_specs, out_specs=out_specs, check_vma=False)
```

```python
import functools
import math

import jax
import jax.numpy as jnp
import numpy as np
from jax import lax
from jax.experimental import pallas as pl
from jax.experimental.pallas import tpu as pltpu
from jax.sharding import PartitionSpec as P


MULTIPLES = (0, 1, -1, 2, -2)
WIENER = 0.1
LANES = 128
GROUP = 16


def factors_of(pixels):
    rows = np.arange(pixels)[:, None]

    def angle(columns):
        return (rows * columns[None, :] % pixels) * (2.0 * math.pi / pixels)

    high = angle(np.arange(pixels // LANES) * LANES)
    low = angle(np.arange(LANES))
    factor = 1.0 / math.sqrt(pixels)
    return (
        jnp.asarray(np.concatenate([np.cos(high), np.sin(high)], axis=1) * factor, jnp.float32),
        jnp.asarray(np.stack([np.cos(low), np.sin(low)]), jnp.float32),
    )


def turn_of(angle):
    square = angle * angle
    cosine = jnp.zeros_like(angle)
    sine = jnp.zeros_like(angle)
    for order in range(9, -1, -1):
        sign = -1.0 if order % 2 else 1.0
        cosine = cosine * square + sign / math.factorial(2 * order)
        sine = sine * square + sign / math.factorial(2 * order + 1)
    return cosine, sine * angle


def band_kernel(
    angles, phases, index_ref, unmix_ref, order_ref, offset_ref, raw_hbm, high_ref, low_ref, *rest
):
    outs = rest[:4]
    cos_hbm, sin_hbm, left_hbm = rest[4:7]
    parts = rest[7:11]
    raw_ref, cos_ref, sin_ref, left_ref, spec, turned, phase, sems, row_sems = rest[11:]
    frames = angles * phases
    slab = raw_ref.shape[0] // frames
    pixels = raw_ref.shape[1]
    lane_tiles = pixels // LANES
    tile = 256
    others = len(MULTIPLES) - 1
    index = index_ref[0]
    core = index & 1
    chip = index >> 1
    near = chip & 1
    pair = 2 * slab

    fetch = pltpu.make_async_copy(raw_hbm, raw_ref, sems.at[0])
    fetch.start()

    @pl.loop(0, pixels // LANES)
    def _(step):
        rows = pl.ds(pl.multiple_of(step * LANES, LANES), LANES)
        low_cos = low_ref[0, rows, :]
        low_sin = low_ref[1, rows, :]
        high = high_ref[rows, :]
        for tab in range(lane_tiles):
            cut = slice(tab * LANES, (tab + 1) * LANES)
            high_cos = high[:, tab : tab + 1]
            high_sin = high[:, lane_tiles + tab : lane_tiles + tab + 1]
            cos_ref[rows, cut] = (high_cos * low_cos - high_sin * low_sin).astype(jnp.bfloat16)
            sin_ref[rows, cut] = (high_sin * low_cos + high_cos * low_sin).astype(jnp.bfloat16)
        first = pl.multiple_of(chip * pair // LANES * LANES, LANES)
        mine = []
        for ref in (cos_ref, sin_ref):
            value = ref[rows, pl.ds(first, LANES)]
            if pair < LANES:
                turn = (LANES - (chip * pair & (LANES - 1))) & (LANES - 1)
                value = pltpu.roll(value.astype(jnp.float32), turn, 1)[:, :pair]
                value = value.astype(jnp.bfloat16)
            mine.append(value)
        left_ref[step, 0:LANES, 0:pair] = mine[0]
        left_ref[step, 0:LANES, pair:] = mine[1]
        left_ref[step, LANES:, 0:pair] = -mine[1]
        left_ref[step, LANES:, pair:] = mine[0]

    keep = [
        pltpu.make_async_copy(cos_ref, cos_hbm, sems.at[1]),
        pltpu.make_async_copy(sin_ref, sin_hbm, sems.at[2]),
        pltpu.make_async_copy(left_ref, left_hbm, sems.at[3]),
    ]
    for copy in keep:
        copy.start()
    fetch.wait()

    @pl.loop(0, pixels // tile)
    def _(step):
        cut = pl.ds(pl.multiple_of(step * tile, tile), tile)
        spec[0, :, cut] = jnp.dot(raw_ref[...], cos_ref[:, cut], preferred_element_type=jnp.float32)
        spec[1, :, cut] = jnp.dot(raw_ref[...], sin_ref[:, cut], preferred_element_type=jnp.float32)

    image_row = index * slab + lax.broadcasted_iota(jnp.int32, (slab, LANES), 0)
    for which in range(angles):
        for m in range(1, others + 1):
            shift = MULTIPLES[m] * offset_ref[which, 0]
            around = ((image_row * shift + pixels // 2) & (pixels - 1)) - pixels // 2
            cosine, sine = turn_of(around.astype(jnp.float32) * (2.0 * math.pi / pixels))
            phase[which * others + m - 1, 0] = cosine
            phase[which * others + m - 1, 1] = sine

    lane = lax.broadcasted_iota(jnp.int32, (GROUP, LANES), 1)
    quarter_tiles = lane_tiles // 4

    def weight(which, m, j):
        column = order_ref[which, j]
        return unmix_ref[0, which, m, column], unmix_ref[1, which, m, column]

    def combine(terms, rows, slot):
        for tab in range(lane_tiles):
            cut = slice(tab * LANES, (tab + 1) * LANES)
            real = imag = None
            for frame, weight_re, weight_im in terms:
                here = pl.ds(pl.multiple_of(frame * slab + rows, GROUP), GROUP)
                cosine_sum = spec[0, here, cut]
                sine_sum = spec[1, here, cut]
                add_re = weight_re * cosine_sum + weight_im * sine_sum
                add_im = weight_im * cosine_sum - weight_re * sine_sum
                real = add_re if real is None else real + add_re
                imag = add_im if imag is None else imag + add_im
            turned[slot, 0, tab] = real
            turned[slot, 1, tab] = imag

    def put_out(band, rows, slot, shift):
        move = (-shift) & (pixels - 1)
        rest_lanes = move & (LANES - 1)
        turn = (LANES - rest_lanes) & (LANES - 1)
        for which, out in enumerate(parts):
            side = (1 - core) if which < 2 else core
            half = (1 - near) if which % 2 == 0 else near
            first = (2 * side + half) * quarter_tiles + move // LANES
            for part in range(2):
                tiles = [
                    pltpu.roll(turned[slot, part, (first + i) & (lane_tiles - 1)], turn, 1)
                    for i in range(quarter_tiles + 1)
                ]
                put = pl.ds(pl.multiple_of(part * slab + rows, GROUP), GROUP)
                for i in range(quarter_tiles):
                    out[band, put, i * LANES : (i + 1) * LANES] = jnp.where(
                        lane < LANES - rest_lanes, tiles[i], tiles[i + 1]
                    ).astype(jnp.bfloat16)

    def copies(step):
        done = []
        for which in range(4):
            for part in range(2):
                put = pl.ds(pl.multiple_of(part * slab + step * GROUP, GROUP), GROUP)
                done.append(
                    pltpu.make_async_copy(
                        parts[which].at[:, put, :],
                        outs[which].at[:, put, :],
                        row_sems.at[step, 2 * which + part],
                    )
                )
        return done

    @pl.loop(0, slab // GROUP)
    def _(step):
        rows = step * GROUP
        terms = [
            (which * phases + j, *weight(which, 0, j))
            for which in range(angles)
            for j in range(phases)
        ]
        combine(terms, rows, 0)
        put_out(0, rows, 0, 0)

        @pl.loop(0, angles * others)
        def _(band):
            which = band // others
            m = band - which * others + 1
            mult = jnp.where(m <= 2, 1, 2) * jnp.where(m & 1, 1, -1)
            here = pl.ds(pl.multiple_of(rows, GROUP), GROUP)
            phase_re = phase[band, 0, here, :]
            phase_im = phase[band, 1, here, :]
            terms = []
            for j in range(phases):
                weight_re, weight_im = weight(which, m, j)
                terms.append(
                    (
                        which * phases + j,
                        weight_re * phase_re - weight_im * phase_im,
                        weight_re * phase_im + weight_im * phase_re,
                    )
                )
            combine(terms, rows, 1)
            put_out(band + 1, rows, 1, mult * offset_ref[which, 1])

        for copy in copies(step):
            copy.start()

    for copy in keep:
        copy.wait()

    @pl.loop(0, slab // GROUP)
    def _(step):
        for copy in copies(step):
            copy.wait()


def numer_kernel(
    slab, bands, columns, masks, with_power, index_ref, offset_ref, own_ref, other_ref, left_ref,
    near_ref, far_ref, *rest
):
    outs = rest[:4]
    power_ref = rest[4] if with_power else None
    wide, total, right = rest[-3:]
    lane_tiles = wide.shape[0]
    pixels = lane_tiles * LANES
    tile = wide.shape[1] - pixels
    tiles = own_ref.shape[2] // LANES
    half = tiles // 2
    pieces = near_ref.shape[0]
    others = len(MULTIPLES) - 1
    index = index_ref[0]
    core = index & 1
    chip = index >> 1
    levels = (pixels // columns // 2).bit_length() - 1
    place = sum(((chip >> bit) & 1) << (levels - 1 - bit) for bit in range(levels))
    quarter = (chip & 1) if with_power else 1 - (chip & 1)
    start_column = (2 * core + quarter) * (pixels // 4)
    own_column = core * (pixels // 2) + place * columns

    def shift_of(band, axis):
        if band == 0:
            return 0
        which, m = divmod(band - 1, others)
        return MULTIPLES[m + 1] * offset_ref[which, axis]

    @pl.loop(0, bands)
    def _(band):
        for ref, side in ((own_ref, core), (other_ref, 1 - core)):
            for part in range(2):
                put = pl.ds(pl.multiple_of((2 * part + side) * slab, slab), slab)
                right[band, put, :] = ref[band, part * slab : (part + 1) * slab, :]

    for piece in range(2 * pieces):
        ref = far_ref if piece >= pieces else near_ref
        start = pl.multiple_of((index ^ masks[piece]) * slab, slab)
        for lane in range(lane_tiles):
            wide[lane, pl.ds(start, slab), :] = ref[
                piece % pieces, :, lane * LANES : (lane + 1) * LANES
            ].astype(jnp.float32)
    for lane in range(lane_tiles):
        wide[lane, pixels : pixels + tile, :] = wide[lane, 0:tile, :]

    lanes = lax.broadcasted_iota(jnp.int32, (tile, LANES), 1)

    def response(q0, band, column, count):
        start = (q0 - shift_of(band, 0)) & (pixels - 1)
        column = (column - shift_of(band, 1)) & (pixels - 1)
        rest_lanes = column & (LANES - 1)
        first = column // LANES
        turn = (LANES - rest_lanes) & (LANES - 1)
        turned = [
            pltpu.roll(wide[(first + i) & (lane_tiles - 1), pl.ds(start, tile), :], turn, 1)
            for i in range(count + 1)
        ]
        return [
            jnp.where(lanes < LANES - rest_lanes, turned[i], turned[i + 1]) for i in range(count)
        ]

    side = (chip >> 1) & 1

    def tile_of(step, upper):
        q0 = pl.multiple_of((step + upper * (pixels // tile // 2)) * tile, tile)
        to = pl.ds(pl.multiple_of(step * tile, tile), tile)
        left = left_ref[step + upper * (pixels // tile // 2)]
        for band in range(bands):
            product = jnp.dot(left, right[band], preferred_element_type=jnp.float32)
            weights = response(q0, band, start_column, tiles)
            for i in range(tiles):
                cut = slice(i * LANES, (i + 1) * LANES)
                for part in range(2):
                    value = weights[i] * product[part * tile : (part + 1) * tile, cut]
                    if band == 0:
                        total[i, part] = value
                    else:
                        total[i, part] += value
        for which in range(2):
            out = outs[2 * which + upper]
            first = (side if which == 1 else 1 - side) * half
            per_tile = LANES // columns
            for i in range(half):
                real = total[first + i, 0]
                imag = total[first + i, 1]
                for j in range(per_tile):
                    cut = slice(j * columns, (j + 1) * columns)
                    out[i * per_tile + j, to, :] = jnp.concatenate(
                        [real[:, cut], imag[:, cut]], axis=1
                    ).astype(jnp.bfloat16)
        if with_power:
            gathered = None
            for band in range(bands):
                value = response(q0, band, own_column, 1)[0]
                value = value * value
                if band == 0:
                    gathered = value * float((bands - 1) // others)
                else:
                    gathered = gathered + value
            power_ref[pl.ds(q0, tile), :] = jnp.concatenate(
                [gathered[:, :columns], gathered[:, :columns]], axis=1
            )

    for upper in range(2):
        pl.loop(0, pixels // tile // 2)(functools.partial(tile_of, upper=upper))


def image_kernel(back_ref, cos_ref, sin_ref, out_ref):
    devices, _, twice = back_ref.shape
    columns = twice // 2
    chips = devices // 2
    levels = chips.bit_length() - 1
    pixels = out_ref.shape[1]
    total = None
    for chip in range(chips):
        place = sum(((chip >> bit) & 1) << (levels - 1 - bit) for bit in range(levels))
        rows = []
        for core in range(2):
            start = core * (pixels // 2) + place * columns
            rows += [cos_ref[start : start + columns, :], sin_ref[start : start + columns, :]]
        left = jnp.concatenate([back_ref[2 * chip], back_ref[2 * chip + 1]], axis=1)
        value = jnp.dot(left, jnp.concatenate(rows, axis=0), preferred_element_type=jnp.float32)
        total = value if total is None else total + value
    out_ref[...] = total


def smem():
    return pl.BlockSpec(memory_space=pltpu.SMEM)


def vmem():
    return pl.BlockSpec(memory_space=pltpu.VMEM)


def swap(value, axis, mask):
    size = lax.axis_size(axis)
    return lax.ppermute(value, axis, [(i, i ^ mask) for i in range(size)])


def shards(raw, otf, offsets, phase_order, unmix):
    pixels = raw.shape[-1]
    slab = raw.shape[3]
    angles, phases = raw.shape[1:3]
    devices = lax.axis_size("row")
    index = lax.axis_index("row")
    slices = raw.shape[0] * lax.axis_size("cuts")
    chips = devices // 2
    levels = chips.bit_length() - 1
    chip = index >> 1
    columns = pixels // devices
    frames = angles * phases
    bands = 1 + angles * (len(MULTIPLES) - 1)

    mine = otf.reshape(slab, pixels).astype(jnp.bfloat16)
    masks = list(range(0, devices, 2))
    pieces = [mine] + [swap(mine, "row", mask) for mask in masks[1:]]
    masks += [mask | 1 for mask in masks]

    quarter = pixels // 4
    where = index.astype(jnp.int32).reshape(1)
    high, low = factors_of(pixels)
    table = jax.ShapeDtypeStruct((pixels, pixels), jnp.bfloat16)
    hbm = pl.BlockSpec(memory_space=pl.ANY)
    part = (bands, 2 * slab, quarter)
    left_shape = (pixels // LANES, 2 * LANES, 4 * slab)
    send_away, send_near, keep_away, keep_near, cosine, sine, left = pl.pallas_call(
        functools.partial(band_kernel, angles, phases),
        out_shape=[jax.ShapeDtypeStruct(part, jnp.bfloat16)] * 4
        + [table] * 2
        + [jax.ShapeDtypeStruct(left_shape, jnp.bfloat16)],
        in_specs=[smem()] * 4 + [hbm] + [vmem()] * 2,
        out_specs=[hbm] * 7,
        scratch_shapes=[pltpu.VMEM(part, jnp.bfloat16)] * 4
        + [
            pltpu.VMEM((frames * slab, pixels), jnp.bfloat16),
            pltpu.VMEM((pixels, pixels), jnp.bfloat16),
            pltpu.VMEM((pixels, pixels), jnp.bfloat16),
            pltpu.VMEM(left_shape, jnp.bfloat16),
            pltpu.VMEM((2, frames * slab, pixels), jnp.float32),
            pltpu.VMEM((2, 2, pixels // LANES, GROUP, LANES), jnp.float32),
            pltpu.VMEM((bands - 1, 2, slab, LANES), jnp.float32),
            pltpu.SemaphoreType.DMA((4,)),
            pltpu.SemaphoreType.DMA((slab // GROUP, 8)),
        ],
        cost_estimate=pl.CostEstimate(
            flops=8 * frames * slab * pixels * pixels,
            bytes_accessed=12 << 20,
            transcendentals=0,
        ),
        name="bands",
    )(where, unmix, phase_order, offsets, raw.reshape(frames * slab, pixels), high, low)

    got_away = swap(send_away, "row", 1)
    own_pieces = jnp.stack(pieces)
    other_pieces = swap(own_pieces, "row", 1)
    got_near = swap(send_near, "row", 1)

    def partial(own, other, with_power):
        half_shape = (chips // 4, pixels // 2, 2 * columns)
        out_shape = [jax.ShapeDtypeStruct(half_shape, jnp.bfloat16)] * 4
        if with_power:
            out_shape = out_shape + [jax.ShapeDtypeStruct((pixels, 2 * columns), jnp.float32)]
        return pl.pallas_call(
            functools.partial(numer_kernel, slab, bands, columns, masks, with_power),
            out_shape=out_shape,
            in_specs=[smem()] * 2 + [vmem()] * 5,
            out_specs=[vmem()] * len(out_shape),
            scratch_shapes=[
                pltpu.VMEM((pixels // LANES, pixels + LANES, LANES), jnp.float32),
                pltpu.VMEM((quarter // LANES, 2, LANES, LANES), jnp.float32),
                pltpu.VMEM((bands, 4 * slab, quarter), jnp.bfloat16),
            ],
            cost_estimate=pl.CostEstimate(
                flops=16 * bands * slab * pixels * quarter,
                bytes_accessed=8 << 20,
                transcendentals=0,
            ),
        )(where, offsets, own, other, left, own_pieces, other_pieces)

    away = partial(keep_away, got_away, False)
    moved = [swap(value, "row", 2) for value in away]
    *kept, power = partial(keep_near, got_near, True)

    def split(blocks, bit):
        count = blocks.shape[0] // 2
        side = (chip >> bit) & 1
        return (
            lax.dynamic_slice_in_dim(blocks, (1 - side) * count, count, 0),
            lax.dynamic_slice_in_dim(blocks, side * count, count, 0),
        )

    def widen(value):
        return value.astype(jnp.float32)

    fars = [widen(moved[h]) + widen(kept[h]) for h in range(2)]
    stays = [widen(moved[2 + h]) + widen(kept[2 + h]) for h in range(2)]
    for bit in range(1, levels):
        got_next = [swap(far.astype(jnp.bfloat16), "row", 2 << bit) for far in fars]
        stays = [stay + widen(got) for stay, got in zip(stays, got_next)]
        if bit < levels - 1:
            fars, stays = zip(*[split(stay, bit + 1) for stay in stays])
    numer = jnp.concatenate([stay[0] for stay in stays])

    total_power = power
    moving = power
    cuts = lax.axis_size("cuts")
    for _ in range(cuts - 1):
        moving = lax.ppermute(moving, "cuts", [(i, (i + 1) % cuts) for i in range(cuts)])
        total_power = total_power + moving
    denom = WIENER + total_power / (slices * angles)
    ratio = (numer / denom).astype(jnp.bfloat16)

    by_cos = jnp.dot(cosine, ratio, preferred_element_type=jnp.float32)
    by_sin = jnp.dot(sine, ratio, preferred_element_type=jnp.float32)
    half = jnp.concatenate(
        [
            by_cos[:, :columns] - by_sin[:, columns:],
            -by_cos[:, columns:] - by_sin[:, :columns],
        ],
        axis=1,
    ).astype(jnp.bfloat16)
    back = lax.all_to_all(
        half.reshape(devices, slab, 2 * columns), "row", split_axis=0, concat_axis=0, tiled=True
    )
    recon = pl.pallas_call(
        image_kernel,
        out_shape=jax.ShapeDtypeStruct((slab, pixels), jnp.float32),
        in_specs=[vmem()] * 3,
        out_specs=vmem(),
        cost_estimate=pl.CostEstimate(
            flops=4 * slab * pixels * pixels, bytes_accessed=6 << 20, transcendentals=0
        ),
        name="image",
    )(back, cosine, sine)
    return recon.reshape(otf.shape)


def solution(mesh):
    in_specs = (P("cuts", None, None, "row", None), P("cuts", "row", None), P(), P(), P())
    out_specs = P("cuts", "row", None)

    return jax.shard_map(shards, mesh=mesh, in_specs=in_specs, out_specs=out_specs, check_vma=False)
```

```python
import functools
import math

import jax
import jax.numpy as jnp
from jax import lax
from jax.experimental import pallas as pl
from jax.experimental.pallas import tpu as pltpu
from jax.sharding import PartitionSpec as P


MULTIPLES = (0, 1, -1, 2, -2)
WIENER = 0.1
LANES = 128
GROUP = 16


def turn_of(angle):
    square = angle * angle
    cosine = jnp.zeros_like(angle)
    sine = jnp.zeros_like(angle)
    for order in range(9, -1, -1):
        sign = -1.0 if order % 2 else 1.0
        cosine = cosine * square + sign / math.factorial(2 * order)
        sine = sine * square + sign / math.factorial(2 * order + 1)
    return cosine, sine * angle


def band_kernel(
    angles, phases, index_ref, scalar_ref, raw_hbm, *rest
):
    parts = rest[:4]
    cos_ref, sin_ref, left_ref, raw_ref, low, spec, turned_even, turned_odd, phase, sem = rest[4:]
    frames = angles * phases
    slab = raw_ref.shape[0] // frames
    pixels = raw_ref.shape[1]
    lane_tiles = pixels // LANES
    tile = 256
    others = len(MULTIPLES) - 1
    index = index_ref[0]
    core = index & 1
    chip = index >> 1
    near = chip & 1
    pair = 2 * slab

    def offset(which, axis):
        return scalar_ref[0, which, 0, 2 * phases + axis].astype(jnp.int32)

    fetch = pltpu.make_async_copy(raw_hbm, raw_ref, sem)
    fetch.start()

    column = lax.broadcasted_iota(jnp.int32, (LANES, LANES), 1)
    unit = 2.0 * math.pi / pixels

    @pl.loop(0, pixels // LANES)
    def _(step):
        first = pl.multiple_of(step * LANES, LANES)
        row = first + lax.broadcasted_iota(jnp.int32, (LANES, LANES), 0)
        around = ((row * column + pixels // 2) & (pixels - 1)) - pixels // 2
        low[0, pl.ds(first, LANES), :], low[1, pl.ds(first, LANES), :] = turn_of(
            around.astype(jnp.float32) * unit
        )

    repeat = lax.broadcasted_iota(jnp.int32, (GROUP, LANES), 0)
    factor = 1.0 / math.sqrt(pixels)

    def build(tab):
        around = ((repeat * (tab * LANES) + pixels // 2) & (pixels - 1)) - pixels // 2
        high_cos, high_sin = turn_of(around.astype(jnp.float32) * unit)
        high_cos = high_cos * factor
        high_sin = high_sin * factor
        for first in range(0, pixels, GROUP):
            rows = slice(first, first + GROUP)
            low_cos = low[0, rows, :]
            low_sin = low[1, rows, :]
            cut = slice(tab * LANES, (tab + 1) * LANES)
            cos_ref[rows, cut] = (high_cos * low_cos - high_sin * low_sin).astype(jnp.bfloat16)
            sin_ref[rows, cut] = (high_sin * low_cos + high_cos * low_sin).astype(jnp.bfloat16)

    per_tile = tile // LANES
    for tab in range(per_tile):
        build(tab)
    fetch.wait()
    for step in range(pixels // tile):
        cut = slice(step * tile, (step + 1) * tile)
        spec[0, :, cut] = jnp.dot(raw_ref[...], cos_ref[:, cut], preferred_element_type=jnp.float32)
        spec[1, :, cut] = jnp.dot(raw_ref[...], sin_ref[:, cut], preferred_element_type=jnp.float32)
        if step + 1 < pixels // tile:
            for tab in range(per_tile):
                build((step + 1) * per_tile + tab)

    @pl.loop(0, pixels // LANES)
    def _(step):
        rows = pl.ds(pl.multiple_of(step * LANES, LANES), LANES)
        first = pl.multiple_of(chip * pair // LANES * LANES, LANES)
        mine = []
        for ref in (cos_ref, sin_ref):
            value = ref[rows, pl.ds(first, LANES)]
            if pair < LANES:
                turn = (LANES - (chip * pair & (LANES - 1))) & (LANES - 1)
                value = pltpu.roll(value.astype(jnp.float32), turn, 1)[:, :pair]
                value = value.astype(jnp.bfloat16)
            mine.append(value)
        left_ref[step, 0:LANES, 0:pair] = mine[0]
        left_ref[step, 0:LANES, pair:] = mine[1]
        left_ref[step, LANES:, 0:pair] = -mine[1]
        left_ref[step, LANES:, pair:] = mine[0]

    image_row = index * slab + lax.broadcasted_iota(jnp.int32, (slab, LANES), 0)
    for which in range(angles):
        for m in range(1, others + 1):
            shift = MULTIPLES[m] * offset(which, 0)
            around = ((image_row * shift + pixels // 2) & (pixels - 1)) - pixels // 2
            cosine, sine = turn_of(around.astype(jnp.float32) * (2.0 * math.pi / pixels))
            phase[which * others + m - 1, 0] = cosine
            phase[which * others + m - 1, 1] = sine

    lane = lax.broadcasted_iota(jnp.int32, (GROUP, LANES), 1)
    quarter_tiles = lane_tiles // 4

    def weight(which, m, j):
        column = scalar_ref[0, which, 0, phases + j].astype(jnp.int32)
        return scalar_ref[0, which, m, column], scalar_ref[1, which, m, column]

    def combine(terms, rows, slot):
        for tab in range(lane_tiles):
            cut = slice(tab * LANES, (tab + 1) * LANES)
            real = imag = None
            for frame, weight_re, weight_im in terms:
                here = pl.ds(pl.multiple_of(frame * slab + rows, GROUP), GROUP)
                cosine_sum = spec[0, here, cut]
                sine_sum = spec[1, here, cut]
                add_re = weight_re * cosine_sum + weight_im * sine_sum
                add_im = weight_im * cosine_sum - weight_re * sine_sum
                real = add_re if real is None else real + add_re
                imag = add_im if imag is None else imag + add_im
            slot[0, tab] = real
            slot[1, tab] = imag

    def put_out(band, rows, slot, shift):
        move = (-shift) & (pixels - 1)
        rest_lanes = move & (LANES - 1)
        turn = (LANES - rest_lanes) & (LANES - 1)
        for which, out in enumerate(parts):
            side = (1 - core) if which < 2 else core
            half = (1 - near) if which % 2 == 0 else near
            first = (2 * side + half) * quarter_tiles + move // LANES
            for part in range(2):
                tiles = [
                    pltpu.roll(slot[part, (first + i) & (lane_tiles - 1)], turn, 1)
                    for i in range(quarter_tiles + 1)
                ]
                put = pl.ds(pl.multiple_of(part * slab + rows, GROUP), GROUP)
                for i in range(quarter_tiles):
                    out[band, put, i * LANES : (i + 1) * LANES] = jnp.where(
                        lane < LANES - rest_lanes, tiles[i], tiles[i + 1]
                    ).astype(jnp.bfloat16)

    def terms_of(band, rows):
        which = band // others
        m = band - which * others + 1
        here = pl.ds(pl.multiple_of(rows, GROUP), GROUP)
        phase_re = phase[band, 0, here, :]
        phase_im = phase[band, 1, here, :]
        terms = []
        for j in range(phases):
            weight_re, weight_im = weight(which, m, j)
            terms.append(
                (
                    which * phases + j,
                    weight_re * phase_re - weight_im * phase_im,
                    weight_re * phase_im + weight_im * phase_re,
                )
            )
        return terms

    def shift_of(band):
        other = jnp.maximum(band - 1, 0)
        which = other // others
        m = other - which * others + 1
        mult = jnp.where(m <= 2, 1, 2) * jnp.where(m % 2 == 1, 1, -1)
        return jnp.where(band == 0, 0, mult * offset(which, 1))

    @pl.loop(0, slab // GROUP)
    def _(step):
        rows = step * GROUP
        terms = [
            (which * phases + j, *weight(which, 0, j))
            for which in range(angles)
            for j in range(phases)
        ]
        combine(terms, rows, turned_even)

        @pl.loop(0, angles * others // 2)
        def _(pair_index):
            band = 2 * pair_index
            combine(terms_of(band, rows), rows, turned_odd)
            put_out(band, rows, turned_even, shift_of(band))
            combine(terms_of(band + 1, rows), rows, turned_even)
            put_out(band + 1, rows, turned_odd, shift_of(band + 1))

        put_out(angles * others, rows, turned_even, shift_of(angles * others))


def numer_kernel(
    slab, bands, columns, masks, with_power, index_ref, scalar_ref, own_ref, other_ref, left_ref,
    near_ref, far_ref, *rest
):
    outs = rest[:4]
    power_ref = rest[4] if with_power else None
    wide, total, right = rest[-3:]
    lane_tiles = wide.shape[0]
    pixels = lane_tiles * LANES
    tile = wide.shape[1] - pixels
    tiles = own_ref.shape[2] // LANES
    half = tiles // 2
    pieces = near_ref.shape[0]
    others = len(MULTIPLES) - 1
    index = index_ref[0]
    core = index & 1
    chip = index >> 1
    levels = (pixels // columns // 2).bit_length() - 1
    place = sum(((chip >> bit) & 1) << (levels - 1 - bit) for bit in range(levels))
    quarter = (chip & 1) if with_power else 1 - (chip & 1)
    start_column = (2 * core + quarter) * (pixels // 4)
    own_column = core * (pixels // 2) + place * columns

    def shift_of(band, axis):
        if band == 0:
            return 0
        which, m = divmod(band - 1, others)
        return MULTIPLES[m + 1] * scalar_ref[0, which, 0, scalar_ref.shape[3] - 2 + axis].astype(
            jnp.int32
        )

    @pl.loop(0, bands)
    def _(band):
        for ref, side in ((own_ref, core), (other_ref, 1 - core)):
            for part in range(2):
                put = pl.ds(pl.multiple_of((2 * part + side) * slab, slab), slab)
                right[band, put, :] = ref[band, part * slab : (part + 1) * slab, :]

    for piece in range(2 * pieces):
        ref = far_ref if piece >= pieces else near_ref
        start = pl.multiple_of((index ^ masks[piece]) * slab, slab)
        for lane in range(lane_tiles):
            wide[lane, pl.ds(start, slab), :] = ref[
                piece % pieces, :, lane * LANES : (lane + 1) * LANES
            ].astype(jnp.float32)
    for lane in range(lane_tiles):
        wide[lane, pixels : pixels + tile, :] = wide[lane, 0:tile, :]

    lanes = lax.broadcasted_iota(jnp.int32, (tile, LANES), 1)

    def response(q0, band, column, count):
        start = (q0 - shift_of(band, 0)) & (pixels - 1)
        column = (column - shift_of(band, 1)) & (pixels - 1)
        rest_lanes = column & (LANES - 1)
        first = column // LANES
        turn = (LANES - rest_lanes) & (LANES - 1)
        turned = [
            pltpu.roll(wide[(first + i) & (lane_tiles - 1), pl.ds(start, tile), :], turn, 1)
            for i in range(count + 1)
        ]
        return [
            jnp.where(lanes < LANES - rest_lanes, turned[i], turned[i + 1]) for i in range(count)
        ]

    side = (chip >> 1) & 1

    def tile_of(step, upper):
        q0 = pl.multiple_of((step + upper * (pixels // tile // 2)) * tile, tile)
        to = pl.ds(pl.multiple_of(step * tile, tile), tile)
        left = left_ref[step + upper * (pixels // tile // 2)]
        for band in range(bands):
            product = jnp.dot(left, right[band], preferred_element_type=jnp.float32)
            weights = response(q0, band, start_column, tiles)
            for i in range(tiles):
                cut = slice(i * LANES, (i + 1) * LANES)
                for part in range(2):
                    value = weights[i] * product[part * tile : (part + 1) * tile, cut]
                    if band == 0:
                        total[i, part] = value
                    else:
                        total[i, part] += value
        for which in range(2):
            out = outs[2 * which + upper]
            first = (side if which == 1 else 1 - side) * half
            per_tile = LANES // columns
            for i in range(half):
                real = total[first + i, 0]
                imag = total[first + i, 1]
                for j in range(per_tile):
                    cut = slice(j * columns, (j + 1) * columns)
                    out[i * per_tile + j, to, :] = jnp.concatenate(
                        [real[:, cut], imag[:, cut]], axis=1
                    ).astype(jnp.bfloat16)
        if with_power:
            gathered = None
            for band in range(bands):
                value = response(q0, band, own_column, 1)[0]
                value = value * value
                if band == 0:
                    gathered = value * float((bands - 1) // others)
                else:
                    gathered = gathered + value
            power_ref[pl.ds(q0, tile), :] = jnp.concatenate(
                [gathered[:, :columns], gathered[:, :columns]], axis=1
            )

    for upper in range(2):
        pl.loop(0, pixels // tile // 2)(functools.partial(tile_of, upper=upper))


def pack_kernel(*refs):
    out_ref = refs[-1]
    for index, ref in enumerate(refs[:-1]):
        out_ref[index] = ref[...]


def image_kernel(back_ref, cos_ref, sin_ref, out_ref):
    devices, _, twice = back_ref.shape
    columns = twice // 2
    chips = devices // 2
    levels = chips.bit_length() - 1
    pixels = out_ref.shape[1]
    total = None
    for chip in range(chips):
        place = sum(((chip >> bit) & 1) << (levels - 1 - bit) for bit in range(levels))
        rows = []
        for core in range(2):
            start = core * (pixels // 2) + place * columns
            rows += [cos_ref[start : start + columns, :], sin_ref[start : start + columns, :]]
        left = jnp.concatenate([back_ref[2 * chip], back_ref[2 * chip + 1]], axis=1)
        value = jnp.dot(left, jnp.concatenate(rows, axis=0), preferred_element_type=jnp.float32)
        total = value if total is None else total + value
    out_ref[...] = total


def smem():
    return pl.BlockSpec(memory_space=pltpu.SMEM)


def vmem():
    return pl.BlockSpec(memory_space=pltpu.VMEM)


def swap(value, axis, mask):
    size = lax.axis_size(axis)
    return lax.ppermute(value, axis, [(i, i ^ mask) for i in range(size)])


def shards(raw, otf, offsets, phase_order, unmix):
    pixels = raw.shape[-1]
    slab = raw.shape[3]
    angles, phases = raw.shape[1:3]
    devices = lax.axis_size("row")
    index = lax.axis_index("row")
    slices = raw.shape[0] * lax.axis_size("cuts")
    chips = devices // 2
    levels = chips.bit_length() - 1
    chip = index >> 1
    columns = pixels // devices
    frames = angles * phases
    bands = 1 + angles * (len(MULTIPLES) - 1)

    mine = otf.reshape(slab, pixels).astype(jnp.bfloat16)
    masks = list(range(0, devices, 2))
    pieces = [mine] + [swap(mine, "row", mask) for mask in masks[1:]]
    masks += [mask | 1 for mask in masks]

    quarter = pixels // 4
    where = index.astype(jnp.int32).reshape(1)
    share = unmix.shape[:3]
    scalars = jnp.concatenate(
        [
            unmix,
            jnp.broadcast_to(phase_order.astype(jnp.float32)[None, :, None, :], share + (phases,)),
            jnp.broadcast_to(offsets.astype(jnp.float32)[None, :, None, :], share + (2,)),
        ],
        axis=3,
    )
    table = jax.ShapeDtypeStruct((pixels, pixels), jnp.bfloat16)
    hbm = pl.BlockSpec(memory_space=pl.ANY)
    part = (bands, 2 * slab, quarter)
    left_shape = (pixels // LANES, 2 * LANES, 4 * slab)
    send_away, send_near, keep_away, keep_near, cosine, sine, left = pl.pallas_call(
        functools.partial(band_kernel, angles, phases),
        out_shape=[jax.ShapeDtypeStruct(part, jnp.bfloat16)] * 4
        + [table] * 2
        + [jax.ShapeDtypeStruct(left_shape, jnp.bfloat16)],
        in_specs=[smem()] * 2 + [hbm],
        out_specs=[vmem()] * 7,
        scratch_shapes=[
            pltpu.VMEM((frames * slab, pixels), jnp.bfloat16),
            pltpu.VMEM((2, pixels, LANES), jnp.float32),
            pltpu.VMEM((2, frames * slab, pixels), jnp.float32),
            pltpu.VMEM((2, pixels // LANES, GROUP, LANES), jnp.float32),
            pltpu.VMEM((2, pixels // LANES, GROUP, LANES), jnp.float32),
            pltpu.VMEM((bands - 1, 2, slab, LANES), jnp.float32),
            pltpu.SemaphoreType.DMA,
        ],
        cost_estimate=pl.CostEstimate(
            flops=8 * frames * slab * pixels * pixels,
            bytes_accessed=12 << 20,
            transcendentals=0,
        ),
        compiler_params=pltpu.CompilerParams(vmem_limit_bytes=26 << 20),
        name="bands",
    )(where, scalars, raw.reshape(frames * slab, pixels))

    got_away = swap(send_away, "row", 1)
    own_pieces = pl.pallas_call(
        pack_kernel,
        out_shape=jax.ShapeDtypeStruct((chips, slab, pixels), jnp.bfloat16),
        in_specs=[vmem()] * chips,
        out_specs=vmem(),
        compiler_params=pltpu.CompilerParams(vmem_limit_bytes=8 << 20),
        cost_estimate=pl.CostEstimate(
            flops=chips * slab * pixels, bytes_accessed=2 << 20, transcendentals=0
        ),
        name="pack",
    )(*pieces)
    other_pieces = swap(own_pieces, "row", 1)
    got_near = swap(send_near, "row", 1)

    def partial(own, other, with_power):
        half_shape = (chips // 4, pixels // 2, 2 * columns)
        out_shape = [jax.ShapeDtypeStruct(half_shape, jnp.bfloat16)] * 4
        if with_power:
            out_shape = out_shape + [jax.ShapeDtypeStruct((pixels, 2 * columns), jnp.float32)]
        return pl.pallas_call(
            functools.partial(numer_kernel, slab, bands, columns, masks, with_power),
            out_shape=out_shape,
            in_specs=[smem()] * 2 + [vmem()] * 5,
            out_specs=[vmem()] * len(out_shape),
            scratch_shapes=[
                pltpu.VMEM((pixels // LANES, pixels + LANES, LANES), jnp.float32),
                pltpu.VMEM((quarter // LANES, 2, LANES, LANES), jnp.float32),
                pltpu.VMEM((bands, 4 * slab, quarter), jnp.bfloat16),
            ],
            cost_estimate=pl.CostEstimate(
                flops=16 * bands * slab * pixels * quarter,
                bytes_accessed=8 << 20,
                transcendentals=0,
            ),
            compiler_params=pltpu.CompilerParams(vmem_limit_bytes=16 << 20),
        )(where, scalars, own, other, left, own_pieces, other_pieces)

    away = partial(keep_away, got_away, False)
    moved = [swap(value, "row", 2) for value in away]
    *kept, power = partial(keep_near, got_near, True)

    def split(blocks, bit):
        count = blocks.shape[0] // 2
        side = (chip >> bit) & 1
        return (
            lax.dynamic_slice_in_dim(blocks, (1 - side) * count, count, 0),
            lax.dynamic_slice_in_dim(blocks, side * count, count, 0),
        )

    def widen(value):
        return value.astype(jnp.float32)

    fars = [widen(moved[h]) + widen(kept[h]) for h in range(2)]
    stays = [widen(moved[2 + h]) + widen(kept[2 + h]) for h in range(2)]
    for bit in range(1, levels):
        got_next = [swap(far.astype(jnp.bfloat16), "row", 2 << bit) for far in fars]
        stays = [stay + widen(got) for stay, got in zip(stays, got_next)]
        if bit < levels - 1:
            fars, stays = zip(*[split(stay, bit + 1) for stay in stays])
    numer = jnp.concatenate([stay[0] for stay in stays])

    total_power = power
    moving = power
    cuts = lax.axis_size("cuts")
    for _ in range(cuts - 1):
        moving = lax.ppermute(moving, "cuts", [(i, (i + 1) % cuts) for i in range(cuts)])
        total_power = total_power + moving
    denom = WIENER + total_power / (slices * angles)
    ratio = (numer / denom).astype(jnp.bfloat16)

    by_cos = jnp.dot(cosine, ratio, preferred_element_type=jnp.float32)
    by_sin = jnp.dot(sine, ratio, preferred_element_type=jnp.float32)
    half = jnp.concatenate(
        [
            by_cos[:, :columns] - by_sin[:, columns:],
            -by_cos[:, columns:] - by_sin[:, :columns],
        ],
        axis=1,
    ).astype(jnp.bfloat16)
    back = lax.all_to_all(
        half.reshape(devices, slab, 2 * columns), "row", split_axis=0, concat_axis=0, tiled=True
    )
    recon = pl.pallas_call(
        image_kernel,
        out_shape=jax.ShapeDtypeStruct((slab, pixels), jnp.float32),
        in_specs=[vmem()] * 3,
        out_specs=vmem(),
        cost_estimate=pl.CostEstimate(
            flops=4 * slab * pixels * pixels, bytes_accessed=6 << 20, transcendentals=0
        ),
        compiler_params=pltpu.CompilerParams(vmem_limit_bytes=12 << 20),
        name="image",
    )(back, cosine, sine)
    return recon.reshape(otf.shape)


def solution(mesh):
    in_specs = (P("cuts", None, None, "row", None), P("cuts", "row", None), P(), P(), P())
    out_specs = P("cuts", "row", None)

    return jax.shard_map(shards, mesh=mesh, in_specs=in_specs, out_specs=out_specs, check_vma=False)
```

```python
import functools
import math

import jax
import jax.numpy as jnp
from jax import lax
from jax.experimental import pallas as pl
from jax.experimental.pallas import tpu as pltpu
from jax.sharding import PartitionSpec as P


MULTIPLES = (0, 1, -1, 2, -2)
WIENER = 0.1
LANES = 128
GROUP = 16


def turn_of(angle):
    square = angle * angle
    cosine = jnp.zeros_like(angle)
    sine = jnp.zeros_like(angle)
    for order in range(9, -1, -1):
        sign = -1.0 if order % 2 else 1.0
        cosine = cosine * square + sign / math.factorial(2 * order)
        sine = sine * square + sign / math.factorial(2 * order + 1)
    return cosine, sine * angle


def band_kernel(
    angles, phases, index_ref, whole_ref, unmix_ref, raw_hbm, *rest
):
    parts = rest[:4]
    cos_ref, sin_ref, left_ref, raw_ref, low, spec, turned_even, turned_odd, phase, sem = rest[4:]
    frames = angles * phases
    slab = raw_ref.shape[0] // frames
    pixels = raw_ref.shape[1]
    lane_tiles = pixels // LANES
    tile = 256
    others = len(MULTIPLES) - 1
    index = index_ref[0]
    core = index & 1
    chip = index >> 1
    near = chip & 1
    pair = 2 * slab

    def offset(which, axis):
        return whole_ref[which, axis]

    fetch = pltpu.make_async_copy(raw_hbm, raw_ref, sem)
    fetch.start()

    column = lax.broadcasted_iota(jnp.int32, (LANES, LANES), 1)
    unit = 2.0 * math.pi / pixels

    @pl.loop(0, pixels // LANES)
    def _(step):
        first = pl.multiple_of(step * LANES, LANES)
        row = first + lax.broadcasted_iota(jnp.int32, (LANES, LANES), 0)
        around = ((row * column + pixels // 2) & (pixels - 1)) - pixels // 2
        low[0, pl.ds(first, LANES), :], low[1, pl.ds(first, LANES), :] = turn_of(
            around.astype(jnp.float32) * unit
        )

    repeat = lax.broadcasted_iota(jnp.int32, (GROUP, LANES), 0)
    factor = 1.0 / math.sqrt(pixels)

    def build(tab):
        around = ((repeat * (tab * LANES) + pixels // 2) & (pixels - 1)) - pixels // 2
        high_cos, high_sin = turn_of(around.astype(jnp.float32) * unit)
        high_cos = high_cos * factor
        high_sin = high_sin * factor
        for first in range(0, pixels, GROUP):
            rows = slice(first, first + GROUP)
            low_cos = low[0, rows, :]
            low_sin = low[1, rows, :]
            cut = slice(tab * LANES, (tab + 1) * LANES)
            cos_ref[rows, cut] = (high_cos * low_cos - high_sin * low_sin).astype(jnp.bfloat16)
            sin_ref[rows, cut] = (high_sin * low_cos + high_cos * low_sin).astype(jnp.bfloat16)

    per_tile = tile // LANES
    for tab in range(per_tile):
        build(tab)
    fetch.wait()
    for step in range(pixels // tile):
        cut = slice(step * tile, (step + 1) * tile)
        spec[0, :, cut] = jnp.dot(raw_ref[...], cos_ref[:, cut], preferred_element_type=jnp.float32)
        spec[1, :, cut] = jnp.dot(raw_ref[...], sin_ref[:, cut], preferred_element_type=jnp.float32)
        if step + 1 < pixels // tile:
            for tab in range(per_tile):
                build((step + 1) * per_tile + tab)

    @pl.loop(0, pixels // LANES)
    def _(step):
        rows = pl.ds(pl.multiple_of(step * LANES, LANES), LANES)
        first = pl.multiple_of(chip * pair // LANES * LANES, LANES)
        mine = []
        for ref in (cos_ref, sin_ref):
            value = ref[rows, pl.ds(first, LANES)]
            if pair < LANES:
                turn = (LANES - (chip * pair & (LANES - 1))) & (LANES - 1)
                value = pltpu.roll(value.astype(jnp.float32), turn, 1)[:, :pair]
                value = value.astype(jnp.bfloat16)
            mine.append(value)
        left_ref[step, 0:LANES, 0:pair] = mine[0]
        left_ref[step, 0:LANES, pair:] = mine[1]
        left_ref[step, LANES:, 0:pair] = -mine[1]
        left_ref[step, LANES:, pair:] = mine[0]

    image_row = index * slab + lax.broadcasted_iota(jnp.int32, (slab, LANES), 0)
    for which in range(angles):
        for m in range(1, others + 1):
            shift = MULTIPLES[m] * offset(which, 0)
            around = ((image_row * shift + pixels // 2) & (pixels - 1)) - pixels // 2
            cosine, sine = turn_of(around.astype(jnp.float32) * (2.0 * math.pi / pixels))
            phase[which * others + m - 1, 0] = cosine
            phase[which * others + m - 1, 1] = sine

    lane = lax.broadcasted_iota(jnp.int32, (GROUP, LANES), 1)
    quarter_tiles = lane_tiles // 4

    def weight(which, m, j):
        column = whole_ref[which, 2 + j]
        return unmix_ref[0, which, m, column], unmix_ref[1, which, m, column]

    def combine(terms, rows, slot):
        for tab in range(lane_tiles):
            cut = slice(tab * LANES, (tab + 1) * LANES)
            real = imag = None
            for frame, weight_re, weight_im in terms:
                here = pl.ds(pl.multiple_of(frame * slab + rows, GROUP), GROUP)
                cosine_sum = spec[0, here, cut]
                sine_sum = spec[1, here, cut]
                add_re = weight_re * cosine_sum + weight_im * sine_sum
                add_im = weight_im * cosine_sum - weight_re * sine_sum
                real = add_re if real is None else real + add_re
                imag = add_im if imag is None else imag + add_im
            slot[0, tab] = real
            slot[1, tab] = imag

    def put_out(band, rows, slot, shift):
        move = (-shift) & (pixels - 1)
        rest_lanes = move & (LANES - 1)
        turn = (LANES - rest_lanes) & (LANES - 1)
        for which, out in enumerate(parts):
            side = (1 - core) if which < 2 else core
            half = (1 - near) if which % 2 == 0 else near
            first = (2 * side + half) * quarter_tiles + move // LANES
            for part in range(2):
                tiles = [
                    pltpu.roll(slot[part, (first + i) & (lane_tiles - 1)], turn, 1)
                    for i in range(quarter_tiles + 1)
                ]
                put = pl.ds(pl.multiple_of(part * slab + rows, GROUP), GROUP)
                for i in range(quarter_tiles):
                    out[band, put, i * LANES : (i + 1) * LANES] = jnp.where(
                        lane < LANES - rest_lanes, tiles[i], tiles[i + 1]
                    ).astype(jnp.bfloat16)

    def terms_of(band, rows):
        which = band // others
        m = band - which * others + 1
        here = pl.ds(pl.multiple_of(rows, GROUP), GROUP)
        phase_re = phase[band, 0, here, :]
        phase_im = phase[band, 1, here, :]
        terms = []
        for j in range(phases):
            weight_re, weight_im = weight(which, m, j)
            terms.append(
                (
                    which * phases + j,
                    weight_re * phase_re - weight_im * phase_im,
                    weight_re * phase_im + weight_im * phase_re,
                )
            )
        return terms

    def shift_of(band):
        other = jnp.maximum(band - 1, 0)
        which = other // others
        m = other - which * others + 1
        mult = jnp.where(m <= 2, 1, 2) * jnp.where(m % 2 == 1, 1, -1)
        return jnp.where(band == 0, 0, mult * offset(which, 1))

    @pl.loop(0, slab // GROUP)
    def _(step):
        rows = step * GROUP
        terms = [
            (which * phases + j, *weight(which, 0, j))
            for which in range(angles)
            for j in range(phases)
        ]
        combine(terms, rows, turned_even)

        @pl.loop(0, angles * others // 2)
        def _(pair_index):
            band = 2 * pair_index
            combine(terms_of(band, rows), rows, turned_odd)
            put_out(band, rows, turned_even, shift_of(band))
            combine(terms_of(band + 1, rows), rows, turned_even)
            put_out(band + 1, rows, turned_odd, shift_of(band + 1))

        put_out(angles * others, rows, turned_even, shift_of(angles * others))


def shift_by(whole_ref, band, axis):
    if band == 0:
        return 0
    which, m = divmod(band - 1, len(MULTIPLES) - 1)
    return MULTIPLES[m + 1] * whole_ref[which, axis]


def widen_otf(wide, masks, index, near_ref, far_ref):
    lane_tiles = wide.shape[0]
    pixels = lane_tiles * LANES
    pieces, slab = near_ref.shape[:2]
    for piece in range(2 * pieces):
        ref = far_ref if piece >= pieces else near_ref
        start = pl.multiple_of((index ^ masks[piece]) * slab, slab)
        for lane in range(lane_tiles):
            wide[lane, pl.ds(start, slab), :] = ref[
                piece % pieces, :, lane * LANES : (lane + 1) * LANES
            ].astype(jnp.float32)
    for lane in range(lane_tiles):
        wide[lane, pixels:, :] = wide[lane, 0 : wide.shape[1] - pixels, :]


def response(wide, whole_ref, q0, band, column, count):
    lane_tiles = wide.shape[0]
    pixels = lane_tiles * LANES
    tile = wide.shape[1] - pixels
    start = (q0 - shift_by(whole_ref, band, 0)) & (pixels - 1)
    column = (column - shift_by(whole_ref, band, 1)) & (pixels - 1)
    rest_lanes = column & (LANES - 1)
    first = column // LANES
    turn = (LANES - rest_lanes) & (LANES - 1)
    lanes = lax.broadcasted_iota(jnp.int32, (tile, LANES), 1)
    turned = [
        pltpu.roll(wide[(first + i) & (lane_tiles - 1), pl.ds(start, tile), :], turn, 1)
        for i in range(count + 1)
    ]
    return [jnp.where(lanes < LANES - rest_lanes, turned[i], turned[i + 1]) for i in range(count)]


def numer_kernel(
    columns, masks, own, index_ref, whole_ref, keep_away, got_away, keep_near, got_near, left_ref,
    near_ref, far_ref, *rest
):
    outs = rest[:4]
    wide, total, right, right_up = rest[4:]
    pixels = wide.shape[0] * LANES
    tile = wide.shape[1] - pixels
    bands, twice, width = keep_away.shape
    slab = twice // 2
    tiles = width // LANES
    half = tiles // 2
    index = index_ref[0]
    core = index & 1
    chip = index >> 1
    sides = (chip & 1, (chip >> 1) & 1)
    chosen = sides if own else (1 - sides[0], 1 - sides[1])
    lower = (keep_near, got_near) if own else (keep_away, got_away)

    @pl.loop(0, bands)
    def _(band):
        cut = pl.ds(pl.multiple_of(chosen[1] * (half * LANES), LANES), half * LANES)
        for which, side in ((0, core), (1, 1 - core)):
            for part in range(2):
                put = pl.ds(pl.multiple_of((2 * part + side) * slab, slab), slab)
                rows = slice(part * slab, (part + 1) * slab)
                right[band, put, :] = lower[which][band, rows, :]
                for i, pair in enumerate(((keep_away, got_away), (keep_near, got_near))):
                    to = slice(i * half * LANES, (i + 1) * half * LANES)
                    right_up[band, put, to] = pair[which][band, rows, cut]

    widen_otf(wide, masks, index, near_ref, far_ref)
    steps = pixels // tile // 2

    def tile_of(step, upper):
        q0 = pl.multiple_of((step + upper * steps) * tile, tile)
        to = pl.ds(pl.multiple_of(step * tile, tile), tile)
        left = left_ref[step + upper * steps]
        for band in range(bands):
            product = jnp.dot(
                left, (right_up if upper else right)[band], preferred_element_type=jnp.float32
            )
            if upper:
                weights = []
                for side in (1 - sides[0], sides[0]):
                    column = (2 * core + side) * width + chosen[1] * (half * LANES)
                    weights += response(wide, whole_ref, q0, band, column, half)
            else:
                column = (2 * core + chosen[0]) * width
                weights = response(wide, whole_ref, q0, band, column, tiles)
            for i in range(tiles):
                cut = slice(i * LANES, (i + 1) * LANES)
                for part in range(2):
                    value = weights[i] * product[part * tile : (part + 1) * tile, cut]
                    if band == 0:
                        total[i, part] = value
                    else:
                        total[i, part] += value
        for which in range(2):
            out = outs[2 * which + upper]
            first = which if upper else (sides[1] if which else 1 - sides[1])
            per_tile = LANES // columns
            for i in range(half):
                real = total[first * half + i, 0]
                imag = total[first * half + i, 1]
                for j in range(per_tile):
                    cut = slice(j * columns, (j + 1) * columns)
                    out[i * per_tile + j, to, :] = jnp.concatenate(
                        [real[:, cut], imag[:, cut]], axis=1
                    ).astype(jnp.bfloat16)

    for upper in range(2):
        pl.loop(0, steps)(functools.partial(tile_of, upper=upper))


def power_kernel(columns, bands, masks, index_ref, whole_ref, near_ref, far_ref, after, power_ref, wide):
    pixels = power_ref.shape[0]
    tile = wide.shape[1] - pixels
    index = index_ref[0]
    core = index & 1
    chip = index >> 1
    levels = (pixels // columns // 2).bit_length() - 1
    place = sum(((chip >> bit) & 1) << (levels - 1 - bit) for bit in range(levels))
    own_column = core * (pixels // 2) + place * columns
    angles = (bands - 1) // (len(MULTIPLES) - 1)
    widen_otf(wide, masks, index, near_ref, far_ref)

    @pl.loop(0, pixels // tile)
    def _(step):
        q0 = pl.multiple_of(step * tile, tile)
        gathered = None
        for band in range(bands):
            value = response(wide, whole_ref, q0, band, own_column, 1)[0]
            value = value * value
            gathered = value * float(angles) if band == 0 else gathered + value
        power_ref[pl.ds(q0, tile), :] = jnp.concatenate(
            [gathered[:, :columns], gathered[:, :columns]], axis=1
        )


def fold_kernel(bit, index_ref, *refs):
    *parts, far_ref, stay_ref = refs
    count = far_ref.shape[0]
    side = (index_ref[0] >> (bit + 1)) & 1
    for block in range(count):
        for out, first in ((far_ref, (1 - side) * count), (stay_ref, side * count)):
            value = None
            for ref in parts:
                one = ref[first + block].astype(jnp.float32)
                value = one if value is None else value + one
            out[block] = value.astype(out.dtype)


def inverse_kernel(columns, total, numers, *refs):
    parts = refs[: 2 * numers]
    *powers, cos_ref, sin_ref, half_ref, ratio = refs[2 * numers :]
    pixels = half_ref.shape[0]
    rows = pixels // 2
    for upper in range(2):
        here = slice(upper * rows, (upper + 1) * rows)
        power = powers[0][here, :]
        for ref in powers[1:]:
            power = power + ref[here, :]
        numer = None
        for ref in parts[upper * numers : (upper + 1) * numers]:
            one = ref[0].astype(jnp.float32)
            numer = one if numer is None else numer + one
        ratio[here, :] = (numer / (WIENER + power / total)).astype(jnp.bfloat16)
    tile = 256
    for first in range(0, pixels, tile):
        here = slice(first, first + tile)
        by_cos = jnp.dot(cos_ref[here, :], ratio[...], preferred_element_type=jnp.float32)
        by_sin = jnp.dot(sin_ref[here, :], ratio[...], preferred_element_type=jnp.float32)
        real = by_cos[:, :columns] - by_sin[:, columns:]
        imag = by_cos[:, columns:] + by_sin[:, :columns]
        half_ref[here, :] = jnp.concatenate([real, -imag], axis=1).astype(jnp.bfloat16)


def pack_kernel(*refs):
    out_ref = refs[-1]
    for index, ref in enumerate(refs[:-1]):
        out_ref[index] = ref[...]


def image_kernel(back_ref, cos_ref, sin_ref, out_ref):
    devices, _, twice = back_ref.shape
    columns = twice // 2
    chips = devices // 2
    levels = chips.bit_length() - 1
    pixels = out_ref.shape[1]
    total = None
    for chip in range(chips):
        place = sum(((chip >> bit) & 1) << (levels - 1 - bit) for bit in range(levels))
        rows = []
        for core in range(2):
            start = core * (pixels // 2) + place * columns
            rows += [ref[start : start + columns, :] for ref in (cos_ref, sin_ref)]
        left = jnp.concatenate([back_ref[2 * chip], back_ref[2 * chip + 1]], axis=1)
        value = jnp.dot(left, jnp.concatenate(rows, axis=0), preferred_element_type=jnp.float32)
        total = value if total is None else total + value
    out_ref[...] = total


def smem():
    return pl.BlockSpec(memory_space=pltpu.SMEM)


def vmem():
    return pl.BlockSpec(memory_space=pltpu.VMEM)


def swap(value, axis, mask):
    size = lax.axis_size(axis)
    return lax.ppermute(value, axis, [(i, i ^ mask) for i in range(size)])


def shards(raw, otf, offsets, phase_order, unmix):
    pixels = raw.shape[-1]
    slab = raw.shape[3]
    angles, phases = raw.shape[1:3]
    devices = lax.axis_size("row")
    index = lax.axis_index("row")
    slices = raw.shape[0] * lax.axis_size("cuts")
    chips = devices // 2
    levels = chips.bit_length() - 1
    columns = pixels // devices
    frames = angles * phases
    bands = 1 + angles * (len(MULTIPLES) - 1)

    mine = otf.reshape(slab, pixels).astype(jnp.bfloat16)
    masks = list(range(0, devices, 2))
    pieces = [mine] + [swap(mine, "row", mask) for mask in masks[1:]]
    masks += [mask | 1 for mask in masks]

    quarter = pixels // 4
    where = index.astype(jnp.int32).reshape(1)
    whole = jnp.concatenate([offsets, phase_order], axis=1)
    hbm = pl.BlockSpec(memory_space=pltpu.HBM)
    part = (bands, 2 * slab, quarter)
    left_shape = (pixels // LANES, 2 * LANES, 4 * slab)
    send_away, send_near, keep_away, keep_near, cosine, sine, left = pl.pallas_call(
        functools.partial(band_kernel, angles, phases),
        out_shape=[jax.ShapeDtypeStruct(part, jnp.bfloat16)] * 4
        + [jax.ShapeDtypeStruct((pixels, pixels), jnp.bfloat16)] * 2
        + [jax.ShapeDtypeStruct(left_shape, jnp.bfloat16)],
        in_specs=[smem()] * 3 + [hbm],
        out_specs=[vmem()] * 7,
        scratch_shapes=[
            pltpu.VMEM((frames * slab, pixels), jnp.bfloat16),
            pltpu.VMEM((2, pixels, LANES), jnp.float32),
            pltpu.VMEM((2, frames * slab, pixels), jnp.float32),
            pltpu.VMEM((2, pixels // LANES, GROUP, LANES), jnp.float32),
            pltpu.VMEM((2, pixels // LANES, GROUP, LANES), jnp.float32),
            pltpu.VMEM((bands - 1, 2, slab, LANES), jnp.float32),
            pltpu.SemaphoreType.DMA,
        ],
        cost_estimate=pl.CostEstimate(
            flops=8 * frames * slab * pixels * pixels,
            bytes_accessed=12 << 20,
            transcendentals=0,
        ),
        compiler_params=pltpu.CompilerParams(vmem_limit_bytes=18 << 20),
        name="bands",
    )(where, whole, unmix, raw.reshape(frames * slab, pixels))

    got_away = swap(send_away, "row", 1)
    own_pieces = pl.pallas_call(
        pack_kernel,
        out_shape=jax.ShapeDtypeStruct((chips, slab, pixels), jnp.bfloat16),
        in_specs=[vmem()] * chips,
        out_specs=vmem(),
        compiler_params=pltpu.CompilerParams(vmem_limit_bytes=8 << 20),
        cost_estimate=pl.CostEstimate(
            flops=chips * slab * pixels, bytes_accessed=2 << 20, transcendentals=0
        ),
        name="pack",
    )(*pieces)
    other_pieces = swap(own_pieces, "row", 1)
    got_near = swap(send_near, "row", 1)

    half_shape = jax.ShapeDtypeStruct((chips // 4, pixels // 2, 2 * columns), jnp.bfloat16)
    wide_scratch = pltpu.VMEM((pixels // LANES, pixels + LANES, LANES), jnp.float32)

    def partial(own):
        return pl.pallas_call(
            functools.partial(numer_kernel, columns, tuple(masks), own),
            out_shape=[half_shape] * 4,
            in_specs=[smem()] * 2 + [vmem()] * 7,
            out_specs=[vmem()] * 4,
            scratch_shapes=[
                wide_scratch,
                pltpu.VMEM((quarter // LANES, 2, LANES, LANES), jnp.float32),
                pltpu.VMEM((bands, 4 * slab, quarter), jnp.bfloat16),
                pltpu.VMEM((bands, 4 * slab, quarter), jnp.bfloat16),
            ],
            cost_estimate=pl.CostEstimate(
                flops=16 * bands * slab * pixels * quarter,
                bytes_accessed=8 << 20,
                transcendentals=0,
            ),
            compiler_params=pltpu.CompilerParams(vmem_limit_bytes=18 << 20),
        )(
            where, whole, keep_away, got_away, keep_near, got_near, left, own_pieces,
            other_pieces
        )

    away = partial(False)
    moved = [swap(value, "row", mask) for value, mask in zip(away, (2, 4, 2, 4))]
    kept = partial(True)
    power = pl.pallas_call(
        functools.partial(power_kernel, columns, bands, tuple(masks)),
        out_shape=jax.ShapeDtypeStruct((pixels, 2 * columns), jnp.float32),
        in_specs=[smem()] * 2 + [vmem()] * 2 + [pl.BlockSpec(memory_space=pl.ANY)],
        out_specs=vmem(),
        scratch_shapes=[wide_scratch],
        cost_estimate=pl.CostEstimate(
            flops=16000 * pixels * columns, bytes_accessed=5 << 20, transcendentals=0
        ),
        compiler_params=pltpu.CompilerParams(vmem_limit_bytes=12 << 20),
        name="power",
    )(where, whole, own_pieces, other_pieces, kept[0])

    def fold(bit, parts):
        blocks, rows, lanes = parts[0].shape
        share = (blocks // 2, rows, lanes)
        return pl.pallas_call(
            functools.partial(fold_kernel, bit),
            out_shape=[
                jax.ShapeDtypeStruct(share, jnp.bfloat16),
                jax.ShapeDtypeStruct(share, jnp.float32),
            ],
            in_specs=[smem()] + [vmem()] * len(parts),
            out_specs=[vmem()] * 2,
            cost_estimate=pl.CostEstimate(
                flops=blocks * rows * lanes * 4, bytes_accessed=1 << 20, transcendentals=0
            ),
            compiler_params=pltpu.CompilerParams(vmem_limit_bytes=8 << 20),
            name="fold",
        )(where, *parts)

    def widen(value):
        return value.astype(jnp.float32)

    fars = [(widen(moved[h]) + widen(kept[h])).astype(jnp.bfloat16) for h in range(2)]
    stays = [[moved[2 + h], kept[2 + h]] for h in range(2)]
    for bit in range(1, levels):
        over = (2 << bit, 2) if bit == 1 else (2 << bit, 2 << bit)
        for h in range(2):
            stays[h].append(swap(fars[h], "row", over[h]))
            if bit < levels - 1:
                fars[h], stay = fold(bit + 1, stays[h])
                stays[h] = [stay]

    powers = [power]
    cuts = lax.axis_size("cuts")
    for _ in range(cuts - 1):
        powers.append(
            lax.ppermute(powers[-1], "cuts", [(i, (i + 1) % cuts) for i in range(cuts)])
        )
    parts = stays[0] + stays[1] + powers
    half = pl.pallas_call(
        functools.partial(inverse_kernel, columns, float(slices * angles), len(stays[0])),
        out_shape=jax.ShapeDtypeStruct((pixels, 2 * columns), jnp.bfloat16),
        in_specs=[vmem()] * (len(parts) + 2),
        out_specs=vmem(),
        scratch_shapes=[pltpu.VMEM((pixels, 2 * columns), jnp.bfloat16)],
        cost_estimate=pl.CostEstimate(
            flops=8 * pixels * pixels * columns, bytes_accessed=6 << 20, transcendentals=0
        ),
        compiler_params=pltpu.CompilerParams(vmem_limit_bytes=12 << 20),
        name="inverse",
    )(*parts, cosine, sine)
    back = lax.all_to_all(
        half.reshape(devices, slab, 2 * columns), "row", split_axis=0, concat_axis=0, tiled=True
    )
    recon = pl.pallas_call(
        image_kernel,
        out_shape=jax.ShapeDtypeStruct((slab, pixels), jnp.float32),
        in_specs=[vmem()] * 3,
        out_specs=vmem(),
        cost_estimate=pl.CostEstimate(
            flops=4 * slab * pixels * pixels, bytes_accessed=6 << 20, transcendentals=0
        ),
        compiler_params=pltpu.CompilerParams(vmem_limit_bytes=8 << 20),
        name="image",
    )(back, cosine, sine)
    return recon.reshape(otf.shape)


def solution(mesh):
    in_specs = (P("cuts", None, None, "row", None), P("cuts", "row", None), P(), P(), P())
    out_specs = P("cuts", "row", None)

    return jax.shard_map(shards, mesh=mesh, in_specs=in_specs, out_specs=out_specs, check_vma=False)
```

```python
import functools
import math

import jax
import jax.numpy as jnp
from jax import lax
from jax.experimental import pallas as pl
from jax.experimental.pallas import tpu as pltpu
from jax.sharding import PartitionSpec as P


MULTIPLES = (0, 1, -1, 2, -2)
WIENER = 0.1
LANES = 128
GROUP = 16


def turn_of(angle):
    square = angle * angle
    cosine = jnp.zeros_like(angle)
    sine = jnp.zeros_like(angle)
    for order in range(9, -1, -1):
        sign = -1.0 if order % 2 else 1.0
        cosine = cosine * square + sign / math.factorial(2 * order)
        sine = sine * square + sign / math.factorial(2 * order + 1)
    return cosine, sine * angle


def spectra_kernel(slab, index_ref, raw_ref, spec, cos_ref, sin_ref, left_ref, low):
    pixels = raw_ref.shape[1]
    tile = 256
    chip = index_ref[0] >> 1
    pair = 2 * slab

    column = lax.broadcasted_iota(jnp.int32, (LANES, LANES), 1)
    unit = 2.0 * math.pi / pixels

    @pl.loop(0, pixels // LANES)
    def _(step):
        first = pl.multiple_of(step * LANES, LANES)
        row = first + lax.broadcasted_iota(jnp.int32, (LANES, LANES), 0)
        around = ((row * column + pixels // 2) & (pixels - 1)) - pixels // 2
        low[0, pl.ds(first, LANES), :], low[1, pl.ds(first, LANES), :] = turn_of(
            around.astype(jnp.float32) * unit
        )

    repeat = lax.broadcasted_iota(jnp.int32, (GROUP, LANES), 0)
    factor = 1.0 / math.sqrt(pixels)

    def build(tab):
        around = ((repeat * (tab * LANES) + pixels // 2) & (pixels - 1)) - pixels // 2
        high_cos, high_sin = turn_of(around.astype(jnp.float32) * unit)
        high_cos = high_cos * factor
        high_sin = high_sin * factor
        for first in range(0, pixels, GROUP):
            rows = slice(first, first + GROUP)
            low_cos = low[0, rows, :]
            low_sin = low[1, rows, :]
            cut = slice(tab * LANES, (tab + 1) * LANES)
            cos_ref[rows, cut] = (high_cos * low_cos - high_sin * low_sin).astype(jnp.bfloat16)
            sin_ref[rows, cut] = (high_sin * low_cos + high_cos * low_sin).astype(jnp.bfloat16)

    per_tile = tile // LANES
    for tab in range(per_tile):
        build(tab)
    for step in range(pixels // tile):
        cut = slice(step * tile, (step + 1) * tile)
        spec[0, :, cut] = jnp.dot(raw_ref[...], cos_ref[:, cut], preferred_element_type=jnp.float32)
        spec[1, :, cut] = jnp.dot(raw_ref[...], sin_ref[:, cut], preferred_element_type=jnp.float32)
        if step + 1 < pixels // tile:
            for tab in range(per_tile):
                build((step + 1) * per_tile + tab)

    @pl.loop(0, pixels // LANES)
    def _(step):
        rows = pl.ds(pl.multiple_of(step * LANES, LANES), LANES)
        first = pl.multiple_of(chip * pair // LANES * LANES, LANES)
        mine = []
        for ref in (cos_ref, sin_ref):
            value = ref[rows, pl.ds(first, LANES)]
            if pair < LANES:
                turn = (LANES - (chip * pair & (LANES - 1))) & (LANES - 1)
                value = pltpu.roll(value.astype(jnp.float32), turn, 1)[:, :pair]
                value = value.astype(jnp.bfloat16)
            mine.append(value)
        left_ref[step, 0:LANES, 0:pair] = mine[0]
        left_ref[step, 0:LANES, pair:] = mine[1]
        left_ref[step, LANES:, 0:pair] = -mine[1]
        left_ref[step, LANES:, pair:] = mine[0]


def band_kernel(
    angles, phases, index_ref, shift_ref, unmix_ref, spec, *rest
):
    parts = rest[:4]
    turned_even, turned_odd, phase = rest[4:]
    frames = angles * phases
    slab = spec.shape[1] // frames
    pixels = spec.shape[2]
    lane_tiles = pixels // LANES
    others = len(MULTIPLES) - 1
    index = index_ref[0]
    core = index & 1
    near = (index >> 1) & 1

    def offset(which, axis):
        return shift_ref[axis, which]

    image_row = index * slab + lax.broadcasted_iota(jnp.int32, (slab, LANES), 0)
    for which in range(angles):
        for m in range(1, others + 1):
            shift = MULTIPLES[m] * offset(which, 0)
            around = ((image_row * shift + pixels // 2) & (pixels - 1)) - pixels // 2
            cosine, sine = turn_of(around.astype(jnp.float32) * (2.0 * math.pi / pixels))
            phase[which * others + m - 1, 0] = cosine
            phase[which * others + m - 1, 1] = sine

    lane = lax.broadcasted_iota(jnp.int32, (GROUP, LANES), 1)
    quarter_tiles = lane_tiles // 4

    def weight(which, m, j):
        column = shift_ref[2 + which, j]
        return unmix_ref[which, m, 0, column], unmix_ref[which, m, 1, column]

    def combine(terms, rows, slot):
        for tab in range(lane_tiles):
            cut = slice(tab * LANES, (tab + 1) * LANES)
            real = imag = None
            for frame, weight_re, weight_im in terms:
                here = pl.ds(pl.multiple_of(frame * slab + rows, GROUP), GROUP)
                cosine_sum = spec[0, here, cut]
                sine_sum = spec[1, here, cut]
                add_re = weight_re * cosine_sum + weight_im * sine_sum
                add_im = weight_im * cosine_sum - weight_re * sine_sum
                real = add_re if real is None else real + add_re
                imag = add_im if imag is None else imag + add_im
            slot[0, tab] = real
            slot[1, tab] = imag

    def put_out(band, rows, slot, shift):
        move = (-shift) & (pixels - 1)
        rest_lanes = move & (LANES - 1)
        turn = (LANES - rest_lanes) & (LANES - 1)
        for which, out in enumerate(parts):
            side = (1 - core) if which < 2 else core
            half = (1 - near) if which % 2 == 0 else near
            first = (2 * side + half) * quarter_tiles + move // LANES
            for part in range(2):
                tiles = [
                    pltpu.roll(slot[part, (first + i) & (lane_tiles - 1)], turn, 1)
                    for i in range(quarter_tiles + 1)
                ]
                put = pl.ds(pl.multiple_of(part * slab + rows, GROUP), GROUP)
                for i in range(quarter_tiles):
                    out[band, put, i * LANES : (i + 1) * LANES] = jnp.where(
                        lane < LANES - rest_lanes, tiles[i], tiles[i + 1]
                    ).astype(jnp.bfloat16)

    def terms_of(band, rows):
        which = band // others
        m = band - which * others + 1
        here = pl.ds(pl.multiple_of(rows, GROUP), GROUP)
        phase_re = phase[band, 0, here, :]
        phase_im = phase[band, 1, here, :]
        terms = []
        for j in range(phases):
            weight_re, weight_im = weight(which, m, j)
            terms.append(
                (
                    which * phases + j,
                    weight_re * phase_re - weight_im * phase_im,
                    weight_re * phase_im + weight_im * phase_re,
                )
            )
        return terms

    def shift_of(band):
        other = jnp.maximum(band - 1, 0)
        which = other // others
        m = other - which * others + 1
        mult = jnp.where(m <= 2, 1, 2) * jnp.where(m % 2 == 1, 1, -1)
        return jnp.where(band == 0, 0, mult * offset(which, 1))

    @pl.loop(0, slab // GROUP)
    def _(step):
        rows = step * GROUP
        terms = [
            (which * phases + j, *weight(which, 0, j))
            for which in range(angles)
            for j in range(phases)
        ]
        combine(terms, rows, turned_even)

        @pl.loop(0, angles * others // 2)
        def _(pair_index):
            band = 2 * pair_index
            combine(terms_of(band, rows), rows, turned_odd)
            put_out(band, rows, turned_even, shift_of(band))
            combine(terms_of(band + 1, rows), rows, turned_even)
            put_out(band + 1, rows, turned_odd, shift_of(band + 1))

        put_out(angles * others, rows, turned_even, shift_of(angles * others))


def shift_by(shift_ref, band, axis):
    if band == 0:
        return 0
    which, m = divmod(band - 1, len(MULTIPLES) - 1)
    return MULTIPLES[m + 1] * shift_ref[axis, which]


def widen_otf(wide, masks, index, refs):
    lane_tiles = wide.shape[0]
    pixels = lane_tiles * LANES
    pieces, slab = refs[0].shape[:2]
    for piece, mask in enumerate(masks):
        ref = refs[piece // pieces]
        start = pl.multiple_of((index ^ mask) * slab, slab)
        for lane in range(lane_tiles):
            wide[lane, pl.ds(start, slab), :] = ref[
                piece % pieces, :, lane * LANES : (lane + 1) * LANES
            ].astype(jnp.float32)
    for lane in range(lane_tiles):
        wide[lane, pixels:, :] = wide[lane, 0 : wide.shape[1] - pixels, :]


def response(wide, shift_ref, q0, band, column, count):
    lane_tiles = wide.shape[0]
    pixels = lane_tiles * LANES
    tile = wide.shape[1] - pixels
    start = (q0 - shift_by(shift_ref, band, 0)) & (pixels - 1)
    column = (column - shift_by(shift_ref, band, 1)) & (pixels - 1)
    rest_lanes = column & (LANES - 1)
    first = column // LANES
    turn = (LANES - rest_lanes) & (LANES - 1)
    lanes = lax.broadcasted_iota(jnp.int32, (tile, LANES), 1)
    turned = [
        pltpu.roll(wide[(first + i) & (lane_tiles - 1), pl.ds(start, tile), :], turn, 1)
        for i in range(count + 1)
    ]
    return [jnp.where(lanes < LANES - rest_lanes, turned[i], turned[i + 1]) for i in range(count)]


def numer_kernel(
    columns, masks, own, index_ref, shift_ref, keep_away, got_away, keep_near, got_near, left_ref,
    *rest
):
    otf_refs = rest[:4]
    outs = rest[4:8]
    wide, total, right, right_up = rest[8:]
    pixels = wide.shape[0] * LANES
    tile = wide.shape[1] - pixels
    bands, twice, width = keep_away.shape
    slab = twice // 2
    tiles = width // LANES
    half = tiles // 2
    index = index_ref[0]
    core = index & 1
    chip = index >> 1
    sides = (chip & 1, (chip >> 1) & 1)
    chosen = sides if own else (1 - sides[0], 1 - sides[1])
    lower = (keep_near, got_near) if own else (keep_away, got_away)

    @pl.loop(0, bands)
    def _(band):
        cut = pl.ds(pl.multiple_of(chosen[1] * (half * LANES), LANES), half * LANES)
        for which, side in ((0, core), (1, 1 - core)):
            for part in range(2):
                put = pl.ds(pl.multiple_of((2 * part + side) * slab, slab), slab)
                rows = slice(part * slab, (part + 1) * slab)
                right[band, put, :] = lower[which][band, rows, :]
                for i, pair in enumerate(((keep_away, got_away), (keep_near, got_near))):
                    to = slice(i * half * LANES, (i + 1) * half * LANES)
                    right_up[band, put, to] = pair[which][band, rows, cut]

    widen_otf(wide, masks, index, otf_refs)
    steps = pixels // tile // 2

    def tile_of(step, upper):
        q0 = pl.multiple_of((step + upper * steps) * tile, tile)
        to = pl.ds(pl.multiple_of(step * tile, tile), tile)
        left = left_ref[step + upper * steps]
        for band in range(bands):
            product = jnp.dot(
                left, (right_up if upper else right)[band], preferred_element_type=jnp.float32
            )
            if upper:
                weights = []
                for side in (1 - sides[0], sides[0]):
                    column = (2 * core + side) * width + chosen[1] * (half * LANES)
                    weights += response(wide, shift_ref, q0, band, column, half)
            else:
                column = (2 * core + chosen[0]) * width
                weights = response(wide, shift_ref, q0, band, column, tiles)
            for i in range(tiles):
                cut = slice(i * LANES, (i + 1) * LANES)
                for part in range(2):
                    value = weights[i] * product[part * tile : (part + 1) * tile, cut]
                    if band == 0:
                        total[i, part] = value
                    else:
                        total[i, part] += value
        for which in range(2):
            out = outs[2 * which + upper]
            first = which if upper else (sides[1] if which else 1 - sides[1])
            per_tile = LANES // columns
            for i in range(half):
                real = total[first * half + i, 0]
                imag = total[first * half + i, 1]
                for j in range(per_tile):
                    cut = slice(j * columns, (j + 1) * columns)
                    out[i * per_tile + j, to, :] = jnp.concatenate(
                        [real[:, cut], imag[:, cut]], axis=1
                    ).astype(jnp.bfloat16)

    for upper in range(2):
        pl.loop(0, steps)(functools.partial(tile_of, upper=upper))


def power_kernel(columns, bands, masks, index_ref, shift_ref, *rest):
    *otf_refs, _, power_ref, wide = rest
    pixels = power_ref.shape[0]
    tile = wide.shape[1] - pixels
    index = index_ref[0]
    core = index & 1
    chip = index >> 1
    levels = (pixels // columns // 2).bit_length() - 1
    place = sum(((chip >> bit) & 1) << (levels - 1 - bit) for bit in range(levels))
    own_column = core * (pixels // 2) + place * columns
    angles = (bands - 1) // (len(MULTIPLES) - 1)
    widen_otf(wide, masks, index, otf_refs)

    @pl.loop(0, pixels // tile)
    def _(step):
        q0 = pl.multiple_of(step * tile, tile)
        gathered = None
        for band in range(bands):
            value = response(wide, shift_ref, q0, band, own_column, 1)[0]
            value = value * value
            gathered = value * float(angles) if band == 0 else gathered + value
        power_ref[pl.ds(q0, tile), :] = jnp.concatenate(
            [gathered[:, :columns], gathered[:, :columns]], axis=1
        )


def fold_kernel(bit, index_ref, *refs):
    *parts, far_ref, stay_ref = refs
    count = far_ref.shape[0]
    side = (index_ref[0] >> (bit + 1)) & 1
    for block in range(count):
        for out, first in ((far_ref, (1 - side) * count), (stay_ref, side * count)):
            value = None
            for ref in parts:
                one = ref[first + block].astype(jnp.float32)
                value = one if value is None else value + one
            out[block] = value.astype(out.dtype)


def inverse_kernel(columns, total, numers, *refs):
    parts = refs[: 2 * numers]
    *powers, cos_ref, sin_ref, half_ref, ratio = refs[2 * numers :]
    pixels = half_ref.shape[0]
    rows = pixels // 2
    for upper in range(2):
        here = slice(upper * rows, (upper + 1) * rows)
        power = powers[0][here, :]
        for ref in powers[1:]:
            power = power + ref[here, :]
        numer = None
        for ref in parts[upper * numers : (upper + 1) * numers]:
            one = ref[0].astype(jnp.float32)
            numer = one if numer is None else numer + one
        ratio[here, :] = (numer / (WIENER + power / total)).astype(jnp.bfloat16)
    tile = 256
    for first in range(0, pixels, tile):
        here = slice(first, first + tile)
        by_cos = jnp.dot(cos_ref[here, :], ratio[...], preferred_element_type=jnp.float32)
        by_sin = jnp.dot(sin_ref[here, :], ratio[...], preferred_element_type=jnp.float32)
        real = by_cos[:, :columns] - by_sin[:, columns:]
        imag = by_cos[:, columns:] + by_sin[:, :columns]
        half_ref[here, :] = jnp.concatenate([real, -imag], axis=1).astype(jnp.bfloat16)


def join_kernel(head_ref, tail_ref, out_ref):
    out_ref[0] = head_ref[...]
    out_ref[1:] = tail_ref[...]


def pack_kernel(*refs):
    out_ref = refs[-1]
    for index, ref in enumerate(refs[:-1]):
        out_ref[index] = ref[...]


def image_kernel(back_ref, cos_ref, sin_ref, out_ref):
    devices, _, twice = back_ref.shape
    columns = twice // 2
    chips = devices // 2
    levels = chips.bit_length() - 1
    pixels = out_ref.shape[1]
    total = None
    for chip in range(chips):
        place = sum(((chip >> bit) & 1) << (levels - 1 - bit) for bit in range(levels))
        rows = []
        for core in range(2):
            start = core * (pixels // 2) + place * columns
            rows += [ref[start : start + columns, :] for ref in (cos_ref, sin_ref)]
        left = jnp.concatenate([back_ref[2 * chip], back_ref[2 * chip + 1]], axis=1)
        value = jnp.dot(left, jnp.concatenate(rows, axis=0), preferred_element_type=jnp.float32)
        total = value if total is None else total + value
    out_ref[...] = total


def smem():
    return pl.BlockSpec(memory_space=pltpu.SMEM)


def vmem():
    return pl.BlockSpec(memory_space=pltpu.VMEM)


def swap(value, axis, mask):
    size = lax.axis_size(axis)
    return lax.ppermute(value, axis, [(i, i ^ mask) for i in range(size)])


def shards(raw, otf, offsets, phase_order, unmix):
    pixels = raw.shape[-1]
    slab = raw.shape[3]
    angles, phases = raw.shape[1:3]
    devices = lax.axis_size("row")
    index = lax.axis_index("row")
    slices = raw.shape[0] * lax.axis_size("cuts")
    chips = devices // 2
    levels = chips.bit_length() - 1
    columns = pixels // devices
    frames = angles * phases
    bands = 1 + angles * (len(MULTIPLES) - 1)

    mine = otf.reshape(slab, pixels).astype(jnp.bfloat16)
    masks = list(range(0, devices, 4))
    far = [swap(mine, "row", mask) for mask in masks[1:]]
    across = swap(mine, "row", 2)
    masks += [mask | 2 for mask in masks]
    masks += [mask | 1 for mask in masks]

    quarter = pixels // 4
    where = index.astype(jnp.int32).reshape(1)
    longer = [(0, 0), (0, phases - angles)]
    shifts = jnp.concatenate([jnp.pad(offsets.T, longer), phase_order], axis=0)
    matrices = jnp.transpose(unmix, (1, 2, 0, 3))
    part = (bands, 2 * slab, quarter)
    left_shape = (pixels // LANES, 2 * LANES, 4 * slab)
    spec, cosine, sine, left = pl.pallas_call(
        functools.partial(spectra_kernel, slab),
        out_shape=[jax.ShapeDtypeStruct((2, frames * slab, pixels), jnp.float32)]
        + [jax.ShapeDtypeStruct((pixels, pixels), jnp.bfloat16)] * 2
        + [jax.ShapeDtypeStruct(left_shape, jnp.bfloat16)],
        in_specs=[smem(), vmem()],
        out_specs=[vmem()] * 4,
        scratch_shapes=[pltpu.VMEM((2, pixels, LANES), jnp.float32)],
        cost_estimate=pl.CostEstimate(
            flops=4 * frames * slab * pixels * pixels,
            bytes_accessed=12 << 20,
            transcendentals=0,
        ),
        compiler_params=pltpu.CompilerParams(vmem_limit_bytes=20 << 20),
        name="spectra",
    )(where, raw.reshape(frames * slab, pixels))

    def join(head, tail):
        return pl.pallas_call(
            join_kernel,
            out_shape=jax.ShapeDtypeStruct((tail.shape[0] + 1, slab, pixels), jnp.bfloat16),
            in_specs=[vmem()] * 2,
            out_specs=vmem(),
            compiler_params=pltpu.CompilerParams(vmem_limit_bytes=8 << 20),
            cost_estimate=pl.CostEstimate(
                flops=slab * pixels, bytes_accessed=2 << 20, transcendentals=0
            ),
            name="join",
        )(head[0], tail)

    def pack(parts):
        return pl.pallas_call(
            pack_kernel,
            out_shape=jax.ShapeDtypeStruct((len(parts), slab, pixels), jnp.bfloat16),
            in_specs=[vmem()] * len(parts),
            out_specs=vmem(),
            compiler_params=pltpu.CompilerParams(vmem_limit_bytes=8 << 20),
            cost_estimate=pl.CostEstimate(
                flops=len(parts) * slab * pixels, bytes_accessed=2 << 20, transcendentals=0
            ),
            name="pack",
        )(*parts)

    first = pack([mine] + far)
    forwarded = swap(pack(far), "row", 2)
    first_other = swap(first, "row", 1)

    send_away, send_near, keep_away, keep_near = pl.pallas_call(
        functools.partial(band_kernel, angles, phases),
        out_shape=[jax.ShapeDtypeStruct(part, jnp.bfloat16)] * 4,
        in_specs=[smem()] * 3 + [vmem()],
        out_specs=[vmem()] * 4,
        scratch_shapes=[
            pltpu.VMEM((2, pixels // LANES, GROUP, LANES), jnp.float32),
            pltpu.VMEM((2, pixels // LANES, GROUP, LANES), jnp.float32),
            pltpu.VMEM((bands - 1, 2, slab, LANES), jnp.float32),
        ],
        cost_estimate=pl.CostEstimate(
            flops=4 * frames * slab * pixels * pixels,
            bytes_accessed=12 << 20,
            transcendentals=0,
        ),
        compiler_params=pltpu.CompilerParams(vmem_limit_bytes=14 << 20),
        name="bands",
    )(where, shifts, matrices, spec)

    second = join([across], forwarded)
    second_other = swap(second, "row", 1)
    got_away = swap(send_away, "row", 1)
    got_near = swap(send_near, "row", 1)
    pieces = [first, second, first_other, second_other]

    half_shape = jax.ShapeDtypeStruct((chips // 4, pixels // 2, 2 * columns), jnp.bfloat16)
    wide_scratch = pltpu.VMEM((pixels // LANES, pixels + LANES, LANES), jnp.float32)

    def partial(own):
        return pl.pallas_call(
            functools.partial(numer_kernel, columns, tuple(masks), own),
            out_shape=[half_shape] * 4,
            in_specs=[smem()] * 2 + [vmem()] * 9,
            out_specs=[vmem()] * 4,
            scratch_shapes=[
                wide_scratch,
                pltpu.VMEM((quarter // LANES, 2, LANES, LANES), jnp.float32),
                pltpu.VMEM((bands, 4 * slab, quarter), jnp.bfloat16),
                pltpu.VMEM((bands, 4 * slab, quarter), jnp.bfloat16),
            ],
            cost_estimate=pl.CostEstimate(
                flops=16 * bands * slab * pixels * quarter,
                bytes_accessed=8 << 20,
                transcendentals=0,
            ),
            compiler_params=pltpu.CompilerParams(vmem_limit_bytes=18 << 20),
        )(
            where, shifts, keep_away, got_away, keep_near, got_near, left, *pieces
        )

    away = partial(False)
    moved = [swap(value, "row", mask) for value, mask in zip(away, (2, 4, 2, 4))]
    kept = partial(True)
    power = pl.pallas_call(
        functools.partial(power_kernel, columns, bands, tuple(masks)),
        out_shape=jax.ShapeDtypeStruct((pixels, 2 * columns), jnp.float32),
        in_specs=[smem()] * 2 + [vmem()] * 4 + [pl.BlockSpec(memory_space=pl.ANY)],
        out_specs=vmem(),
        scratch_shapes=[wide_scratch],
        cost_estimate=pl.CostEstimate(
            flops=16000 * pixels * columns, bytes_accessed=5 << 20, transcendentals=0
        ),
        compiler_params=pltpu.CompilerParams(vmem_limit_bytes=12 << 20),
        name="power",
    )(where, shifts, *pieces, kept[0])

    def fold(bit, parts):
        blocks, rows, lanes = parts[0].shape
        share = (blocks // 2, rows, lanes)
        return pl.pallas_call(
            functools.partial(fold_kernel, bit),
            out_shape=[
                jax.ShapeDtypeStruct(share, jnp.bfloat16),
                jax.ShapeDtypeStruct(share, jnp.float32),
            ],
            in_specs=[smem()] + [vmem()] * len(parts),
            out_specs=[vmem()] * 2,
            cost_estimate=pl.CostEstimate(
                flops=blocks * rows * lanes * 4, bytes_accessed=1 << 20, transcendentals=0
            ),
            compiler_params=pltpu.CompilerParams(vmem_limit_bytes=8 << 20),
            name="fold",
        )(where, *parts)

    def widen(value):
        return value.astype(jnp.float32)

    fars = [(widen(moved[h]) + widen(kept[h])).astype(jnp.bfloat16) for h in range(2)]
    stays = [[moved[2 + h], kept[2 + h]] for h in range(2)]
    for bit in range(1, levels):
        over = (2 << bit, 2) if bit == 1 else (2 << bit, 2 << bit)
        for h in range(2):
            stays[h].append(swap(fars[h], "row", over[h]))
            if bit < levels - 1:
                fars[h], stay = fold(bit + 1, stays[h])
                stays[h] = [stay]

    powers = [power]
    cuts = lax.axis_size("cuts")
    for _ in range(cuts - 1):
        powers.append(
            lax.ppermute(powers[-1], "cuts", [(i, (i + 1) % cuts) for i in range(cuts)])
        )
    parts = stays[0] + stays[1] + powers
    half = pl.pallas_call(
        functools.partial(inverse_kernel, columns, float(slices * angles), len(stays[0])),
        out_shape=jax.ShapeDtypeStruct((pixels, 2 * columns), jnp.bfloat16),
        in_specs=[vmem()] * (len(parts) + 2),
        out_specs=vmem(),
        scratch_shapes=[pltpu.VMEM((pixels, 2 * columns), jnp.bfloat16)],
        cost_estimate=pl.CostEstimate(
            flops=8 * pixels * pixels * columns, bytes_accessed=6 << 20, transcendentals=0
        ),
        compiler_params=pltpu.CompilerParams(vmem_limit_bytes=12 << 20),
        name="inverse",
    )(*parts, cosine, sine)
    back = lax.all_to_all(
        half.reshape(devices, slab, 2 * columns), "row", split_axis=0, concat_axis=0, tiled=True
    )
    recon = pl.pallas_call(
        image_kernel,
        out_shape=jax.ShapeDtypeStruct((slab, pixels), jnp.float32),
        in_specs=[vmem()] * 3,
        out_specs=vmem(),
        cost_estimate=pl.CostEstimate(
            flops=4 * slab * pixels * pixels, bytes_accessed=6 << 20, transcendentals=0
        ),
        compiler_params=pltpu.CompilerParams(vmem_limit_bytes=8 << 20),
        name="image",
    )(back, cosine, sine)
    return recon.reshape(otf.shape)


def solution(mesh):
    in_specs = (P("cuts", None, None, "row", None), P("cuts", "row", None), P(), P(), P())
    out_specs = P("cuts", "row", None)

    return jax.shard_map(shards, mesh=mesh, in_specs=in_specs, out_specs=out_specs, check_vma=False)
```

```python
import functools
import math

import jax
import jax.numpy as jnp
from jax import lax
from jax.experimental import pallas as pl
from jax.experimental.pallas import tpu as pltpu
from jax.sharding import PartitionSpec as P


MULTIPLES = (0, 1, -1, 2, -2)
WIENER = 0.1
LANES = 128
GROUP = 16


def turn_of(angle):
    square = angle * angle
    cosine = jnp.zeros_like(angle)
    sine = jnp.zeros_like(angle)
    for order in range(9, -1, -1):
        sign = -1.0 if order % 2 else 1.0
        cosine = cosine * square + sign / math.factorial(2 * order)
        sine = sine * square + sign / math.factorial(2 * order + 1)
    return cosine, sine * angle


def spectra_kernel(slab, index_ref, raw_hbm, spec, cos_ref, sin_ref, left_ref, low, raw_ref, sem):
    fetch = pltpu.make_async_copy(raw_hbm, raw_ref, sem)
    fetch.start()
    pixels = raw_ref.shape[1]
    tile = 256
    chip = index_ref[0] >> 1
    pair = 2 * slab

    column = lax.broadcasted_iota(jnp.int32, (LANES, LANES), 1)
    unit = 2.0 * math.pi / pixels

    @pl.loop(0, pixels // LANES)
    def _(step):
        first = pl.multiple_of(step * LANES, LANES)
        row = first + lax.broadcasted_iota(jnp.int32, (LANES, LANES), 0)
        around = ((row * column + pixels // 2) & (pixels - 1)) - pixels // 2
        low[0, pl.ds(first, LANES), :], low[1, pl.ds(first, LANES), :] = turn_of(
            around.astype(jnp.float32) * unit
        )

    repeat = lax.broadcasted_iota(jnp.int32, (GROUP, LANES), 0)
    factor = 1.0 / math.sqrt(pixels)

    def build(tab):
        around = ((repeat * (tab * LANES) + pixels // 2) & (pixels - 1)) - pixels // 2
        high_cos, high_sin = turn_of(around.astype(jnp.float32) * unit)
        high_cos = high_cos * factor
        high_sin = high_sin * factor
        for first in range(0, pixels, GROUP):
            rows = slice(first, first + GROUP)
            low_cos = low[0, rows, :]
            low_sin = low[1, rows, :]
            cut = slice(tab * LANES, (tab + 1) * LANES)
            cos_ref[rows, cut] = (high_cos * low_cos - high_sin * low_sin).astype(jnp.bfloat16)
            sin_ref[rows, cut] = (high_sin * low_cos + high_cos * low_sin).astype(jnp.bfloat16)

    per_tile = tile // LANES
    for tab in range(per_tile):
        build(tab)
    fetch.wait()
    for step in range(pixels // tile):
        cut = slice(step * tile, (step + 1) * tile)
        spec[0, :, cut] = jnp.dot(raw_ref[...], cos_ref[:, cut], preferred_element_type=jnp.float32)
        spec[1, :, cut] = jnp.dot(raw_ref[...], sin_ref[:, cut], preferred_element_type=jnp.float32)
        if step + 1 < pixels // tile:
            for tab in range(per_tile):
                build((step + 1) * per_tile + tab)

    @pl.loop(0, pixels // LANES)
    def _(step):
        rows = pl.ds(pl.multiple_of(step * LANES, LANES), LANES)
        first = pl.multiple_of(chip * pair // LANES * LANES, LANES)
        mine = []
        for ref in (cos_ref, sin_ref):
            value = ref[rows, pl.ds(first, LANES)]
            if pair < LANES:
                turn = (LANES - (chip * pair & (LANES - 1))) & (LANES - 1)
                value = pltpu.roll(value.astype(jnp.float32), turn, 1)[:, :pair]
                value = value.astype(jnp.bfloat16)
            mine.append(value)
        left_ref[step, 0:LANES, 0:pair] = mine[0]
        left_ref[step, 0:LANES, pair:] = mine[1]
        left_ref[step, LANES:, 0:pair] = -mine[1]
        left_ref[step, LANES:, pair:] = mine[0]


def plain_kernel(angles, phases, index_ref, shift_ref, unmix_ref, spec, phase, *rest):
    outs = rest[:4]
    held = rest[4]
    frames = angles * phases
    slab = spec.shape[1] // frames
    pixels = spec.shape[2]
    lane_tiles = pixels // LANES
    others = len(MULTIPLES) - 1
    index = index_ref[0]
    core = index & 1
    near = (index >> 1) & 1
    quarter_tiles = lane_tiles // 4

    def offset(which, axis):
        return shift_ref[axis, which]

    image_row = index * slab + lax.broadcasted_iota(jnp.int32, (slab, LANES), 0)
    for which in range(angles):
        for m in range(1, others + 1):
            shift = MULTIPLES[m] * offset(which, 0)
            around = ((image_row * shift + pixels // 2) & (pixels - 1)) - pixels // 2
            cosine, sine = turn_of(around.astype(jnp.float32) * (2.0 * math.pi / pixels))
            phase[which * others + m - 1, 0] = cosine
            phase[which * others + m - 1, 1] = sine

    @pl.loop(0, slab // GROUP)
    def _(step):
        rows = step * GROUP
        terms = []
        for which in range(angles):
            for j in range(phases):
                column = shift_ref[2 + which, j]
                here = pl.ds(
                    pl.multiple_of((which * phases + j) * slab + rows, GROUP), GROUP
                )
                terms.append(
                    (here, unmix_ref[which, 0, 0, column], unmix_ref[which, 0, 1, column])
                )
        for tab in range(lane_tiles):
            cut = slice(tab * LANES, (tab + 1) * LANES)
            real = imag = None
            for here, weight_re, weight_im in terms:
                cosine_sum = spec[0, here, cut]
                sine_sum = spec[1, here, cut]
                add_re = weight_re * cosine_sum + weight_im * sine_sum
                add_im = weight_im * cosine_sum - weight_re * sine_sum
                real = add_re if real is None else real + add_re
                imag = add_im if imag is None else imag + add_im
            held[0, tab] = real
            held[1, tab] = imag
        for which, out in enumerate(outs):
            side = (1 - core) if which < 2 else core
            half = (1 - near) if which % 2 == 0 else near
            first = (2 * side + half) * quarter_tiles
            for part in range(2):
                put = pl.ds(pl.multiple_of(part * slab + rows, GROUP), GROUP)
                for i in range(quarter_tiles):
                    out[put, i * LANES : (i + 1) * LANES] = held[part, first + i].astype(
                        jnp.bfloat16
                    )


def band_kernel(
    angles, phases, index_ref, shift_ref, unmix_ref, spec, *rest
):
    phase = rest[0]
    plain = rest[1:5]
    parts = rest[5:9]
    turned_even, turned_odd = rest[9:]
    frames = angles * phases
    slab = spec.shape[1] // frames
    pixels = spec.shape[2]
    lane_tiles = pixels // LANES
    others = len(MULTIPLES) - 1
    index = index_ref[0]
    core = index & 1
    near = (index >> 1) & 1

    def offset(which, axis):
        return shift_ref[axis, which]

    lane = lax.broadcasted_iota(jnp.int32, (GROUP, LANES), 1)
    quarter_tiles = lane_tiles // 4

    def weight(which, m, j):
        column = shift_ref[2 + which, j]
        return unmix_ref[which, m, 0, column], unmix_ref[which, m, 1, column]

    def combine(terms, rows, slot):
        for tab in range(lane_tiles):
            cut = slice(tab * LANES, (tab + 1) * LANES)
            real = imag = None
            for frame, weight_re, weight_im in terms:
                here = pl.ds(pl.multiple_of(frame * slab + rows, GROUP), GROUP)
                cosine_sum = spec[0, here, cut]
                sine_sum = spec[1, here, cut]
                add_re = weight_re * cosine_sum + weight_im * sine_sum
                add_im = weight_im * cosine_sum - weight_re * sine_sum
                real = add_re if real is None else real + add_re
                imag = add_im if imag is None else imag + add_im
            slot[0, tab] = real
            slot[1, tab] = imag

    def put_out(band, rows, slot, shift):
        move = (-shift) & (pixels - 1)
        rest_lanes = move & (LANES - 1)
        turn = (LANES - rest_lanes) & (LANES - 1)
        for which, out in enumerate(parts):
            side = (1 - core) if which < 2 else core
            half = (1 - near) if which % 2 == 0 else near
            first = (2 * side + half) * quarter_tiles + move // LANES
            for part in range(2):
                tiles = [
                    pltpu.roll(slot[part, (first + i) & (lane_tiles - 1)], turn, 1)
                    for i in range(quarter_tiles + 1)
                ]
                put = pl.ds(pl.multiple_of(part * slab + rows, GROUP), GROUP)
                for i in range(quarter_tiles):
                    out[band, put, i * LANES : (i + 1) * LANES] = jnp.where(
                        lane < LANES - rest_lanes, tiles[i], tiles[i + 1]
                    ).astype(jnp.bfloat16)

    def terms_of(band, rows):
        which = band // others
        m = band - which * others + 1
        here = pl.ds(pl.multiple_of(rows, GROUP), GROUP)
        phase_re = phase[band, 0, here, :]
        phase_im = phase[band, 1, here, :]
        terms = []
        for j in range(phases):
            weight_re, weight_im = weight(which, m, j)
            terms.append(
                (
                    which * phases + j,
                    weight_re * phase_re - weight_im * phase_im,
                    weight_re * phase_im + weight_im * phase_re,
                )
            )
        return terms

    def shift_of(band):
        other = jnp.maximum(band - 1, 0)
        which = other // others
        m = other - which * others + 1
        mult = jnp.where(m <= 2, 1, 2) * jnp.where(m % 2 == 1, 1, -1)
        return jnp.where(band == 0, 0, mult * offset(which, 1))

    count = angles * others
    for ref, out in zip(plain, parts):
        out[0] = ref[...]

    @pl.loop(0, slab // GROUP)
    def _(step):
        rows = step * GROUP
        combine(terms_of(0, rows), rows, turned_odd)

        @pl.loop(0, count // 2 - 1)
        def _(pair_index):
            band = 2 * pair_index + 1
            combine(terms_of(band, rows), rows, turned_even)
            put_out(band, rows, turned_odd, shift_of(band))
            combine(terms_of(band + 1, rows), rows, turned_odd)
            put_out(band + 1, rows, turned_even, shift_of(band + 1))

        combine(terms_of(count - 1, rows), rows, turned_even)
        put_out(count - 1, rows, turned_odd, shift_of(count - 1))
        put_out(count, rows, turned_even, shift_of(count))


def shift_by(shift_ref, band, axis):
    if band == 0:
        return 0
    which, m = divmod(band - 1, len(MULTIPLES) - 1)
    return MULTIPLES[m + 1] * shift_ref[axis, which]


def widen_otf(wide, masks, index, refs):
    lane_tiles = wide.shape[0]
    pixels = lane_tiles * LANES
    pieces, slab = refs[0].shape[:2]
    for piece, mask in enumerate(masks):
        ref = refs[piece // pieces]
        start = pl.multiple_of((index ^ mask) * slab, slab)
        for lane in range(lane_tiles):
            wide[lane, pl.ds(start, slab), :] = ref[
                piece % pieces, :, lane * LANES : (lane + 1) * LANES
            ].astype(jnp.float32)
    for lane in range(lane_tiles):
        wide[lane, pixels:, :] = wide[lane, 0 : wide.shape[1] - pixels, :]


def response(wide, shift_ref, q0, band, column, count):
    lane_tiles = wide.shape[0]
    pixels = lane_tiles * LANES
    tile = wide.shape[1] - pixels
    start = (q0 - shift_by(shift_ref, band, 0)) & (pixels - 1)
    column = (column - shift_by(shift_ref, band, 1)) & (pixels - 1)
    rest_lanes = column & (LANES - 1)
    first = column // LANES
    turn = (LANES - rest_lanes) & (LANES - 1)
    lanes = lax.broadcasted_iota(jnp.int32, (tile, LANES), 1)
    turned = [
        pltpu.roll(wide[(first + i) & (lane_tiles - 1), pl.ds(start, tile), :], turn, 1)
        for i in range(count + 1)
    ]
    return [jnp.where(lanes < LANES - rest_lanes, turned[i], turned[i + 1]) for i in range(count)]


def numer_kernel(
    columns, masks, own, index_ref, shift_ref, keep_away, got_away, keep_near, got_near, left_ref,
    *rest
):
    otf_refs = rest[:4]
    outs = rest[4:8]
    wide, total, right, right_up = rest[8:]
    pixels = wide.shape[0] * LANES
    tile = wide.shape[1] - pixels
    bands, twice, width = keep_away.shape
    slab = twice // 2
    tiles = width // LANES
    half = tiles // 2
    index = index_ref[0]
    core = index & 1
    chip = index >> 1
    sides = (chip & 1, (chip >> 1) & 1)
    chosen = sides if own else (1 - sides[0], 1 - sides[1])
    lower = (keep_near, got_near) if own else (keep_away, got_away)

    @pl.loop(0, bands)
    def _(band):
        cut = pl.ds(pl.multiple_of(chosen[1] * (half * LANES), LANES), half * LANES)
        for which, side in ((0, core), (1, 1 - core)):
            for part in range(2):
                put = pl.ds(pl.multiple_of((2 * part + side) * slab, slab), slab)
                rows = slice(part * slab, (part + 1) * slab)
                right[band, put, :] = lower[which][band, rows, :]
                for i, pair in enumerate(((keep_away, got_away), (keep_near, got_near))):
                    to = slice(i * half * LANES, (i + 1) * half * LANES)
                    right_up[band, put, to] = pair[which][band, rows, cut]

    widen_otf(wide, masks, index, otf_refs)
    steps = pixels // tile // 2

    def tile_of(step, upper):
        q0 = pl.multiple_of((step + upper * steps) * tile, tile)
        to = pl.ds(pl.multiple_of(step * tile, tile), tile)
        left = left_ref[step + upper * steps]
        for band in range(bands):
            product = jnp.dot(
                left, (right_up if upper else right)[band], preferred_element_type=jnp.float32
            )
            if upper:
                weights = []
                for side in (1 - sides[0], sides[0]):
                    column = (2 * core + side) * width + chosen[1] * (half * LANES)
                    weights += response(wide, shift_ref, q0, band, column, half)
            else:
                column = (2 * core + chosen[0]) * width
                weights = response(wide, shift_ref, q0, band, column, tiles)
            for i in range(tiles):
                cut = slice(i * LANES, (i + 1) * LANES)
                for part in range(2):
                    value = weights[i] * product[part * tile : (part + 1) * tile, cut]
                    if band == 0:
                        total[i, part] = value
                    else:
                        total[i, part] += value
        for which in range(2):
            out = outs[2 * which + upper]
            first = which if upper else (sides[1] if which else 1 - sides[1])
            per_tile = LANES // columns
            for i in range(half):
                real = total[first * half + i, 0]
                imag = total[first * half + i, 1]
                for j in range(per_tile):
                    cut = slice(j * columns, (j + 1) * columns)
                    out[i * per_tile + j, to, :] = jnp.concatenate(
                        [real[:, cut], imag[:, cut]], axis=1
                    ).astype(jnp.bfloat16)

    for upper in range(2):
        pl.loop(0, steps)(functools.partial(tile_of, upper=upper))


def power_kernel(columns, bands, masks, index_ref, shift_ref, *rest):
    *otf_refs, _, power_ref, wide = rest
    pixels = power_ref.shape[0]
    tile = wide.shape[1] - pixels
    index = index_ref[0]
    core = index & 1
    chip = index >> 1
    levels = (pixels // columns // 2).bit_length() - 1
    place = sum(((chip >> bit) & 1) << (levels - 1 - bit) for bit in range(levels))
    own_column = core * (pixels // 2) + place * columns
    angles = (bands - 1) // (len(MULTIPLES) - 1)
    widen_otf(wide, masks, index, otf_refs)

    @pl.loop(0, pixels // tile)
    def _(step):
        q0 = pl.multiple_of(step * tile, tile)
        gathered = None
        for band in range(bands):
            value = response(wide, shift_ref, q0, band, own_column, 1)[0]
            value = value * value
            gathered = value * float(angles) if band == 0 else gathered + value
        power_ref[pl.ds(q0, tile), :] = jnp.concatenate(
            [gathered[:, :columns], gathered[:, :columns]], axis=1
        )


def fold_kernel(bit, index_ref, *refs):
    *parts, far_ref, stay_ref = refs
    count = far_ref.shape[0]
    side = (index_ref[0] >> (bit + 1)) & 1
    for block in range(count):
        for out, first in ((far_ref, (1 - side) * count), (stay_ref, side * count)):
            value = None
            for ref in parts:
                one = ref[first + block].astype(jnp.float32)
                value = one if value is None else value + one
            out[block] = value.astype(out.dtype)


def inverse_kernel(columns, total, numers, *refs):
    parts = refs[: 2 * numers]
    *powers, cos_ref, sin_ref, half_ref, ratio = refs[2 * numers :]
    pixels = half_ref.shape[0]
    rows = pixels // 2
    for upper in range(2):
        here = slice(upper * rows, (upper + 1) * rows)
        power = powers[0][here, :]
        for ref in powers[1:]:
            power = power + ref[here, :]
        numer = None
        for ref in parts[upper * numers : (upper + 1) * numers]:
            one = ref[0].astype(jnp.float32)
            numer = one if numer is None else numer + one
        ratio[here, :] = (numer / (WIENER + power / total)).astype(jnp.bfloat16)
    tile = 256
    for first in range(0, pixels, tile):
        here = slice(first, first + tile)
        by_cos = jnp.dot(cos_ref[here, :], ratio[...], preferred_element_type=jnp.float32)
        by_sin = jnp.dot(sin_ref[here, :], ratio[...], preferred_element_type=jnp.float32)
        real = by_cos[:, :columns] - by_sin[:, columns:]
        imag = by_cos[:, columns:] + by_sin[:, :columns]
        half_ref[here, :] = jnp.concatenate([real, -imag], axis=1).astype(jnp.bfloat16)


def join_kernel(head_ref, tail_ref, out_ref):
    out_ref[0] = head_ref[...]
    out_ref[1:] = tail_ref[...]


def pack_kernel(*refs):
    out_ref = refs[-1]
    for index, ref in enumerate(refs[:-1]):
        out_ref[index] = ref[...]


def image_kernel(back_ref, cos_ref, sin_ref, out_ref):
    devices, _, twice = back_ref.shape
    columns = twice // 2
    chips = devices // 2
    levels = chips.bit_length() - 1
    pixels = out_ref.shape[1]
    total = None
    for chip in range(chips):
        place = sum(((chip >> bit) & 1) << (levels - 1 - bit) for bit in range(levels))
        rows = []
        for core in range(2):
            start = core * (pixels // 2) + place * columns
            rows += [ref[start : start + columns, :] for ref in (cos_ref, sin_ref)]
        left = jnp.concatenate([back_ref[2 * chip], back_ref[2 * chip + 1]], axis=1)
        value = jnp.dot(left, jnp.concatenate(rows, axis=0), preferred_element_type=jnp.float32)
        total = value if total is None else total + value
    out_ref[...] = total


def smem():
    return pl.BlockSpec(memory_space=pltpu.SMEM)


def vmem():
    return pl.BlockSpec(memory_space=pltpu.VMEM)


def swap(value, axis, mask):
    size = lax.axis_size(axis)
    return lax.ppermute(value, axis, [(i, i ^ mask) for i in range(size)])


def shards(raw, otf, offsets, phase_order, unmix):
    pixels = raw.shape[-1]
    slab = raw.shape[3]
    angles, phases = raw.shape[1:3]
    devices = lax.axis_size("row")
    index = lax.axis_index("row")
    slices = raw.shape[0] * lax.axis_size("cuts")
    chips = devices // 2
    levels = chips.bit_length() - 1
    columns = pixels // devices
    frames = angles * phases
    bands = 1 + angles * (len(MULTIPLES) - 1)

    mine = otf.reshape(slab, pixels).astype(jnp.bfloat16)
    masks = list(range(0, devices, 4))
    far = [swap(mine, "row", mask) for mask in masks[1:]]
    across = swap(mine, "row", 2)
    masks += [mask | 2 for mask in masks]
    masks += [mask | 1 for mask in masks]

    quarter = pixels // 4
    where = index.astype(jnp.int32).reshape(1)
    longer = [(0, 0), (0, phases - angles)]
    shifts = jnp.concatenate([jnp.pad(offsets.T, longer), phase_order], axis=0)
    matrices = jnp.transpose(unmix, (1, 2, 0, 3))
    part = (bands, 2 * slab, quarter)
    left_shape = (pixels // LANES, 2 * LANES, 4 * slab)
    spec, cosine, sine, left = pl.pallas_call(
        functools.partial(spectra_kernel, slab),
        out_shape=[jax.ShapeDtypeStruct((2, frames * slab, pixels), jnp.float32)]
        + [jax.ShapeDtypeStruct((pixels, pixels), jnp.bfloat16)] * 2
        + [jax.ShapeDtypeStruct(left_shape, jnp.bfloat16)],
        in_specs=[smem(), pl.BlockSpec(memory_space=pltpu.HBM)],
        out_specs=[vmem()] * 4,
        scratch_shapes=[
            pltpu.VMEM((2, pixels, LANES), jnp.float32),
            pltpu.VMEM((frames * slab, pixels), jnp.bfloat16),
            pltpu.SemaphoreType.DMA,
        ],
        cost_estimate=pl.CostEstimate(
            flops=4 * frames * slab * pixels * pixels,
            bytes_accessed=12 << 20,
            transcendentals=0,
        ),
        compiler_params=pltpu.CompilerParams(vmem_limit_bytes=20 << 20),
        name="spectra",
    )(where, pltpu.with_memory_space_constraint(raw.reshape(frames * slab, pixels), pltpu.HBM))

    def join(head, tail):
        return pl.pallas_call(
            join_kernel,
            out_shape=jax.ShapeDtypeStruct((tail.shape[0] + 1, slab, pixels), jnp.bfloat16),
            in_specs=[vmem()] * 2,
            out_specs=vmem(),
            compiler_params=pltpu.CompilerParams(vmem_limit_bytes=8 << 20),
            cost_estimate=pl.CostEstimate(
                flops=slab * pixels, bytes_accessed=2 << 20, transcendentals=0
            ),
            name="join",
        )(head[0], tail)

    def pack(parts):
        return pl.pallas_call(
            pack_kernel,
            out_shape=jax.ShapeDtypeStruct((len(parts), slab, pixels), jnp.bfloat16),
            in_specs=[vmem()] * len(parts),
            out_specs=vmem(),
            compiler_params=pltpu.CompilerParams(vmem_limit_bytes=8 << 20),
            cost_estimate=pl.CostEstimate(
                flops=len(parts) * slab * pixels, bytes_accessed=2 << 20, transcendentals=0
            ),
            name="pack",
        )(*parts)

    phase, *plain = pl.pallas_call(
        functools.partial(plain_kernel, angles, phases),
        out_shape=[jax.ShapeDtypeStruct((bands - 1, 2, slab, LANES), jnp.float32)]
        + [jax.ShapeDtypeStruct(part[1:], jnp.bfloat16)] * 4,
        in_specs=[smem()] * 3 + [vmem()],
        out_specs=[vmem()] * 5,
        scratch_shapes=[pltpu.VMEM((2, pixels // LANES, GROUP, LANES), jnp.float32)],
        cost_estimate=pl.CostEstimate(
            flops=frames * slab * pixels * pixels,
            bytes_accessed=8 << 20,
            transcendentals=0,
        ),
        compiler_params=pltpu.CompilerParams(vmem_limit_bytes=12 << 20),
        name="plain",
    )(where, shifts, matrices, spec)

    first = pack([mine] + far)
    forwarded = swap(pack(far), "row", 2)
    first_other = swap(first, "row", 1)

    send_away, send_near, keep_away, keep_near = pl.pallas_call(
        functools.partial(band_kernel, angles, phases),
        out_shape=[jax.ShapeDtypeStruct(part, jnp.bfloat16)] * 4,
        in_specs=[smem()] * 3 + [vmem()] * 6,
        out_specs=[vmem()] * 4,
        scratch_shapes=[
            pltpu.VMEM((2, pixels // LANES, GROUP, LANES), jnp.float32),
            pltpu.VMEM((2, pixels // LANES, GROUP, LANES), jnp.float32),
        ],
        cost_estimate=pl.CostEstimate(
            flops=4 * frames * slab * pixels * pixels,
            bytes_accessed=12 << 20,
            transcendentals=0,
        ),
        compiler_params=pltpu.CompilerParams(vmem_limit_bytes=14 << 20),
        name="bands",
    )(where, shifts, matrices, spec, phase, *plain)

    second = join([across], forwarded)
    second_other = swap(second, "row", 1)
    got_away = swap(send_away, "row", 1)
    got_near = swap(send_near, "row", 1)
    pieces = [first, second, first_other, second_other]

    half_shape = jax.ShapeDtypeStruct((chips // 4, pixels // 2, 2 * columns), jnp.bfloat16)
    wide_scratch = pltpu.VMEM((pixels // LANES, pixels + LANES, LANES), jnp.float32)

    def partial(own):
        return pl.pallas_call(
            functools.partial(numer_kernel, columns, tuple(masks), own),
            out_shape=[half_shape] * 4,
            in_specs=[smem()] * 2 + [vmem()] * 9,
            out_specs=[vmem()] * 4,
            scratch_shapes=[
                wide_scratch,
                pltpu.VMEM((quarter // LANES, 2, LANES, LANES), jnp.float32),
                pltpu.VMEM((bands, 4 * slab, quarter), jnp.bfloat16),
                pltpu.VMEM((bands, 4 * slab, quarter), jnp.bfloat16),
            ],
            cost_estimate=pl.CostEstimate(
                flops=16 * bands * slab * pixels * quarter,
                bytes_accessed=8 << 20,
                transcendentals=0,
            ),
            compiler_params=pltpu.CompilerParams(vmem_limit_bytes=18 << 20),
        )(
            where, shifts, keep_away, got_away, keep_near, got_near, left, *pieces
        )

    away = partial(False)
    moved = [swap(value, "row", mask) for value, mask in zip(away, (2, 4, 2, 4))]
    kept = partial(True)
    power = pl.pallas_call(
        functools.partial(power_kernel, columns, bands, tuple(masks)),
        out_shape=jax.ShapeDtypeStruct((pixels, 2 * columns), jnp.float32),
        in_specs=[smem()] * 2 + [vmem()] * 4 + [pl.BlockSpec(memory_space=pl.ANY)],
        out_specs=vmem(),
        scratch_shapes=[wide_scratch],
        cost_estimate=pl.CostEstimate(
            flops=16000 * pixels * columns, bytes_accessed=5 << 20, transcendentals=0
        ),
        compiler_params=pltpu.CompilerParams(vmem_limit_bytes=12 << 20),
        name="power",
    )(where, shifts, *pieces, kept[0])

    def fold(bit, parts):
        blocks, rows, lanes = parts[0].shape
        share = (blocks // 2, rows, lanes)
        return pl.pallas_call(
            functools.partial(fold_kernel, bit),
            out_shape=[
                jax.ShapeDtypeStruct(share, jnp.bfloat16),
                jax.ShapeDtypeStruct(share, jnp.float32),
            ],
            in_specs=[smem()] + [vmem()] * len(parts),
            out_specs=[vmem()] * 2,
            cost_estimate=pl.CostEstimate(
                flops=blocks * rows * lanes * 4, bytes_accessed=1 << 20, transcendentals=0
            ),
            compiler_params=pltpu.CompilerParams(vmem_limit_bytes=8 << 20),
            name="fold",
        )(where, *parts)

    def widen(value):
        return value.astype(jnp.float32)

    fars = [(widen(moved[h]) + widen(kept[h])).astype(jnp.bfloat16) for h in range(2)]
    stays = [[moved[2 + h], kept[2 + h]] for h in range(2)]
    for bit in range(1, levels):
        over = (2 << bit, 2) if bit == 1 else (2 << bit, 2 << bit)
        for h in range(2):
            stays[h].append(swap(fars[h], "row", over[h]))
            if bit < levels - 1:
                fars[h], stay = fold(bit + 1, stays[h])
                stays[h] = [stay]

    powers = [power]
    cuts = lax.axis_size("cuts")
    for _ in range(cuts - 1):
        powers.append(
            lax.ppermute(powers[-1], "cuts", [(i, (i + 1) % cuts) for i in range(cuts)])
        )
    parts = stays[0] + stays[1] + powers
    half = pl.pallas_call(
        functools.partial(inverse_kernel, columns, float(slices * angles), len(stays[0])),
        out_shape=jax.ShapeDtypeStruct((pixels, 2 * columns), jnp.bfloat16),
        in_specs=[vmem()] * (len(parts) + 2),
        out_specs=vmem(),
        scratch_shapes=[pltpu.VMEM((pixels, 2 * columns), jnp.bfloat16)],
        cost_estimate=pl.CostEstimate(
            flops=8 * pixels * pixels * columns, bytes_accessed=6 << 20, transcendentals=0
        ),
        compiler_params=pltpu.CompilerParams(vmem_limit_bytes=12 << 20),
        name="inverse",
    )(*parts, cosine, sine)
    back = lax.all_to_all(
        half.reshape(devices, slab, 2 * columns), "row", split_axis=0, concat_axis=0, tiled=True
    )
    recon = pl.pallas_call(
        image_kernel,
        out_shape=jax.ShapeDtypeStruct((slab, pixels), jnp.float32),
        in_specs=[vmem()] * 3,
        out_specs=vmem(),
        cost_estimate=pl.CostEstimate(
            flops=4 * slab * pixels * pixels, bytes_accessed=6 << 20, transcendentals=0
        ),
        compiler_params=pltpu.CompilerParams(vmem_limit_bytes=8 << 20),
        name="image",
    )(back, cosine, sine)
    return recon.reshape(otf.shape)


def solution(mesh):
    in_specs = (P("cuts", None, None, "row", None), P("cuts", "row", None), P(), P(), P())
    out_specs = P("cuts", "row", None)

    return jax.shard_map(shards, mesh=mesh, in_specs=in_specs, out_specs=out_specs, check_vma=False)
```

```python
import functools
import math

import jax
import jax.numpy as jnp
from jax import lax
from jax.experimental import pallas as pl
from jax.experimental.pallas import tpu as pltpu
from jax.sharding import PartitionSpec as P


MULTIPLES = (0, 1, -1, 2, -2)
WIENER = 0.1
LANES = 128
GROUP = 16


def turn_of(angle):
    square = angle * angle
    cosine = jnp.zeros_like(angle)
    sine = jnp.zeros_like(angle)
    for order in range(9, -1, -1):
        sign = -1.0 if order % 2 else 1.0
        cosine = cosine * square + sign / math.factorial(2 * order)
        sine = sine * square + sign / math.factorial(2 * order + 1)
    return cosine, sine * angle


def spectra_kernel(slab, index_ref, raw_hbm, spec, cos_ref, sin_ref, left_ref, low, raw_ref, sem):
    fetch = pltpu.make_async_copy(raw_hbm, raw_ref, sem)
    fetch.start()
    pixels = raw_ref.shape[1]
    tile = 256
    chip = index_ref[0] >> 1
    pair = 2 * slab

    column = lax.broadcasted_iota(jnp.int32, (LANES, LANES), 1)
    unit = 2.0 * math.pi / pixels

    @pl.loop(0, pixels // LANES)
    def _(step):
        first = pl.multiple_of(step * LANES, LANES)
        row = first + lax.broadcasted_iota(jnp.int32, (LANES, LANES), 0)
        around = ((row * column + pixels // 2) & (pixels - 1)) - pixels // 2
        low[0, pl.ds(first, LANES), :], low[1, pl.ds(first, LANES), :] = turn_of(
            around.astype(jnp.float32) * unit
        )

    repeat = lax.broadcasted_iota(jnp.int32, (GROUP, LANES), 0)
    factor = 1.0 / math.sqrt(pixels)

    def build(tab):
        around = ((repeat * (tab * LANES) + pixels // 2) & (pixels - 1)) - pixels // 2
        high_cos, high_sin = turn_of(around.astype(jnp.float32) * unit)
        high_cos = high_cos * factor
        high_sin = high_sin * factor
        for first in range(0, pixels, GROUP):
            rows = slice(first, first + GROUP)
            low_cos = low[0, rows, :]
            low_sin = low[1, rows, :]
            cut = slice(tab * LANES, (tab + 1) * LANES)
            cos_ref[rows, cut] = (high_cos * low_cos - high_sin * low_sin).astype(jnp.bfloat16)
            sin_ref[rows, cut] = (high_sin * low_cos + high_cos * low_sin).astype(jnp.bfloat16)

    per_tile = tile // LANES
    for tab in range(per_tile):
        build(tab)
    fetch.wait()
    for step in range(pixels // tile):
        cut = slice(step * tile, (step + 1) * tile)
        spec[0, :, cut] = jnp.dot(raw_ref[...], cos_ref[:, cut], preferred_element_type=jnp.float32)
        spec[1, :, cut] = jnp.dot(raw_ref[...], sin_ref[:, cut], preferred_element_type=jnp.float32)
        if step + 1 < pixels // tile:
            for tab in range(per_tile):
                build((step + 1) * per_tile + tab)

    @pl.loop(0, pixels // LANES)
    def _(step):
        rows = pl.ds(pl.multiple_of(step * LANES, LANES), LANES)
        first = pl.multiple_of(chip * pair // LANES * LANES, LANES)
        mine = []
        for ref in (cos_ref, sin_ref):
            value = ref[rows, pl.ds(first, LANES)]
            if pair < LANES:
                turn = (LANES - (chip * pair & (LANES - 1))) & (LANES - 1)
                value = pltpu.roll(value.astype(jnp.float32), turn, 1)[:, :pair]
                value = value.astype(jnp.bfloat16)
            mine.append(value)
        left_ref[step, 0:LANES, 0:pair] = mine[0]
        left_ref[step, 0:LANES, pair:] = mine[1]
        left_ref[step, LANES:, 0:pair] = -mine[1]
        left_ref[step, LANES:, pair:] = mine[0]


def plain_kernel(angles, phases, index_ref, shift_ref, unmix_ref, spec, phase, *rest):
    outs = rest[:4]
    held = rest[4]
    frames = angles * phases
    slab = spec.shape[1] // frames
    pixels = spec.shape[2]
    lane_tiles = pixels // LANES
    others = len(MULTIPLES) - 1
    index = index_ref[0]
    core = index & 1
    near = (index >> 1) & 1
    quarter_tiles = lane_tiles // 4

    def offset(which, axis):
        return shift_ref[axis, which]

    image_row = index * slab + lax.broadcasted_iota(jnp.int32, (slab, LANES), 0)
    for which in range(angles):
        for m in range(1, others + 1):
            shift = MULTIPLES[m] * offset(which, 0)
            around = ((image_row * shift + pixels // 2) & (pixels - 1)) - pixels // 2
            cosine, sine = turn_of(around.astype(jnp.float32) * (2.0 * math.pi / pixels))
            phase[which * others + m - 1, 0] = cosine
            phase[which * others + m - 1, 1] = sine

    @pl.loop(0, slab // GROUP)
    def _(step):
        rows = step * GROUP
        terms = []
        for which in range(angles):
            for j in range(phases):
                column = shift_ref[2 + which, j]
                here = pl.ds(
                    pl.multiple_of((which * phases + j) * slab + rows, GROUP), GROUP
                )
                terms.append(
                    (here, unmix_ref[which, 0, 0, column], unmix_ref[which, 0, 1, column])
                )
        for tab in range(lane_tiles):
            cut = slice(tab * LANES, (tab + 1) * LANES)
            real = imag = None
            for here, weight_re, weight_im in terms:
                cosine_sum = spec[0, here, cut]
                sine_sum = spec[1, here, cut]
                add_re = weight_re * cosine_sum + weight_im * sine_sum
                add_im = weight_im * cosine_sum - weight_re * sine_sum
                real = add_re if real is None else real + add_re
                imag = add_im if imag is None else imag + add_im
            held[0, tab] = real
            held[1, tab] = imag
        for which, out in enumerate(outs):
            side = (1 - core) if which < 2 else core
            half = (1 - near) if which % 2 == 0 else near
            first = (2 * side + half) * quarter_tiles
            for part in range(2):
                put = pl.ds(pl.multiple_of(part * slab + rows, GROUP), GROUP)
                for i in range(quarter_tiles):
                    out[put, i * LANES : (i + 1) * LANES] = held[part, first + i].astype(
                        jnp.bfloat16
                    )


def band_kernel(
    angles, phases, index_ref, shift_ref, unmix_ref, spec, *rest
):
    phase = rest[0]
    plain = rest[1:5]
    parts = rest[5:9]
    turned_even, turned_odd = rest[9:]
    frames = angles * phases
    slab = spec.shape[1] // frames
    pixels = spec.shape[2]
    lane_tiles = pixels // LANES
    others = len(MULTIPLES) - 1
    index = index_ref[0]
    core = index & 1
    near = (index >> 1) & 1

    def offset(which, axis):
        return shift_ref[axis, which]

    lane = lax.broadcasted_iota(jnp.int32, (GROUP, LANES), 1)
    quarter_tiles = lane_tiles // 4

    def weight(which, m, j):
        column = shift_ref[2 + which, j]
        return unmix_ref[which, m, 0, column], unmix_ref[which, m, 1, column]

    def combine(terms, rows, slot):
        for tab in range(lane_tiles):
            cut = slice(tab * LANES, (tab + 1) * LANES)
            real = imag = None
            for frame, weight_re, weight_im in terms:
                here = pl.ds(pl.multiple_of(frame * slab + rows, GROUP), GROUP)
                cosine_sum = spec[0, here, cut]
                sine_sum = spec[1, here, cut]
                add_re = weight_re * cosine_sum + weight_im * sine_sum
                add_im = weight_im * cosine_sum - weight_re * sine_sum
                real = add_re if real is None else real + add_re
                imag = add_im if imag is None else imag + add_im
            slot[0, tab] = real
            slot[1, tab] = imag

    def put_out(band, rows, slot, shift):
        move = (-shift) & (pixels - 1)
        rest_lanes = move & (LANES - 1)
        turn = (LANES - rest_lanes) & (LANES - 1)
        for which, out in enumerate(parts):
            side = (1 - core) if which < 2 else core
            half = (1 - near) if which % 2 == 0 else near
            first = (2 * side + half) * quarter_tiles + move // LANES
            for part in range(2):
                tiles = [
                    pltpu.roll(slot[part, (first + i) & (lane_tiles - 1)], turn, 1)
                    for i in range(quarter_tiles + 1)
                ]
                put = pl.ds(pl.multiple_of(part * slab + rows, GROUP), GROUP)
                for i in range(quarter_tiles):
                    out[band, put, i * LANES : (i + 1) * LANES] = jnp.where(
                        lane < LANES - rest_lanes, tiles[i], tiles[i + 1]
                    ).astype(jnp.bfloat16)

    def terms_of(band, rows):
        which = band // others
        m = band - which * others + 1
        here = pl.ds(pl.multiple_of(rows, GROUP), GROUP)
        phase_re = phase[band, 0, here, :]
        phase_im = phase[band, 1, here, :]
        terms = []
        for j in range(phases):
            weight_re, weight_im = weight(which, m, j)
            terms.append(
                (
                    which * phases + j,
                    weight_re * phase_re - weight_im * phase_im,
                    weight_re * phase_im + weight_im * phase_re,
                )
            )
        return terms

    def shift_of(band):
        other = jnp.maximum(band - 1, 0)
        which = other // others
        m = other - which * others + 1
        mult = jnp.where(m <= 2, 1, 2) * jnp.where(m % 2 == 1, 1, -1)
        return jnp.where(band == 0, 0, mult * offset(which, 1))

    count = angles * others
    for ref, out in zip(plain, parts):
        out[0] = ref[...]

    @pl.loop(0, slab // GROUP)
    def _(step):
        rows = step * GROUP
        combine(terms_of(0, rows), rows, turned_odd)

        @pl.loop(0, count // 2 - 1)
        def _(pair_index):
            band = 2 * pair_index + 1
            combine(terms_of(band, rows), rows, turned_even)
            put_out(band, rows, turned_odd, shift_of(band))
            combine(terms_of(band + 1, rows), rows, turned_odd)
            put_out(band + 1, rows, turned_even, shift_of(band + 1))

        combine(terms_of(count - 1, rows), rows, turned_even)
        put_out(count - 1, rows, turned_odd, shift_of(count - 1))
        put_out(count, rows, turned_even, shift_of(count))


def shift_by(shift_ref, band, axis):
    if band == 0:
        return 0
    which, m = divmod(band - 1, len(MULTIPLES) - 1)
    return MULTIPLES[m + 1] * shift_ref[axis, which]


def widen_otf(wide, masks, index, refs):
    lane_tiles = wide.shape[0]
    pixels = lane_tiles * LANES
    pieces, slab = refs[0].shape[:2]
    for piece, mask in enumerate(masks):
        ref = refs[piece // pieces]
        start = pl.multiple_of((index ^ mask) * slab, slab)
        for lane in range(lane_tiles):
            wide[lane, pl.ds(start, slab), :] = ref[
                piece % pieces, :, lane * LANES : (lane + 1) * LANES
            ].astype(jnp.float32)
    for lane in range(lane_tiles):
        wide[lane, pixels:, :] = wide[lane, 0 : wide.shape[1] - pixels, :]


def response(wide, shift_ref, q0, band, column, count):
    lane_tiles = wide.shape[0]
    pixels = lane_tiles * LANES
    tile = wide.shape[1] - pixels
    start = (q0 - shift_by(shift_ref, band, 0)) & (pixels - 1)
    column = (column - shift_by(shift_ref, band, 1)) & (pixels - 1)
    rest_lanes = column & (LANES - 1)
    first = column // LANES
    turn = (LANES - rest_lanes) & (LANES - 1)
    lanes = lax.broadcasted_iota(jnp.int32, (tile, LANES), 1)
    turned = [
        pltpu.roll(wide[(first + i) & (lane_tiles - 1), pl.ds(start, tile), :], turn, 1)
        for i in range(count + 1)
    ]
    return [jnp.where(lanes < LANES - rest_lanes, turned[i], turned[i + 1]) for i in range(count)]


def numer_kernel(
    columns, masks, own, index_ref, shift_ref, keep_away, got_away, keep_near, got_near, left_ref,
    *rest
):
    otf_refs = rest[:4]
    outs = rest[4:8]
    wide, total, right, right_up = rest[8:]
    pixels = wide.shape[0] * LANES
    tile = wide.shape[1] - pixels
    bands, twice, width = keep_away.shape
    slab = twice // 2
    tiles = width // LANES
    half = tiles // 2
    index = index_ref[0]
    core = index & 1
    chip = index >> 1
    sides = (chip & 1, (chip >> 1) & 1)
    chosen = sides if own else (1 - sides[0], 1 - sides[1])
    lower = (keep_near, got_near) if own else (keep_away, got_away)

    @pl.loop(0, bands)
    def _(band):
        cut = pl.ds(pl.multiple_of(chosen[1] * (half * LANES), LANES), half * LANES)
        for which, side in ((0, core), (1, 1 - core)):
            for part in range(2):
                put = pl.ds(pl.multiple_of((2 * part + side) * slab, slab), slab)
                rows = slice(part * slab, (part + 1) * slab)
                right[band, put, :] = lower[which][band, rows, :]
                for i, pair in enumerate(((keep_away, got_away), (keep_near, got_near))):
                    to = slice(i * half * LANES, (i + 1) * half * LANES)
                    right_up[band, put, to] = pair[which][band, rows, cut]

    widen_otf(wide, masks, index, otf_refs)
    steps = pixels // tile // 2

    def tile_of(step, upper):
        q0 = pl.multiple_of((step + upper * steps) * tile, tile)
        to = pl.ds(pl.multiple_of(step * tile, tile), tile)
        left = left_ref[step + upper * steps]
        for band in range(bands):
            product = jnp.dot(
                left, (right_up if upper else right)[band], preferred_element_type=jnp.float32
            )
            if upper:
                weights = []
                for side in (1 - sides[0], sides[0]):
                    column = (2 * core + side) * width + chosen[1] * (half * LANES)
                    weights += response(wide, shift_ref, q0, band, column, half)
            else:
                column = (2 * core + chosen[0]) * width
                weights = response(wide, shift_ref, q0, band, column, tiles)
            for i in range(tiles):
                cut = slice(i * LANES, (i + 1) * LANES)
                for part in range(2):
                    value = weights[i] * product[part * tile : (part + 1) * tile, cut]
                    if band == 0:
                        total[i, part] = value
                    else:
                        total[i, part] += value
        for which in range(2):
            out = outs[2 * which + upper]
            first = which if upper else (sides[1] if which else 1 - sides[1])
            per_tile = LANES // columns
            for i in range(half):
                real = total[first * half + i, 0]
                imag = total[first * half + i, 1]
                for j in range(per_tile):
                    cut = slice(j * columns, (j + 1) * columns)
                    out[i * per_tile + j, to, :] = jnp.concatenate(
                        [real[:, cut], imag[:, cut]], axis=1
                    ).astype(jnp.bfloat16)

    for upper in range(2):
        pl.loop(0, steps)(functools.partial(tile_of, upper=upper))


def power_kernel(columns, bands, masks, index_ref, shift_ref, *rest):
    *otf_refs, _, power_ref, wide = rest
    pixels = 2 * power_ref.shape[0]
    tile = wide.shape[1] - pixels
    index = index_ref[0]
    core = index & 1
    chip = index >> 1
    levels = (pixels // columns // 2).bit_length() - 1
    place = sum(((chip >> bit) & 1) << (levels - 1 - bit) for bit in range(levels))
    own_column = core * (pixels // 2) + place * columns
    angles = (bands - 1) // (len(MULTIPLES) - 1)
    widen_otf(wide, masks, index, otf_refs)

    @pl.loop(0, pixels // tile // 2)
    def _(step):
        halves = []
        for upper in range(2):
            q0 = pl.multiple_of(step * tile + upper * (pixels // 2), tile)
            gathered = None
            for band in range(bands):
                value = response(wide, shift_ref, q0, band, own_column, 1)[0]
                value = value * value
                gathered = value * float(angles) if band == 0 else gathered + value
            halves.append(gathered[:, :columns])
        power_ref[pl.ds(pl.multiple_of(step * tile, tile), tile), :] = jnp.concatenate(
            halves, axis=1
        )


def fold_kernel(bit, index_ref, *refs):
    *parts, far_ref, stay_ref = refs
    count = far_ref.shape[0]
    side = (index_ref[0] >> (bit + 1)) & 1
    for block in range(count):
        for out, first in ((far_ref, (1 - side) * count), (stay_ref, side * count)):
            value = None
            for ref in parts:
                one = ref[first + block].astype(jnp.float32)
                value = one if value is None else value + one
            out[block] = value.astype(out.dtype)


def inverse_kernel(columns, total, numers, *refs):
    parts = refs[: 2 * numers]
    *powers, cos_ref, sin_ref, half_ref, ratio = refs[2 * numers :]
    pixels = half_ref.shape[0]
    rows = pixels // 2
    for upper in range(2):
        here = slice(upper * rows, (upper + 1) * rows)
        cut = slice(upper * columns, (upper + 1) * columns)
        power = powers[0][:, cut]
        for ref in powers[1:]:
            power = power + ref[:, cut]
        power = jnp.concatenate([power, power], axis=1)
        numer = None
        for ref in parts[upper * numers : (upper + 1) * numers]:
            one = ref[0].astype(jnp.float32)
            numer = one if numer is None else numer + one
        ratio[here, :] = (numer / (WIENER + power / total)).astype(jnp.bfloat16)
    tile = 256
    for first in range(0, pixels, tile):
        here = slice(first, first + tile)
        by_cos = jnp.dot(cos_ref[here, :], ratio[...], preferred_element_type=jnp.float32)
        by_sin = jnp.dot(sin_ref[here, :], ratio[...], preferred_element_type=jnp.float32)
        real = by_cos[:, :columns] - by_sin[:, columns:]
        imag = by_cos[:, columns:] + by_sin[:, :columns]
        half_ref[here, :] = jnp.concatenate([real, -imag], axis=1).astype(jnp.bfloat16)


def join_kernel(head_ref, tail_ref, out_ref):
    out_ref[0] = head_ref[...]
    out_ref[1:] = tail_ref[...]


def pack_kernel(*refs):
    out_ref = refs[-1]
    for index, ref in enumerate(refs[:-1]):
        out_ref[index] = ref[...]


def image_kernel(back_ref, cos_ref, sin_ref, out_ref):
    devices, _, twice = back_ref.shape
    columns = twice // 2
    chips = devices // 2
    levels = chips.bit_length() - 1
    pixels = out_ref.shape[1]
    total = None
    for chip in range(chips):
        place = sum(((chip >> bit) & 1) << (levels - 1 - bit) for bit in range(levels))
        rows = []
        for core in range(2):
            start = core * (pixels // 2) + place * columns
            rows += [ref[start : start + columns, :] for ref in (cos_ref, sin_ref)]
        left = jnp.concatenate([back_ref[2 * chip], back_ref[2 * chip + 1]], axis=1)
        value = jnp.dot(left, jnp.concatenate(rows, axis=0), preferred_element_type=jnp.float32)
        total = value if total is None else total + value
    out_ref[...] = total


def smem():
    return pl.BlockSpec(memory_space=pltpu.SMEM)


def vmem():
    return pl.BlockSpec(memory_space=pltpu.VMEM)


def swap(value, axis, mask):
    size = lax.axis_size(axis)
    return lax.ppermute(value, axis, [(i, i ^ mask) for i in range(size)])


def shards(raw, otf, offsets, phase_order, unmix):
    pixels = raw.shape[-1]
    slab = raw.shape[3]
    angles, phases = raw.shape[1:3]
    devices = lax.axis_size("row")
    index = lax.axis_index("row")
    slices = raw.shape[0] * lax.axis_size("cuts")
    chips = devices // 2
    levels = chips.bit_length() - 1
    columns = pixels // devices
    frames = angles * phases
    bands = 1 + angles * (len(MULTIPLES) - 1)

    mine = otf.reshape(slab, pixels).astype(jnp.bfloat16)
    masks = list(range(0, devices, 4))
    far = [swap(mine, "row", mask) for mask in masks[1:]]
    across = swap(mine, "row", 2)
    masks += [mask | 2 for mask in masks]
    masks += [mask | 1 for mask in masks]

    quarter = pixels // 4
    where = index.astype(jnp.int32).reshape(1)
    longer = [(0, 0), (0, phases - angles)]
    shifts = jnp.concatenate([jnp.pad(offsets.T, longer), phase_order], axis=0)
    matrices = jnp.transpose(unmix, (1, 2, 0, 3))
    part = (bands, 2 * slab, quarter)
    left_shape = (pixels // LANES, 2 * LANES, 4 * slab)
    spec, cosine, sine, left = pl.pallas_call(
        functools.partial(spectra_kernel, slab),
        out_shape=[jax.ShapeDtypeStruct((2, frames * slab, pixels), jnp.float32)]
        + [jax.ShapeDtypeStruct((pixels, pixels), jnp.bfloat16)] * 2
        + [jax.ShapeDtypeStruct(left_shape, jnp.bfloat16)],
        in_specs=[smem(), pl.BlockSpec(memory_space=pltpu.HBM)],
        out_specs=[vmem()] * 4,
        scratch_shapes=[
            pltpu.VMEM((2, pixels, LANES), jnp.float32),
            pltpu.VMEM((frames * slab, pixels), jnp.bfloat16),
            pltpu.SemaphoreType.DMA,
        ],
        cost_estimate=pl.CostEstimate(
            flops=4 * frames * slab * pixels * pixels,
            bytes_accessed=12 << 20,
            transcendentals=0,
        ),
        compiler_params=pltpu.CompilerParams(vmem_limit_bytes=20 << 20),
        name="spectra",
    )(where, pltpu.with_memory_space_constraint(raw.reshape(frames * slab, pixels), pltpu.HBM))

    def join(head, tail):
        return pl.pallas_call(
            join_kernel,
            out_shape=jax.ShapeDtypeStruct((tail.shape[0] + 1, slab, pixels), jnp.bfloat16),
            in_specs=[vmem()] * 2,
            out_specs=vmem(),
            compiler_params=pltpu.CompilerParams(vmem_limit_bytes=8 << 20),
            cost_estimate=pl.CostEstimate(
                flops=slab * pixels, bytes_accessed=2 << 20, transcendentals=0
            ),
            name="join",
        )(head[0], tail)

    def pack(parts):
        return pl.pallas_call(
            pack_kernel,
            out_shape=jax.ShapeDtypeStruct((len(parts), slab, pixels), jnp.bfloat16),
            in_specs=[vmem()] * len(parts),
            out_specs=vmem(),
            compiler_params=pltpu.CompilerParams(vmem_limit_bytes=8 << 20),
            cost_estimate=pl.CostEstimate(
                flops=len(parts) * slab * pixels, bytes_accessed=2 << 20, transcendentals=0
            ),
            name="pack",
        )(*parts)

    phase, *plain = pl.pallas_call(
        functools.partial(plain_kernel, angles, phases),
        out_shape=[jax.ShapeDtypeStruct((bands - 1, 2, slab, LANES), jnp.float32)]
        + [jax.ShapeDtypeStruct(part[1:], jnp.bfloat16)] * 4,
        in_specs=[smem()] * 3 + [vmem()],
        out_specs=[vmem()] * 5,
        scratch_shapes=[pltpu.VMEM((2, pixels // LANES, GROUP, LANES), jnp.float32)],
        cost_estimate=pl.CostEstimate(
            flops=frames * slab * pixels * pixels,
            bytes_accessed=8 << 20,
            transcendentals=0,
        ),
        compiler_params=pltpu.CompilerParams(vmem_limit_bytes=12 << 20),
        name="plain",
    )(where, shifts, matrices, spec)

    first = pack([mine] + far)
    forwarded = swap(pack(far), "row", 2)
    first_other = swap(first, "row", 1)

    send_away, send_near, keep_away, keep_near = pl.pallas_call(
        functools.partial(band_kernel, angles, phases),
        out_shape=[jax.ShapeDtypeStruct(part, jnp.bfloat16)] * 4,
        in_specs=[smem()] * 3 + [vmem()] * 6,
        out_specs=[vmem()] * 4,
        scratch_shapes=[
            pltpu.VMEM((2, pixels // LANES, GROUP, LANES), jnp.float32),
            pltpu.VMEM((2, pixels // LANES, GROUP, LANES), jnp.float32),
        ],
        cost_estimate=pl.CostEstimate(
            flops=4 * frames * slab * pixels * pixels,
            bytes_accessed=12 << 20,
            transcendentals=0,
        ),
        compiler_params=pltpu.CompilerParams(vmem_limit_bytes=14 << 20),
        name="bands",
    )(where, shifts, matrices, spec, phase, *plain)

    second = join([across], forwarded)
    second_other = swap(second, "row", 1)
    got_away = swap(send_away, "row", 1)
    got_near = swap(send_near, "row", 1)
    pieces = [first, second, first_other, second_other]

    half_shape = jax.ShapeDtypeStruct((chips // 4, pixels // 2, 2 * columns), jnp.bfloat16)
    wide_scratch = pltpu.VMEM((pixels // LANES, pixels + LANES, LANES), jnp.float32)

    def partial(own):
        return pl.pallas_call(
            functools.partial(numer_kernel, columns, tuple(masks), own),
            out_shape=[half_shape] * 4,
            in_specs=[smem()] * 2 + [vmem()] * 9,
            out_specs=[vmem()] * 4,
            scratch_shapes=[
                wide_scratch,
                pltpu.VMEM((quarter // LANES, 2, LANES, LANES), jnp.float32),
                pltpu.VMEM((bands, 4 * slab, quarter), jnp.bfloat16),
                pltpu.VMEM((bands, 4 * slab, quarter), jnp.bfloat16),
            ],
            cost_estimate=pl.CostEstimate(
                flops=16 * bands * slab * pixels * quarter,
                bytes_accessed=8 << 20,
                transcendentals=0,
            ),
            compiler_params=pltpu.CompilerParams(vmem_limit_bytes=18 << 20),
        )(
            where, shifts, keep_away, got_away, keep_near, got_near, left, *pieces
        )

    away = partial(False)
    moved = [swap(value, "row", mask) for value, mask in zip(away[:2], (2, 4))]
    moved += [swap(value, "row", mask) for value, mask in zip(away[2:], (2, 4))]
    kept = partial(True)
    power = pl.pallas_call(
        functools.partial(power_kernel, columns, bands, tuple(masks)),
        out_shape=jax.ShapeDtypeStruct((pixels // 2, 2 * columns), jnp.float32),
        in_specs=[smem()] * 2 + [vmem()] * 4 + [pl.BlockSpec(memory_space=pl.ANY)],
        out_specs=vmem(),
        scratch_shapes=[wide_scratch],
        cost_estimate=pl.CostEstimate(
            flops=16000 * pixels * columns, bytes_accessed=5 << 20, transcendentals=0
        ),
        compiler_params=pltpu.CompilerParams(vmem_limit_bytes=12 << 20),
        name="power",
    )(where, shifts, *pieces, kept[0])

    def fold(bit, parts):
        blocks, rows, lanes = parts[0].shape
        share = (blocks // 2, rows, lanes)
        return pl.pallas_call(
            functools.partial(fold_kernel, bit),
            out_shape=[
                jax.ShapeDtypeStruct(share, jnp.bfloat16),
                jax.ShapeDtypeStruct(share, jnp.float32),
            ],
            in_specs=[smem()] + [vmem()] * len(parts),
            out_specs=[vmem()] * 2,
            cost_estimate=pl.CostEstimate(
                flops=blocks * rows * lanes * 4, bytes_accessed=1 << 20, transcendentals=0
            ),
            compiler_params=pltpu.CompilerParams(vmem_limit_bytes=8 << 20),
            name="fold",
        )(where, *parts)

    def widen(value):
        return value.astype(jnp.float32)

    fars = [(widen(moved[h]) + widen(kept[h])).astype(jnp.bfloat16) for h in range(2)]
    stays = [[moved[2 + h], kept[2 + h]] for h in range(2)]
    for bit in range(1, levels):
        over = (2 << bit, 2) if bit == 1 else (2 << bit, 2 << bit)
        for h in range(2):
            stays[h].append(swap(fars[h], "row", over[h]))
            if bit < levels - 1:
                fars[h], stay = fold(bit + 1, stays[h])
                stays[h] = [stay]

    powers = [power]
    cuts = lax.axis_size("cuts")
    for _ in range(cuts - 1):
        powers.append(lax.ppermute(powers[-1], "cuts", [(i, (i + 1) % cuts) for i in range(cuts)]))
    parts = stays[0] + stays[1] + powers
    half = pl.pallas_call(
        functools.partial(inverse_kernel, columns, float(slices * angles), len(stays[0])),
        out_shape=jax.ShapeDtypeStruct((pixels, 2 * columns), jnp.bfloat16),
        in_specs=[vmem()] * (len(parts) + 2),
        out_specs=vmem(),
        scratch_shapes=[pltpu.VMEM((pixels, 2 * columns), jnp.bfloat16)],
        cost_estimate=pl.CostEstimate(
            flops=8 * pixels * pixels * columns, bytes_accessed=6 << 20, transcendentals=0
        ),
        compiler_params=pltpu.CompilerParams(vmem_limit_bytes=12 << 20),
        name="inverse",
    )(*parts, cosine, sine)
    back = lax.all_to_all(
        half.reshape(devices, slab, 2 * columns), "row", split_axis=0, concat_axis=0, tiled=True
    )
    recon = pl.pallas_call(
        image_kernel,
        out_shape=jax.ShapeDtypeStruct((slab, pixels), jnp.float32),
        in_specs=[vmem()] * 3,
        out_specs=vmem(),
        cost_estimate=pl.CostEstimate(
            flops=4 * slab * pixels * pixels, bytes_accessed=6 << 20, transcendentals=0
        ),
        compiler_params=pltpu.CompilerParams(vmem_limit_bytes=8 << 20),
        name="image",
    )(back, cosine, sine)
    return recon.reshape(otf.shape)


def solution(mesh):
    in_specs = (P("cuts", None, None, "row", None), P("cuts", "row", None), P(), P(), P())
    out_specs = P("cuts", "row", None)

    return jax.shard_map(shards, mesh=mesh, in_specs=in_specs, out_specs=out_specs, check_vma=False)
```
